64 devices in a mesh: data: 4 (over x, y), model: 16 (over z, core).
Axes of the slice: x: 2, y: 2, z: 8, core: 2. Of those that a mesh axis runs over, the one named last changes fastest.
The devices are a block of a 4x4x8 slice.
Arguments:
- images: bfloat16 [12, 256, 256, 64], P('data', None, None, 'model'), parts along dimension 0
- w_conv1: bfloat16 [3, 3, 64, 128], P(None, None, 'model')
- b_conv1: float32 [128], replicated
- w_conv2: bfloat16 [3, 3, 128, 128], replicated
- b_conv2: float32 [128], replicated
- w_short: bfloat16 [64, 128], P('model')
Outputs:
- output: float32 [12, 256, 256, 128], P('data', 'model'), parts along dimension 0
There are 4 independent parts. The reference program is written for one: setup_inputs(seed, part) draws one part's arguments, and reference() takes and returns one part's arrays. A program takes and returns all parts, laid end to end along the dimension named above; an argument that names none is the same for every part.
All inputs are finite; a program needn't handle non-finite values.
Results may differ from the reference program's by a relative error of at most 0.00609846.
Values are sent between devices in bfloat16 or wider.
A program may use at most 768 MiB of HBM per device.

```python
import jax
import jax.numpy as jnp
from jax import lax

IMAGES = 3
IMG_HEIGHT = 256
IMG_WIDTH = 256
C_IN = 64
C_MID = 128
C_OUT = 128
CONV_LAYOUT = ('NHWC', 'HWIO', 'NHWC')


def setup_inputs(seed: int = 0, part: int = 0) -> dict:
    subkeys = jax.random.split(jax.random.key(seed), 6)
    img_key = jax.random.fold_in(subkeys[0], part)
    images = jax.random.normal(img_key, (IMAGES, IMG_HEIGHT, IMG_WIDTH, C_IN), jnp.float32)
    w_conv1 = jax.random.normal(subkeys[1], (3, 3, C_IN, C_MID), jnp.float32) * (9 * C_IN) ** -0.5
    b_conv1 = 0.5 * jax.random.normal(subkeys[2], (C_MID,), jnp.float32)
    w_conv2 = jax.random.normal(subkeys[3], (3, 3, C_MID, C_OUT), jnp.float32) * (4.5 * C_MID) ** -0.5
    b_conv2 = 0.5 * jax.random.normal(subkeys[4], (C_OUT,), jnp.float32)
    w_short = jax.random.normal(subkeys[5], (C_IN, C_OUT), jnp.float32) * C_IN ** -0.5
    return dict(images=images.astype(jnp.bfloat16), w_conv1=w_conv1.astype(jnp.bfloat16), b_conv1=b_conv1, w_conv2=w_conv2.astype(jnp.bfloat16), b_conv2=b_conv2, w_short=w_short.astype(jnp.bfloat16))


def reference(images, w_conv1, b_conv1, w_conv2, b_conv2, w_short):
    kern_one = w_conv1.astype(jnp.float32)
    kern_two = w_conv2.astype(jnp.float32)

    def one_image(img_data):
        z_sum = lax.conv_general_dilated(img_data.astype(jnp.float32)[None], kern_one, (1, 1), 'SAME', dimension_numbers=CONV_LAYOUT)
        hidden = jax.nn.relu(z_sum + b_conv1).astype(jnp.bfloat16)
        conv_two = lax.conv_general_dilated(hidden.astype(jnp.float32), kern_two, (1, 1), 'SAME', dimension_numbers=CONV_LAYOUT)
        shortcut = jnp.dot(img_data.reshape(IMG_HEIGHT * IMG_WIDTH, C_IN), w_short, preferred_element_type=jnp.float32)
        return conv_two[0] + b_conv2 + shortcut.reshape(IMG_HEIGHT, IMG_WIDTH, C_OUT)

    return lax.map(one_image, images)
```

```python
import functools

import jax
import jax.numpy as jnp
from jax import lax
from jax.experimental import pallas as pl
from jax.experimental.pallas import tpu as pltpu
from jax.sharding import PartitionSpec as P

MESH = pl.DeviceIdType.MESH
LANES = 128


def shift_right(v):
    return jnp.concatenate([jnp.zeros((v.shape[0], 1), v.dtype), v[:, :-1]], axis=1)


def shift_left(v):
    return jnp.concatenate([v[:, 1:], jnp.zeros((v.shape[0], 1), v.dtype)], axis=1)


def kernel(n, x_ref, w1_ref, b1_ref, w2_ref, b2_ref, ws_ref, out_ref,
           xbuf, gw, gs, wk, wt, sk, st, w2t, y1s, sbuf, ybuf,
           send_x, recv_x, send_h, recv_top, recv_bot, send_w, recv_w, send_v, recv_v, out_sem):
    ni, height, ch, width = x_ref.shape
    halves = width // LANES
    tile = height // n
    nz = n // 2
    c_mid = w1_ref.shape[3]
    c_out = ws_ref.shape[1]
    me = lax.axis_index('model')
    my_z, my_c = me // 2, me % 2
    sibling = me + 1 - 2 * my_c

    barrier = pltpu.get_barrier_semaphore()
    for k in range(1, n):
        pl.semaphore_signal(barrier, inc=1, device_id={'model': (me + k) % n}, device_id_type=MESH)

    def own_rows(img, h):
        return pltpu.make_async_copy(
            x_ref.at[img, pl.ds(me * tile, tile), :, pl.ds(h * LANES, LANES)],
            xbuf.at[img, me, h, pl.ds(2, tile)], recv_x.at[img])

    for img in range(ni):
        for h in range(halves):
            own_rows(img, h).start()
    own_w = pltpu.make_async_copy(w1_ref, gw.at[my_z, my_c], recv_w.at[0])
    own_s = pltpu.make_async_copy(ws_ref, gs.at[my_z, my_c], recv_w.at[1])
    own_w.start()
    own_s.start()

    pl.semaphore_wait(barrier, n - 1)

    def send_rows(img, dest, h):
        return pltpu.make_async_remote_copy(
            src_ref=x_ref.at[img, pl.ds(dest * tile, tile), :, pl.ds(h * LANES, LANES)],
            dst_ref=xbuf.at[img, me, h, pl.ds(2, tile)],
            send_sem=send_x, recv_sem=recv_x.at[img], device_id={'model': dest}, device_id_type=MESH)

    hops = [nz // 2]
    for d in range(nz // 2 - 1, 0, -1):
        hops += [d, nz - d]

    def send_image(img):
        for d in hops:
            for c in range(2):
                dest = ((my_z + d) % nz) * 2 + (my_c + c) % 2
                for h in range(halves):
                    send_rows(img, dest, h).start()
        for h in range(halves):
            send_rows(img, sibling, h).start()

    send_image(0)
    for d in hops:
        dest = ((my_z + d) % nz) * 2 + my_c
        pltpu.make_async_remote_copy(
            src_ref=w1_ref, dst_ref=gw.at[my_z, my_c], send_sem=send_w.at[0], recv_sem=recv_w.at[0],
            device_id={'model': dest}, device_id_type=MESH).start()
        pltpu.make_async_remote_copy(
            src_ref=ws_ref, dst_ref=gs.at[my_z, my_c], send_sem=send_w.at[1], recv_sem=recv_w.at[1],
            device_id={'model': dest}, device_id_type=MESH).start()
    for img in range(1, ni):
        send_image(img)

    @pl.when(me == 0)
    def _():
        for img in range(ni):
            for h in range(halves):
                xbuf[img, :, h, 0:2] = jnp.zeros((n, 2, ch, LANES), xbuf.dtype)

    @pl.when(me == n - 1)
    def _():
        for img in range(ni):
            for h in range(halves):
                xbuf[img, :, h, tile + 2:tile + 4] = jnp.zeros((n, 2, ch, LANES), xbuf.dtype)

    for t in range(9):
        w2t[:, t * c_mid:(t + 1) * c_mid] = w2_ref[t // 3, t % 3].astype(jnp.float32).T.astype(w2t.dtype)
    wk[...] = jnp.zeros_like(wk)
    sk[...] = jnp.zeros_like(sk)

    for k, ref in enumerate((gw.at[:, my_c], gs.at[:, my_c])):
        pltpu.make_async_remote_copy(src_ref=ref, dst_ref=ref, send_sem=send_v.at[k], recv_sem=recv_w.at[k],
                                     device_id={'model': sibling}, device_id_type=MESH).wait_recv()

    share_w = pltpu.make_async_remote_copy(
        src_ref=gw.at[:, my_c], dst_ref=gw.at[:, my_c], send_sem=send_v.at[0], recv_sem=recv_v.at[0],
        device_id={'model': sibling}, device_id_type=MESH)
    share_s = pltpu.make_async_remote_copy(
        src_ref=gs.at[:, my_c], dst_ref=gs.at[:, my_c], send_sem=send_v.at[1], recv_sem=recv_v.at[1],
        device_id={'model': sibling}, device_id_type=MESH)
    share_w.start()
    share_s.start()
    share_w.wait()
    share_s.wait()

    def place(z, _):
        for c in range(2):
            src = z * 2 + c
            for dh in range(3):
                for dw in range(3):
                    piece = gw[z, c, dh, dw].astype(jnp.float32)
                    for a in range(2):
                        wk[dw, src, (dh + a) * ch:(dh + a + 1) * ch, a * c_mid:(a + 1) * c_mid] = piece
            piece = gs[z, c].astype(jnp.float32)
            for a in range(2):
                sk[src, (1 + a) * ch:(2 + a) * ch, a * c_out:(a + 1) * c_out] = piece
        return 0

    lax.fori_loop(0, nz, place, 0)
    kb = n * 4 * ch
    for dw in range(3):
        wt[:, dw * kb:(dw + 1) * kb] = wk[dw].reshape(kb, 2 * c_mid).T.astype(wt.dtype)
    st[...] = sk[...].reshape(kb, 2 * c_out).T.astype(st.dtype)

    xk = xbuf.reshape(ni, n, halves, (tile + 4) * ch, LANES)
    b1_col = b1_ref[...]
    b2_row = b2_ref[...]

    def pair(img, p):
        x0 = jnp.concatenate(
            [xk[img, :, h, pl.ds(pl.multiple_of(p * 2 * ch, 2 * ch), 4 * ch), :].reshape(kb, LANES) for h in range(halves)], axis=1)
        rhs = jnp.concatenate([shift_right(x0), x0, shift_left(x0)], axis=0)
        z2 = jnp.dot(wt[...], rhs, preferred_element_type=jnp.float32)
        s2 = jnp.dot(st[...], x0, preferred_element_type=jnp.float32)
        for a in range(2):
            y = jnp.maximum(z2[a * c_mid:(a + 1) * c_mid] + b1_col, 0.0)
            row = me * tile - 1 + 2 * p + a
            y = jnp.where((row >= 0) & (row < height), y, 0.0).astype(jnp.bfloat16)
            base = pl.multiple_of((2 * p + a) * 3 * c_mid, 3 * c_mid)
            y1s[pl.ds(base, c_mid), :] = shift_right(y)
            y1s[pl.ds(base + c_mid, c_mid), :] = y
            y1s[pl.ds(base + 2 * c_mid, c_mid), :] = shift_left(y)
            sbuf[2 * p + a] = s2[a * c_out:(a + 1) * c_out]

    def out_copy(img, r):
        return pltpu.make_async_copy(ybuf.at[img, r], out_ref.at[img, r], out_sem)

    def second(img, r):
        rhs = y1s[pl.ds(pl.multiple_of(r * 3 * c_mid, 3 * c_mid), 9 * c_mid), :]
        y2 = jnp.dot(w2t[...], rhs, preferred_element_type=jnp.float32) + sbuf[r + 1]
        ybuf[img, r] = y2.T + b2_row
        out_copy(img, r).start()

    def halo(img, src_row, dst_row, dest, k, recv):
        return pltpu.make_async_remote_copy(
            src_ref=xbuf.at[img, :, :, pl.ds(src_row, 2)], dst_ref=xbuf.at[img, :, :, pl.ds(dst_row, 2)],
            send_sem=send_h.at[img, k], recv_sem=recv.at[img], device_id={'model': dest}, device_id_type=MESH)

    def up(img):
        return halo(img, 2, tile + 2, me - 1, 0, recv_bot)

    def down(img):
        return halo(img, tile, 0, me + 1, 1, recv_top)

    def one_image(img, _):
        pltpu.make_async_remote_copy(
            src_ref=xbuf.at[img, :, :, pl.ds(2, tile)], dst_ref=xbuf.at[img, :, :, pl.ds(2, tile)],
            send_sem=send_x, recv_sem=recv_x.at[img], device_id={'model': sibling}, device_id_type=MESH).wait_recv()

        @pl.when(me > 0)
        def _():
            up(img).start()

        @pl.when(me < n - 1)
        def _():
            down(img).start()

        def inner(p, _):
            pair(img, p)
            return 0

        lax.fori_loop(1, tile // 2, inner, 0)

        @pl.when(me > 0)
        def _():
            halo(img, 2, 0, me, 1, recv_top).wait_recv()

        @pl.when(me < n - 1)
        def _():
            halo(img, 2, tile + 2, me, 0, recv_bot).wait_recv()

        def edge(q, _):
            pair(img, q * (tile // 2))
            return 0

        lax.fori_loop(0, 2, edge, 0)

        def rows(r, _):
            second(img, r)
            return 0

        lax.fori_loop(0, tile, rows, 0, unroll=2)
        return 0

    lax.fori_loop(0, ni, one_image, 0)

    pltpu.make_async_copy(ybuf, out_ref, out_sem).wait()
    sent = xbuf.at[:, pl.ds(0, n - 1), :, pl.ds(2, tile)]
    pltpu.make_async_remote_copy(src_ref=sent, dst_ref=sent, send_sem=send_x, recv_sem=recv_x.at[0],
                                 device_id={'model': sibling}, device_id_type=MESH).wait_send()
    sent_w, sent_s = gw.at[pl.ds(0, nz - 1), 0], gs.at[pl.ds(0, nz - 1), 0]
    for k, ref in enumerate((sent_w, sent_s)):
        pltpu.make_async_remote_copy(src_ref=ref, dst_ref=ref, send_sem=send_w.at[k], recv_sem=recv_w.at[k],
                                     device_id={'model': sibling}, device_id_type=MESH).wait_send()
    for img in range(ni):
        @pl.when(me > 0)
        def _():
            up(img).wait_send()

        @pl.when(me < n - 1)
        def _():
            down(img).wait_send()


def solution(mesh):
    n = mesh.shape['model']

    def local_step(images, w_conv1, b_conv1, w_conv2, b_conv2, w_short):
        x = images.transpose(0, 1, 3, 2)
        ni, height, ch, width = x.shape
        c_mid, c_out = w_conv1.shape[3], w_short.shape[1]
        tile, halves, nz = height // n, width // LANES, n // 2
        kb = n * 4 * ch
        vmem = pl.BlockSpec(memory_space=pltpu.VMEM)
        hbm = pl.BlockSpec(memory_space=pl.ANY)
        dma = pltpu.SemaphoreType.DMA
        return pl.pallas_call(
            functools.partial(kernel, n),
            out_shape=jax.ShapeDtypeStruct((ni, tile, width, c_out), jnp.float32),
            in_specs=[hbm, hbm, vmem, vmem, vmem, hbm],
            out_specs=hbm,
            scratch_shapes=[
                pltpu.VMEM((ni, n, halves, tile + 4, ch, LANES), jnp.bfloat16),
                pltpu.VMEM((nz, 2, 3, 3, ch, c_mid), jnp.bfloat16),
                pltpu.VMEM((nz, 2, ch, c_out), jnp.bfloat16),
                pltpu.VMEM((3, n, 4 * ch, 2 * c_mid), jnp.float32),
                pltpu.VMEM((2 * c_mid, 3 * kb), jnp.bfloat16),
                pltpu.VMEM((n, 4 * ch, 2 * c_out), jnp.float32),
                pltpu.VMEM((2 * c_out, kb), jnp.bfloat16),
                pltpu.VMEM((c_out, 9 * c_mid), jnp.bfloat16),
                pltpu.VMEM(((tile + 2) * 3 * c_mid, width), jnp.bfloat16),
                pltpu.VMEM((tile + 2, c_out, width), jnp.float32),
                pltpu.VMEM((ni, tile, width, c_out), jnp.float32),
                dma, dma((ni,)), dma((ni, 2)), dma((ni,)), dma((ni,)), dma((2,)), dma((2,)), dma((2,)), dma((2,)), dma,
            ],
            compiler_params=pltpu.CompilerParams(collective_id=0, has_side_effects=True),
        )(x, w_conv1, b_conv1.reshape(c_mid, 1), w_conv2, b_conv2.reshape(1, c_out), w_short)

    return jax.shard_map(local_step, mesh=mesh, in_specs=(P('data', None, None, 'model'), P(None, None, 'model', None), P(), P(), P(), P('model', None)), out_specs=P('data', 'model', None, None), check_vma=False)
```

```python
import functools

import jax
import jax.numpy as jnp
from jax import lax
from jax.experimental import pallas as pl
from jax.experimental.pallas import tpu as pltpu
from jax.sharding import PartitionSpec as P

MESH = pl.DeviceIdType.MESH
LANES = 128
EDGE = 4


def shift_right(v):
    return jnp.concatenate([jnp.zeros((v.shape[0], 1), v.dtype), v[:, :-1]], axis=1)


def shift_left(v):
    return jnp.concatenate([v[:, 1:], jnp.zeros((v.shape[0], 1), v.dtype)], axis=1)


def first_pair(n, height, img, p, xbuf, wt, st, b1c, y1s, sbuf):
    ni, _, halves, rows, ch, _ = xbuf.shape
    tile = rows - 4
    c_mid, c_out = wt.shape[0] // 2, st.shape[0] // 2
    kb = n * 4 * ch
    me = lax.axis_index('model')
    xk = xbuf.reshape(ni, n, halves, rows * ch, LANES)
    start = p * (2 * ch) if isinstance(p, int) else pl.multiple_of(p * 2 * ch, 2 * ch)
    x0 = jnp.concatenate([xk[img, :, h, pl.ds(start, 4 * ch), :].reshape(kb, LANES) for h in range(halves)], axis=1)
    rhs = jnp.concatenate([shift_right(x0), x0, shift_left(x0)], axis=0)
    z2 = jnp.dot(wt[...], rhs, preferred_element_type=jnp.float32)
    s2 = jnp.dot(st[...], x0, preferred_element_type=jnp.float32)
    for a in range(2):
        y = jnp.maximum(z2[a * c_mid:(a + 1) * c_mid] + b1c[:, 0:1], 0.0)
        row = me * tile - 1 + 2 * p + a
        y = jnp.where((row >= 0) & (row < height), y, 0.0).astype(jnp.bfloat16)
        base = (2 * p + a) * 3 * c_mid
        if not isinstance(p, int):
            base = pl.multiple_of(base, c_mid)
        y1s[pl.ds(base, c_mid), :] = shift_right(y)
        y1s[pl.ds(base + c_mid, c_mid), :] = y
        y1s[pl.ds(base + 2 * c_mid, c_mid), :] = shift_left(y)
        sbuf[2 * p + a] = s2[a * c_out:(a + 1) * c_out]


def second_row(r, w2t, b2_ref, y1s, sbuf):
    c_mid = w2t.shape[1] // 9
    base = r * 3 * c_mid
    if not isinstance(r, int):
        base = pl.multiple_of(base, c_mid)
    y2 = jnp.dot(w2t[...], y1s[pl.ds(base, 9 * c_mid), :], preferred_element_type=jnp.float32) + sbuf[r + 1]
    return y2.T + b2_ref[...]


def loop(lo, hi, body, unroll=1):
    def step(i, _):
        body(i)
        return 0

    lax.fori_loop(lo, hi, step, 0, unroll=unroll)


def gather_kernel(n, x_ref, w1_ref, b1_hbm, w2_hbm, b2_hbm, ws_ref,
                  xbuf, wt, st, w2t, b1c, b2_ref, y1s, sbuf, y2,
                  gw, gs, wk, sk, w2_ref, b1_ref,
                  local, phase, send_x, recv_x, send_h, recv_top, recv_bot, send_w, recv_w, send_v, recv_v):
    ni, height, ch, width = x_ref.shape
    halves = width // LANES
    tile = height // n
    nz = n // 2
    last = ni - 1
    c_mid, c_out = w1_ref.shape[3], ws_ref.shape[1]
    kb = n * 4 * ch
    me = lax.axis_index('model')
    my_z, my_c = me // 2, me % 2
    sibling = me + 1 - 2 * my_c

    def core(d, c):
        return ((my_z + d) % nz) * 2 + (my_c + c) % 2

    barrier = pltpu.get_barrier_semaphore()
    for dest in (sibling, core(1, 0), core(1, 1), core(nz - 1, 0), core(nz - 1, 1)):
        pl.semaphore_signal(barrier, inc=1, device_id={'model': dest}, device_id_type=MESH)

    whole = [((0, tile), img) for img in range(last)]
    ends = [((0, EDGE), last), ((tile - EDGE, EDGE), last)]
    middle = [((EDGE, tile - 2 * EDGE), ni)]

    def ends_of(img, part, h, dest):
        (r0, rows), k = part
        return (x_ref.at[img, pl.ds(dest * tile + r0, rows), :, pl.ds(h * LANES, LANES)],
                xbuf.at[img, me, h, pl.ds(2 + r0, rows)], recv_x.at[k])

    def keep(img, parts):
        for part in parts:
            for h in range(halves):
                src, dst, sem = ends_of(img, part, h, me)
                pltpu.make_async_copy(src, dst, sem).start()

    def send(img, parts, hops):
        for d in hops:
            for c in range(2) if d else (1,):
                dest = core(d, c)
                for part in parts:
                    for h in range(halves):
                        src, dst, sem = ends_of(img, part, h, dest)
                        pltpu.make_async_remote_copy(src_ref=src, dst_ref=dst, send_sem=send_x, recv_sem=sem,
                                                     device_id={'model': dest}, device_id_type=MESH).start()

    def send_weights(hops):
        for d in hops:
            for k, (src, dst) in enumerate(((w1_ref, gw), (ws_ref, gs))):
                pltpu.make_async_remote_copy(
                    src_ref=src, dst_ref=dst.at[my_z, my_c], send_sem=send_w.at[k], recv_sem=recv_w.at[k],
                    device_id={'model': core(d, 0)}, device_id_type=MESH).start()

    def arrived(ref, sem):
        pltpu.make_async_remote_copy(src_ref=ref, dst_ref=ref, send_sem=send_x, recv_sem=sem,
                                     device_id={'model': sibling}, device_id_type=MESH).wait_recv()

    for img in range(last):
        keep(img, [whole[img]])
    keep(last, ends + middle)
    pltpu.make_async_copy(w1_ref, gw.at[my_z, my_c], recv_w.at[0]).start()
    pltpu.make_async_copy(ws_ref, gs.at[my_z, my_c], recv_w.at[1]).start()

    fetches = [pltpu.make_async_copy(src, dst, local.at[k])
               for k, (src, dst) in enumerate(((b1_hbm, b1_ref), (b2_hbm, b2_ref), (w2_hbm, w2_ref)))]
    for fetch in fetches:
        fetch.start()

    pl.semaphore_wait(barrier, 5)
    for d in range(1, nz // 2 + 1):
        if d < nz // 2:
            for side in (1, nz - 1):
                pl.semaphore_signal(phase.at[d - 1], inc=1, device_id={'model': core(side, 0)}, device_id_type=MESH)
        send(0, [whole[0]], [d, nz - d] if d < nz // 2 else [d])
        if d < nz // 2:
            pl.semaphore_wait(phase.at[d - 1], 2)
    send(0, [whole[0]], [0])
    near = [d for k in range(1, nz // 2) for d in (k, nz - k)]
    far = [nz // 2] + near[::-1]
    first, rest = far[:3], far[3:] + [0]
    send_weights(far)
    send(1, [whole[1]], first)

    for owner, r0 in ((0, 0), (n - 1, tile + 2)):
        @pl.when(me == owner)
        def _():
            for img in range(ni):
                for h in range(halves):
                    xbuf[img, :, h, r0:r0 + 2] = jnp.zeros((n, 2, ch, LANES), xbuf.dtype)

    for fetch in fetches:
        fetch.wait()
    b1c[...] = jnp.broadcast_to(b1_ref[...], (c_mid, c_mid)).T
    for t in range(9):
        w2t[:, t * c_mid:(t + 1) * c_mid] = w2_ref[t // 3, t % 3].astype(jnp.float32).T.astype(w2t.dtype)
    wk[...] = jnp.zeros_like(wk)
    sk[...] = jnp.zeros_like(sk)

    shares = []
    for k, ref in enumerate((gw.at[:, my_c], gs.at[:, my_c])):
        arrived(ref, recv_w.at[k])
        shares.append(pltpu.make_async_remote_copy(
            src_ref=ref, dst_ref=ref, send_sem=send_v.at[k], recv_sem=recv_v.at[k],
            device_id={'model': sibling}, device_id_type=MESH))
        shares[k].start()
    for share in shares:
        share.wait()

    def place(z):
        for c in range(2):
            src = z * 2 + c
            for dh in range(3):
                for dw in range(3):
                    piece = gw[z, c, dh, dw].astype(jnp.float32)
                    for a in range(2):
                        wk[dw, src, (dh + a) * ch:(dh + a + 1) * ch, a * c_mid:(a + 1) * c_mid] = piece
            piece = gs[z, c].astype(jnp.float32)
            for a in range(2):
                sk[src, (1 + a) * ch:(2 + a) * ch, a * c_out:(a + 1) * c_out] = piece

    loop(0, nz, place)
    for dw in range(3):
        wt[:, dw * kb:(dw + 1) * kb] = wk[dw].reshape(kb, 2 * c_mid).T.astype(wt.dtype)
    st[...] = sk[...].reshape(kb, 2 * c_out).T.astype(st.dtype)

    def pair(img, p):
        first_pair(n, height, img, p, xbuf, wt, st, b1c, y1s, sbuf)

    def second(img, r):
        y2[img, r] = second_row(r, w2t, b2_ref, y1s, sbuf)

    def halo(img, src_row, dst_row, dest, k, recv):
        return pltpu.make_async_remote_copy(
            src_ref=xbuf.at[img, :, :, pl.ds(src_row, 2)], dst_ref=xbuf.at[img, :, :, pl.ds(dst_row, 2)],
            send_sem=send_h.at[img, k], recv_sem=recv.at[img], device_id={'model': dest}, device_id_type=MESH)

    def halo_up(img):
        return halo(img, 2, tile + 2, me - 1, 0, recv_bot)

    def halo_down(img):
        return halo(img, tile, 0, me + 1, 1, recv_top)

    def start_halos(img):
        @pl.when(me > 0)
        def _():
            halo_up(img).start()

        @pl.when(me < n - 1)
        def _():
            halo_down(img).start()

    def wait_halos(img):
        @pl.when(me > 0)
        def _():
            halo(img, 2, 0, me, 1, recv_top).wait_recv()

        @pl.when(me < n - 1)
        def _():
            halo(img, 2, tile + 2, me, 0, recv_bot).wait_recv()

    last_pair = tile // 2
    for img in range(last):
        arrived(xbuf.at[img, :, :, pl.ds(2, tile)], recv_x.at[img])
        start_halos(img)
        if img + 1 < last:
            send(img + 1, [whole[img + 1]], rest)
        else:
            send(last, middle, far + [0])
        loop(1, last_pair, lambda p: pair(img, p))
        loop(2, tile - 2, lambda r: second(img, r), unroll=2)
        if img + 2 < last:
            send(img + 2, [whole[img + 2]], first)
        elif img + 2 == last:
            send(last, ends, far + [0])
        wait_halos(img)
        loop(0, 2, lambda q: pair(img, q * last_pair))
        loop(0, 2, lambda q: [second(img, q * (tile - 2) + k) for k in range(2)])

    arrived(xbuf.at[last, :, :, pl.ds(2, 2 * EDGE)], recv_x.at[last])
    start_halos(last)
    wait_halos(last)
    loop(0, 4, lambda q: pair(last, q + (q // 2) * (last_pair - 3)))
    loop(0, 2, lambda q: [second(last, q * (tile - 2) + k) for k in range(2)])

    sent = xbuf.at[:, pl.ds(0, n - 1), :, pl.ds(2, tile)]
    pltpu.make_async_remote_copy(src_ref=sent, dst_ref=sent, send_sem=send_x, recv_sem=recv_x.at[0],
                                 device_id={'model': sibling}, device_id_type=MESH).wait_send()
    for k, ref in enumerate((gw.at[pl.ds(0, nz - 1), 0], gs.at[pl.ds(0, nz - 1), 0])):
        pltpu.make_async_remote_copy(src_ref=ref, dst_ref=ref, send_sem=send_w.at[k], recv_sem=recv_w.at[k],
                                     device_id={'model': sibling}, device_id_type=MESH).wait_send()
    for img in range(ni):
        @pl.when(me > 0)
        def _():
            halo_up(img).wait_send()

        @pl.when(me < n - 1)
        def _():
            halo_down(img).wait_send()
    arrived(xbuf.at[last, :, :, pl.ds(2 + EDGE, tile - 2 * EDGE)], recv_x.at[ni])


def finish_kernel(n, height, xbuf, wt, st, w2t, b1c, b2_ref, y1s_in, sbuf_in, y2, out_ref, y1s, sbuf, yb, sem):
    ni, tile = y2.shape[0], y2.shape[1]
    last = ni - 1
    copies = [pltpu.make_async_copy(y2.at[pl.ds(0, last)], out_ref.at[pl.ds(0, last)], sem.at[0])]
    for k, r in enumerate((0, tile - 2)):
        copies.append(pltpu.make_async_copy(y2.at[last, pl.ds(r, 2)], out_ref.at[last, pl.ds(r, 2)], sem.at[1 + k]))
    for copy in copies:
        copy.start()
    step = 3 * b1c.shape[0]
    for i in (2, tile - 2):
        y1s[i * step:(i + 2) * step] = y1s_in[i * step:(i + 2) * step]
    for i in (3, tile - 2):
        sbuf[i] = sbuf_in[i]
    loop(EDGE // 2, tile // 2 + 1 - EDGE // 2, lambda p: first_pair(n, height, last, p, xbuf, wt, st, b1c, y1s, sbuf))

    def row(r):
        yb[r - 2] = second_row(r, w2t, b2_ref, y1s, sbuf)
        pltpu.make_async_copy(yb.at[r - 2], out_ref.at[last, r], sem.at[3]).start()

    loop(2, tile - 2, row, unroll=2)
    for copy in copies:
        copy.wait()
    pltpu.make_async_copy(yb, out_ref.at[last, pl.ds(2, tile - 4)], sem.at[3]).wait()


def solution(mesh):
    n = mesh.shape['model']

    def local_step(images, w_conv1, b_conv1, w_conv2, b_conv2, w_short):
        x = images.transpose(0, 1, 3, 2)
        ni, height, ch, width = x.shape
        c_mid, c_out = w_conv1.shape[3], w_short.shape[1]
        tile, halves, nz = height // n, width // LANES, n // 2
        kb = n * 4 * ch
        vmem = pl.BlockSpec(memory_space=pltpu.VMEM)
        hbm = pl.BlockSpec(memory_space=pltpu.HBM)
        dma = pltpu.SemaphoreType.DMA
        y1s = pltpu.VMEM(((tile + 2) * 3 * c_mid, width), jnp.bfloat16)
        sbuf = pltpu.VMEM((tile + 2, c_out, width), jnp.float32)
        parts = pl.pallas_call(
            functools.partial(gather_kernel, n),
            out_shape=[
                pltpu.VMEM((ni, n, halves, tile + 4, ch, LANES), jnp.bfloat16),
                pltpu.VMEM((2 * c_mid, 3 * kb), jnp.bfloat16),
                pltpu.VMEM((2 * c_out, kb), jnp.bfloat16),
                pltpu.VMEM((c_out, 9 * c_mid), jnp.bfloat16),
                pltpu.VMEM((c_mid, c_mid), jnp.float32),
                pltpu.VMEM((1, c_out), jnp.float32),
                y1s,
                sbuf,
                pltpu.VMEM((ni, tile, width, c_out), jnp.float32),
            ],
            in_specs=[hbm] * 6,
            out_specs=[vmem] * 9,
            scratch_shapes=[
                pltpu.VMEM((nz, 2, 3, 3, ch, c_mid), jnp.bfloat16),
                pltpu.VMEM((nz, 2, ch, c_out), jnp.bfloat16),
                pltpu.VMEM((3, n, 4 * ch, 2 * c_mid), jnp.float32),
                pltpu.VMEM((n, 4 * ch, 2 * c_out), jnp.float32),
                pltpu.VMEM(w_conv2.shape, w_conv2.dtype),
                pltpu.VMEM((1, c_mid), jnp.float32),
                dma((3,)), pltpu.SemaphoreType.REGULAR((nz // 2,)),
                dma, dma((ni + 1,)), dma((ni, 2)), dma((ni,)), dma((ni,)), dma((2,)), dma((2,)), dma((2,)), dma((2,)),
            ],
            compiler_params=pltpu.CompilerParams(collective_id=0, has_side_effects=True, vmem_limit_bytes=20 * 2**20),
        )(*[pltpu.with_memory_space_constraint(v, pltpu.HBM) for v in (x, w_conv1, b_conv1.reshape(1, c_mid), w_conv2, b_conv2.reshape(1, c_out), w_short)])
        return pl.pallas_call(
            functools.partial(finish_kernel, n, height),
            out_shape=jax.ShapeDtypeStruct((ni, tile, width, c_out), jnp.float32),
            in_specs=[vmem] * 9,
            out_specs=hbm,
            scratch_shapes=[y1s, sbuf, pltpu.VMEM((tile - 4, width, c_out), jnp.float32), dma((4,))],
            compiler_params=pltpu.CompilerParams(vmem_limit_bytes=20 * 2**20),
        )(*parts)

    return jax.shard_map(local_step, mesh=mesh, in_specs=(P('data', None, None, 'model'), P(None, None, 'model', None), P(), P(), P(), P('model', None)), out_specs=P('data', 'model', None, None), check_vma=False)
```

```python
import functools

import jax
import jax.numpy as jnp
from jax import lax
from jax.experimental import pallas as pl
from jax.experimental.pallas import tpu as pltpu
from jax.sharding import PartitionSpec as P

MESH = pl.DeviceIdType.MESH
LANES = 128
LATE = 6
SLOT = (0, 2, 1, 3)


def shift_right(v):
    return jnp.concatenate([jnp.zeros((v.shape[0], 1), v.dtype), v[:, :-1]], axis=1)


def shift_left(v):
    return jnp.concatenate([v[:, 1:], jnp.zeros((v.shape[0], 1), v.dtype)], axis=1)


def first_pair(n, height, img, p, xbuf, wt, st, b1c, y1s, sbuf):
    ni, _, rows, halves, ch, _ = xbuf.shape
    tile = rows - 4
    c_mid, c_out = wt.shape[0] // 2, st.shape[0] // 2
    kb = n * 4 * ch
    me = lax.axis_index('model')
    xk = xbuf.reshape(ni, n, rows * halves * ch, LANES)
    two = 2 * halves * ch
    xa = xk[img, :, pl.ds(pl.multiple_of(p * two, two), two), :]
    xb = xk[img, :, pl.ds(pl.multiple_of((p + 1) * two, two), two), :]
    left = lax.broadcasted_iota(jnp.int32, xa.shape, 1) % (2 * ch) < ch
    x_left = jnp.where(left, xa, pltpu.roll(xb, ch, axis=1))
    x_right = jnp.where(left, pltpu.roll(xa, two - ch, axis=1), xb)
    x0 = jnp.concatenate([x_left.reshape(kb, LANES), x_right.reshape(kb, LANES)], axis=1)
    rhs = jnp.concatenate([shift_right(x0), x0, shift_left(x0)], axis=0)
    z2 = jnp.dot(wt[...], rhs, preferred_element_type=jnp.float32)
    s2 = jnp.dot(st[...], x0, preferred_element_type=jnp.float32)
    for a in range(2):
        y = jnp.maximum(z2[a * c_mid:(a + 1) * c_mid] + b1c[:, 0:1], 0.0)
        row = me * tile - 1 + 2 * p + a
        y = jnp.where((row >= 0) & (row < height), y, 0.0).astype(jnp.bfloat16)
        base = pl.multiple_of((2 * p + a) * 3 * c_mid, c_mid)
        y1s[pl.ds(base, c_mid), :] = shift_right(y)
        y1s[pl.ds(base + c_mid, c_mid), :] = y
        y1s[pl.ds(base + 2 * c_mid, c_mid), :] = shift_left(y)
        sbuf[2 * p + a] = s2[a * c_out:(a + 1) * c_out]


def second_row(r, w2t, b2_ref, y1s, sbuf):
    c_mid = w2t.shape[1] // 9
    base = pl.multiple_of(r * 3 * c_mid, c_mid)
    y2 = jnp.dot(w2t[...], y1s[pl.ds(base, 9 * c_mid), :], preferred_element_type=jnp.float32) + sbuf[r + 1]
    return y2.T + b2_ref[...]


def loop(lo, hi, body, unroll=1):
    def step(i, _):
        body(i)
        return 0

    lax.fori_loop(lo, hi, step, 0, unroll=unroll)


def gather_kernel(n, x_ref, w1_ref, b1_hbm, w2_hbm, b2_hbm, ws_ref,
                  xbuf, wt, st, w2t, b1c, b2_ref, y1s, sbuf, y2,
                  gw, gs, wk, sk, w2_ref, b1_ref,
                  local, phase, send_x, recv_x, send_h, recv_h, send_w, recv_w, send_v, recv_v):
    ni, height, halves, ch, _ = x_ref.shape
    tile = height // n
    nz = n // 2
    last = ni - 1
    c_mid, c_out = w1_ref.shape[3], ws_ref.shape[1]
    kb = n * 4 * ch
    me = lax.axis_index('model')
    my_z, my_c = me // 2, me % 2
    sibling = me + 1 - 2 * my_c

    def core(d, c):
        return ((my_z + d) % nz) * 2 + (my_c + c) % 2

    barrier = pltpu.get_barrier_semaphore()
    for dest in (sibling, core(1, 0), core(1, 1), core(nz - 1, 0), core(nz - 1, 1)):
        pl.semaphore_signal(barrier, inc=1, device_id={'model': dest}, device_id_type=MESH)

    block = tile + 2
    inner, outer = (block - LATE, last), (LATE, ni)

    def part_copy(img, dest, odd, part):
        rows, k = part
        base = jnp.clip(dest * tile - 2 * (1 - odd), 0, height - block)
        off = {block: 0, block - LATE: (1 - odd) * LATE, LATE: odd * (block - LATE)}[rows]
        return (x_ref.at[img, pl.ds(base + off, rows)], xbuf.at[img, me, pl.ds(base + off - dest * tile + 2, rows)], recv_x.at[k])

    def parts_of(img):
        return [(block, img)] if img < last else [inner, outer]

    def send(img, hops, parts):
        for part in parts:
            for d in hops:
                for c in range(2) if d else (1,):
                    dest = core(d, c)
                    src, dst, sem = part_copy(img, dest, (my_c + c) % 2, part)
                    pltpu.make_async_remote_copy(src_ref=src, dst_ref=dst, send_sem=send_x, recv_sem=sem,
                                                 device_id={'model': dest}, device_id_type=MESH).start()

    def send_weights(hops):
        for d in hops:
            for k, (src, dst) in enumerate(((w1_ref, gw), (ws_ref, gs))):
                pltpu.make_async_remote_copy(
                    src_ref=src, dst_ref=dst.at[my_z, my_c], send_sem=send_w.at[k], recv_sem=recv_w.at[k],
                    device_id={'model': core(d, 0)}, device_id_type=MESH).start()

    def arrived(ref, sem):
        pltpu.make_async_remote_copy(src_ref=ref, dst_ref=ref, send_sem=send_x, recv_sem=sem,
                                     device_id={'model': sibling}, device_id_type=MESH).wait_recv()

    for img in range(ni):
        for part in parts_of(img):
            src, dst, sem = part_copy(img, me, my_c, part)
            pltpu.make_async_copy(src, dst, sem).start()
    pltpu.make_async_copy(w1_ref, gw.at[my_z, my_c], recv_w.at[0]).start()
    pltpu.make_async_copy(ws_ref, gs.at[my_z, my_c], recv_w.at[1]).start()

    fetches = [pltpu.make_async_copy(src, dst, local.at[k])
               for k, (src, dst) in enumerate(((b1_hbm, b1_ref), (b2_hbm, b2_ref), (w2_hbm, w2_ref)))]
    for fetch in fetches:
        fetch.start()

    pl.semaphore_wait(barrier, 5)
    for d in range(1, nz // 2 + 1):
        if d < nz // 2:
            for side in (1, nz - 1):
                pl.semaphore_signal(phase.at[d - 1], inc=1, device_id={'model': core(side, 0)}, device_id_type=MESH)
        send(0, [d, nz - d] if d < nz // 2 else [d], parts_of(0))
        if d < nz // 2:
            pl.semaphore_wait(phase.at[d - 1], 2)
    send(0, [0], parts_of(0))
    near = [d for k in range(1, nz // 2) for d in (k, nz - k)]
    far = [nz // 2] + near[::-1]
    send_weights(far)
    for img in range(1, ni):
        send(img, far + [0], parts_of(img))

    for owner, r0 in ((0, 0), (n - 1, tile + 2)):
        @pl.when(me == owner)
        def _():
            for img in range(ni):
                xbuf[img, :, r0:r0 + 2] = jnp.zeros((n, 2, halves, ch, LANES), xbuf.dtype)

    for fetch in fetches:
        fetch.wait()
    b1c[...] = jnp.broadcast_to(b1_ref[...], (c_mid, c_mid)).T
    for t in range(9):
        w2t[:, t * c_mid:(t + 1) * c_mid] = w2_ref[t // 3, t % 3].astype(jnp.float32).T.astype(w2t.dtype)
    wk[...] = jnp.zeros_like(wk)
    sk[...] = jnp.zeros_like(sk)

    shares = []
    for k, ref in enumerate((gw.at[:, my_c], gs.at[:, my_c])):
        arrived(ref, recv_w.at[k])
        shares.append(pltpu.make_async_remote_copy(
            src_ref=ref, dst_ref=ref, send_sem=send_v.at[k], recv_sem=recv_v.at[k],
            device_id={'model': sibling}, device_id_type=MESH))
        shares[k].start()
    for share in shares:
        share.wait()

    def place(z):
        for c in range(2):
            src = z * 2 + c
            for dh in range(3):
                for dw in range(3):
                    piece = gw[z, c, dh, dw].astype(jnp.float32)
                    for a in range(2):
                        wk[dw, src, SLOT[dh + a] * ch:(SLOT[dh + a] + 1) * ch, a * c_mid:(a + 1) * c_mid] = piece
            piece = gs[z, c].astype(jnp.float32)
            for a in range(2):
                sk[src, SLOT[1 + a] * ch:(SLOT[1 + a] + 1) * ch, a * c_out:(a + 1) * c_out] = piece

    loop(0, nz, place)
    for dw in range(3):
        wt[:, dw * kb:(dw + 1) * kb] = wk[dw].reshape(kb, 2 * c_mid).T.astype(wt.dtype)
    st[...] = sk[...].reshape(kb, 2 * c_out).T.astype(st.dtype)

    def pair(img, p):
        first_pair(n, height, img, p, xbuf, wt, st, b1c, y1s, sbuf)

    def second(img, r):
        y2[img, r] = second_row(r, w2t, b2_ref, y1s, sbuf)

    def halo(img):
        return pltpu.make_async_remote_copy(
            src_ref=xbuf.at[img, :, pl.ds(2 + (1 - my_c) * (tile - 2), 2)],
            dst_ref=xbuf.at[img, :, pl.ds(my_c * (tile + 2), 2)],
            send_sem=send_h.at[img], recv_sem=recv_h.at[img], device_id={'model': sibling}, device_id_type=MESH)

    sends_halo = (me != 1) & (me != n - 2)
    takes_halo = (me != 0) & (me != n - 1)

    def start_halo(img):
        @pl.when(sends_halo)
        def _():
            halo(img).start()

    def wait_halo(img):
        @pl.when(takes_halo)
        def _():
            halo(img).wait_recv()

    pairs = tile // 2 + 1
    flip = pairs - 1
    for img in range(last):
        arrived(xbuf.at[img, :, pl.ds(0, block)], recv_x.at[img])
        start_halo(img)
        loop(0, pairs - 1, lambda k: pair(img, k + my_c * (flip - 2 * k)))
        wait_halo(img)
        pair(img, (1 - my_c) * flip)
        loop(0, tile, lambda r: second(img, r), unroll=2)

    arrived(xbuf.at[last, :, pl.ds(0, block - LATE)], recv_x.at[last])
    start_halo(last)
    first_p = LATE // 2 + 1
    loop(first_p, pairs - 1, lambda k: pair(last, k + my_c * (flip - 2 * k)))
    wait_halo(last)
    pair(last, (1 - my_c) * flip)
    done = tile - 2 * first_p
    loop(0, done, lambda r: second(last, r + (1 - my_c) * (tile - done)), unroll=2)

    sent = xbuf.at[:, pl.ds(0, n - 1), pl.ds(0, block)]
    pltpu.make_async_remote_copy(src_ref=sent, dst_ref=sent, send_sem=send_x, recv_sem=recv_x.at[0],
                                 device_id={'model': sibling}, device_id_type=MESH).wait_send()
    for k, ref in enumerate((gw.at[pl.ds(0, nz - 1), 0], gs.at[pl.ds(0, nz - 1), 0])):
        pltpu.make_async_remote_copy(src_ref=ref, dst_ref=ref, send_sem=send_w.at[k], recv_sem=recv_w.at[k],
                                     device_id={'model': sibling}, device_id_type=MESH).wait_send()
    @pl.when(sends_halo)
    def _():
        for img in range(ni):
            halo(img).wait_send()

    arrived(xbuf.at[last, :, pl.ds(0, LATE)], recv_x.at[ni])


def finish_kernel(n, height, xbuf, wt, st, w2t, b1c, b2_ref, y1s_in, sbuf_in, y2, out_ref, y1s, sbuf, yb, sem):
    ni, tile = y2.shape[0], y2.shape[1]
    last = ni - 1
    my_c = lax.axis_index('model') % 2
    first_p = LATE // 2 + 1
    left = 2 * first_p
    done = tile - left
    ready = (1 - my_c) * left
    todo = my_c * done
    copies = [pltpu.make_async_copy(y2.at[pl.ds(0, last)], out_ref.at[pl.ds(0, last)], sem.at[0]),
              pltpu.make_async_copy(y2.at[last, pl.ds(ready, done)], out_ref.at[last, pl.ds(ready, done)], sem.at[1])]
    for copy in copies:
        copy.start()
    step = 3 * b1c.shape[0]
    edge = (1 - my_c) * left + my_c * (tile - left)
    y1s[pl.ds(pl.multiple_of(edge * step, step), 2 * step), :] = y1s_in[pl.ds(pl.multiple_of(edge * step, step), 2 * step), :]
    sbuf[pl.ds(edge, 2)] = sbuf_in[pl.ds(edge, 2)]
    flip = tile // 2
    loop(0, first_p, lambda k: first_pair(n, height, last, k + my_c * (flip - 2 * k), xbuf, wt, st, b1c, y1s, sbuf))

    def row(k):
        yb[k] = second_row(k + todo, w2t, b2_ref, y1s, sbuf)
        pltpu.make_async_copy(yb.at[k], out_ref.at[last, k + todo], sem.at[2]).start()

    loop(0, left, row, unroll=2)
    for copy in copies:
        copy.wait()
    pltpu.make_async_copy(yb, out_ref.at[last, pl.ds(todo, left)], sem.at[2]).wait()


def solution(mesh):
    n = mesh.shape['model']

    def local_step(images, w_conv1, b_conv1, w_conv2, b_conv2, w_short):
        ni, height, width, ch = images.shape
        c_mid, c_out = w_conv1.shape[3], w_short.shape[1]
        tile, halves, nz = height // n, width // LANES, n // 2
        kb = n * 4 * ch
        x = images.transpose(0, 1, 3, 2).reshape(ni, height, ch, halves, LANES).transpose(0, 1, 3, 2, 4)
        vmem = pl.BlockSpec(memory_space=pltpu.VMEM)
        hbm = pl.BlockSpec(memory_space=pltpu.HBM)
        dma = pltpu.SemaphoreType.DMA
        y1s = pltpu.VMEM(((tile + 2) * 3 * c_mid, width), jnp.bfloat16)
        sbuf = pltpu.VMEM((tile + 2, c_out, width), jnp.float32)
        parts = pl.pallas_call(
            functools.partial(gather_kernel, n),
            out_shape=[
                pltpu.VMEM((ni, n, tile + 4, halves, ch, LANES), jnp.bfloat16),
                pltpu.VMEM((2 * c_mid, 3 * kb), jnp.bfloat16),
                pltpu.VMEM((2 * c_out, kb), jnp.bfloat16),
                pltpu.VMEM((c_out, 9 * c_mid), jnp.bfloat16),
                pltpu.VMEM((c_mid, c_mid), jnp.float32),
                pltpu.VMEM((1, c_out), jnp.float32),
                y1s,
                sbuf,
                pltpu.VMEM((ni, tile, width, c_out), jnp.float32),
            ],
            in_specs=[hbm] * 6,
            out_specs=[vmem] * 9,
            scratch_shapes=[
                pltpu.VMEM((nz, 2, 3, 3, ch, c_mid), jnp.bfloat16),
                pltpu.VMEM((nz, 2, ch, c_out), jnp.bfloat16),
                pltpu.VMEM((3, n, 4 * ch, 2 * c_mid), jnp.float32),
                pltpu.VMEM((n, 4 * ch, 2 * c_out), jnp.float32),
                pltpu.VMEM(w_conv2.shape, w_conv2.dtype),
                pltpu.VMEM((1, c_mid), jnp.float32),
                dma((3,)), pltpu.SemaphoreType.REGULAR((nz // 2,)),
                dma, dma((ni + 1,)), dma((ni,)), dma((ni,)), dma((2,)), dma((2,)), dma((2,)), dma((2,)),
            ],
            compiler_params=pltpu.CompilerParams(collective_id=0, has_side_effects=True, vmem_limit_bytes=20 * 2**20),
        )(*[pltpu.with_memory_space_constraint(v, pltpu.HBM) for v in (x, w_conv1, b_conv1.reshape(1, c_mid), w_conv2, b_conv2.reshape(1, c_out), w_short)])
        return pl.pallas_call(
            functools.partial(finish_kernel, n, height),
            out_shape=jax.ShapeDtypeStruct((ni, tile, width, c_out), jnp.float32),
            in_specs=[vmem] * 9,
            out_specs=hbm,
            scratch_shapes=[y1s, sbuf, pltpu.VMEM((LATE + 2, width, c_out), jnp.float32), dma((3,))],
            compiler_params=pltpu.CompilerParams(vmem_limit_bytes=20 * 2**20),
        )(*parts)

    return jax.shard_map(local_step, mesh=mesh, in_specs=(P('data', None, None, 'model'), P(None, None, 'model', None), P(), P(), P(), P('model', None)), out_specs=P('data', 'model', None, None), check_vma=False)
```

```python
import functools

import jax
import jax.numpy as jnp
from jax import lax
from jax.experimental import pallas as pl
from jax.experimental.pallas import tpu as pltpu
from jax.sharding import PartitionSpec as P

MESH = pl.DeviceIdType.MESH
LANES = 128
LATE = 6


def shift_right(v):
    first = lax.broadcasted_iota(jnp.int32, v.shape, 1) == 0
    return jnp.where(first, jnp.zeros_like(v), pltpu.roll(v, 1, axis=1))


def shift_left(v):
    last = lax.broadcasted_iota(jnp.int32, v.shape, 1) == v.shape[1] - 1
    return jnp.where(last, jnp.zeros_like(v), pltpu.roll(v, v.shape[1] - 1, axis=1))


def first_pair(n, height, img, p, xbuf, wt, st, b1c, y1s, sbuf):
    ni, _, rows, halves, ch, _ = xbuf.shape
    tile = rows - 4
    c_mid, c_out = wt.shape[0] // 2, st.shape[0] // 2
    kb = n * 4 * ch
    me = lax.axis_index('model')
    x_left = xbuf[img, :, pl.ds(2 * p, 4), 0]
    x_right = xbuf[img, :, pl.ds(2 * p, 4), 1]
    x0 = jnp.concatenate([x_left.reshape(kb, LANES), x_right.reshape(kb, LANES)], axis=1)
    rhs = jnp.concatenate([shift_right(x0), x0, shift_left(x0)], axis=0)
    z2 = jnp.dot(wt[...], rhs, preferred_element_type=jnp.float32)
    s2 = jnp.dot(st[...], x0, preferred_element_type=jnp.float32)
    for a in range(2):
        y = jnp.maximum(z2[a * c_mid:(a + 1) * c_mid] + jnp.concatenate([b1c[...]] * halves, axis=1), 0.0)
        row = me * tile - 1 + 2 * p + a
        y = jnp.where((row >= 0) & (row < height), y, 0.0).astype(jnp.bfloat16)
        base = pl.multiple_of((2 * p + a) * 3 * c_mid, c_mid)
        y1s[pl.ds(base, c_mid), :] = shift_right(y)
        y1s[pl.ds(base + c_mid, c_mid), :] = y
        y1s[pl.ds(base + 2 * c_mid, c_mid), :] = shift_left(y)
        sbuf[2 * p + a] = s2[a * c_out:(a + 1) * c_out]


def second_row(r, w2t, b2_ref, y1s, sbuf):
    c_mid = w2t.shape[1] // 9
    base = pl.multiple_of(r * 3 * c_mid, c_mid)
    y2 = jnp.dot(w2t[...], y1s[pl.ds(base, 9 * c_mid), :], preferred_element_type=jnp.float32) + sbuf[r + 1]
    return y2.T + b2_ref[...]


def loop(lo, hi, body, unroll=1):
    def step(i, _):
        body(i)
        return 0

    lax.fori_loop(lo, hi, step, 0, unroll=unroll)


def gather_kernel(n, x_ref, w1_ref, b1_hbm, w2_hbm, b2_hbm, ws_ref,
                  xbuf, wt, st, w2t, b1c, b2_ref, y1s, sbuf, y2,
                  gw, gs, wk, sk, w2_ref, b1_ref,
                  local, phase, send_x, recv_x, send_h, recv_h, send_w, recv_w, send_v, recv_v):
    ni, height, halves, ch, _ = x_ref.shape
    tile = height // n
    nz = n // 2
    last = ni - 1
    c_mid, c_out = w1_ref.shape[3], ws_ref.shape[1]
    kb = n * 4 * ch
    me = lax.axis_index('model')
    my_z, my_c = me // 2, me % 2
    sibling = me + 1 - 2 * my_c

    def core(d, c):
        return ((my_z + d) % nz) * 2 + (my_c + c) % 2

    barrier = pltpu.get_barrier_semaphore()
    for dest in (sibling, core(1, 0), core(1, 1), core(nz - 1, 0), core(nz - 1, 1)):
        pl.semaphore_signal(barrier, inc=1, device_id={'model': dest}, device_id_type=MESH)

    block = tile + 2
    inner, outer = (block - LATE, last), (LATE, ni)

    def part_copy(img, dest, odd, part):
        rows, k = part
        base = jnp.clip(dest * tile - 2 * (1 - odd), 0, height - block)
        off = {block: 0, block - LATE: (1 - odd) * LATE, LATE: odd * (block - LATE)}[rows]
        return (x_ref.at[img, pl.ds(base + off, rows)], xbuf.at[img, me, pl.ds(base + off - dest * tile + 2, rows)], recv_x.at[k])

    def parts_of(img):
        return [(block, img)] if img < last else [inner, outer]

    def send(img, hops, parts):
        for part in parts:
            for d in hops:
                for c in range(2) if d else (1,):
                    dest = core(d, c)
                    src, dst, sem = part_copy(img, dest, (my_c + c) % 2, part)
                    pltpu.make_async_remote_copy(src_ref=src, dst_ref=dst, send_sem=send_x, recv_sem=sem,
                                                 device_id={'model': dest}, device_id_type=MESH).start()

    def send_weights(hops):
        for d in hops:
            for k, (src, dst) in enumerate(((w1_ref, gw), (ws_ref, gs))):
                pltpu.make_async_remote_copy(
                    src_ref=src, dst_ref=dst.at[my_z, my_c], send_sem=send_w.at[k], recv_sem=recv_w.at[k],
                    device_id={'model': core(d, 0)}, device_id_type=MESH).start()

    def arrived(ref, sem):
        pltpu.make_async_remote_copy(src_ref=ref, dst_ref=ref, send_sem=send_x, recv_sem=sem,
                                     device_id={'model': sibling}, device_id_type=MESH).wait_recv()

    for img in range(ni):
        for part in parts_of(img):
            src, dst, sem = part_copy(img, me, my_c, part)
            pltpu.make_async_copy(src, dst, sem).start()
    pltpu.make_async_copy(w1_ref, gw.at[my_z, my_c], recv_w.at[0]).start()
    pltpu.make_async_copy(ws_ref, gs.at[my_z, my_c], recv_w.at[1]).start()

    fetches = [pltpu.make_async_copy(src, dst, local.at[k])
               for k, (src, dst) in enumerate(((b1_hbm, b1_ref), (b2_hbm, b2_ref), (w2_hbm, w2_ref)))]
    for fetch in fetches:
        fetch.start()

    pl.semaphore_wait(barrier, 5)
    for d in range(1, nz // 2 + 1):
        if d < nz // 2:
            for side in (1, nz - 1):
                pl.semaphore_signal(phase.at[d - 1], inc=1, device_id={'model': core(side, 0)}, device_id_type=MESH)
        send(0, [d, nz - d] if d < nz // 2 else [d], parts_of(0))
        if d < nz // 2:
            pl.semaphore_wait(phase.at[d - 1], 2)
    send(0, [0], parts_of(0))
    near = [d for k in range(1, nz // 2) for d in (k, nz - k)]
    far = [nz // 2] + near[::-1]
    send_weights(far)
    for img in range(1, ni):
        send(img, far + [0], parts_of(img))

    for owner, r0 in ((0, 0), (n - 1, tile + 2)):
        @pl.when(me == owner)
        def _():
            for img in range(ni):
                xbuf[img, :, r0:r0 + 2] = jnp.zeros((n, 2, halves, ch, LANES), xbuf.dtype)

    for fetch in fetches:
        fetch.wait()
    b1c[...] = jnp.broadcast_to(b1_ref[...], (LANES, c_mid)).T
    for t in range(9):
        w2t[:, t * c_mid:(t + 1) * c_mid] = w2_ref[t // 3, t % 3].astype(jnp.float32).T.astype(w2t.dtype)
    wk[...] = jnp.zeros_like(wk)
    sk[...] = jnp.zeros_like(sk)

    shares = []
    for k, ref in enumerate((gw.at[:, my_c], gs.at[:, my_c])):
        arrived(ref, recv_w.at[k])
        shares.append(pltpu.make_async_remote_copy(
            src_ref=ref, dst_ref=ref, send_sem=send_v.at[k], recv_sem=recv_v.at[k],
            device_id={'model': sibling}, device_id_type=MESH))
        shares[k].start()
    for share in shares:
        share.wait()

    def place(z):
        for c in range(2):
            src = z * 2 + c
            for dh in range(3):
                for dw in range(3):
                    piece = gw[z, c, dh, dw].astype(jnp.float32)
                    for a in range(2):
                        wk[dw, src, (dh + a) * ch:(dh + a + 1) * ch, a * c_mid:(a + 1) * c_mid] = piece
            piece = gs[z, c].astype(jnp.float32)
            for a in range(2):
                sk[src, (1 + a) * ch:(2 + a) * ch, a * c_out:(a + 1) * c_out] = piece

    loop(0, nz, place)
    for dw in range(3):
        wt[:, dw * kb:(dw + 1) * kb] = wk[dw].reshape(kb, 2 * c_mid).T.astype(wt.dtype)
    st[...] = sk[...].reshape(kb, 2 * c_out).T.astype(st.dtype)

    def pair(img, p):
        first_pair(n, height, img, p, xbuf, wt, st, b1c, y1s, sbuf)

    def second(img, r):
        y2[img, r] = second_row(r, w2t, b2_ref, y1s, sbuf)

    def halo(img):
        return pltpu.make_async_remote_copy(
            src_ref=xbuf.at[img, :, pl.ds(2 + (1 - my_c) * (tile - 2), 2)],
            dst_ref=xbuf.at[img, :, pl.ds(my_c * (tile + 2), 2)],
            send_sem=send_h.at[img], recv_sem=recv_h.at[img], device_id={'model': sibling}, device_id_type=MESH)

    sends_halo = (me != 1) & (me != n - 2)
    takes_halo = (me != 0) & (me != n - 1)

    def start_halo(img):
        @pl.when(sends_halo)
        def _():
            halo(img).start()

    def wait_halo(img):
        @pl.when(takes_halo)
        def _():
            halo(img).wait_recv()

    pairs = tile // 2 + 1
    flip = pairs - 1
    for img in range(last):
        arrived(xbuf.at[img, :, pl.ds(0, block)], recv_x.at[img])
        start_halo(img)
        loop(0, pairs - 1, lambda k: pair(img, k + my_c * (flip - 2 * k)), unroll=4)
        wait_halo(img)
        pair(img, (1 - my_c) * flip)
        loop(0, tile, lambda r: second(img, r), unroll=4)

    arrived(xbuf.at[last, :, pl.ds(0, block - LATE)], recv_x.at[last])
    start_halo(last)
    first_p = LATE // 2 + 1
    loop(first_p, pairs - 1, lambda k: pair(last, k + my_c * (flip - 2 * k)), unroll=4)
    wait_halo(last)
    pair(last, (1 - my_c) * flip)
    done = tile - 2 * first_p
    loop(0, done, lambda r: second(last, r + (1 - my_c) * (tile - done)), unroll=4)

    sent = xbuf.at[:, pl.ds(0, n - 1), pl.ds(0, block)]
    pltpu.make_async_remote_copy(src_ref=sent, dst_ref=sent, send_sem=send_x, recv_sem=recv_x.at[0],
                                 device_id={'model': sibling}, device_id_type=MESH).wait_send()
    for k, ref in enumerate((gw.at[pl.ds(0, nz - 1), 0], gs.at[pl.ds(0, nz - 1), 0])):
        pltpu.make_async_remote_copy(src_ref=ref, dst_ref=ref, send_sem=send_w.at[k], recv_sem=recv_w.at[k],
                                     device_id={'model': sibling}, device_id_type=MESH).wait_send()
    @pl.when(sends_halo)
    def _():
        for img in range(ni):
            halo(img).wait_send()

    arrived(xbuf.at[last, :, pl.ds(0, LATE)], recv_x.at[ni])


def finish_kernel(n, height, xbuf, wt, st, w2t, b1c, b2_ref, y1s_in, sbuf_in, y2, out_ref, y1s, sbuf, yb, sem):
    ni, tile = y2.shape[0], y2.shape[1]
    last = ni - 1
    my_c = lax.axis_index('model') % 2
    first_p = LATE // 2 + 1
    left = 2 * first_p
    done = tile - left
    ready = (1 - my_c) * left
    todo = my_c * done
    copies = [pltpu.make_async_copy(y2.at[pl.ds(0, last)], out_ref.at[pl.ds(0, last)], sem.at[0]),
              pltpu.make_async_copy(y2.at[last, pl.ds(ready, done)], out_ref.at[last, pl.ds(ready, done)], sem.at[1])]
    for copy in copies:
        copy.start()
    step = 3 * b1c.shape[0]
    edge = (1 - my_c) * left + my_c * (tile - left)
    y1s[pl.ds(pl.multiple_of(edge * step, step), 2 * step), :] = y1s_in[pl.ds(pl.multiple_of(edge * step, step), 2 * step), :]
    sbuf[pl.ds(edge, 2)] = sbuf_in[pl.ds(edge, 2)]
    flip = tile // 2
    loop(0, first_p, lambda k: first_pair(n, height, last, k + my_c * (flip - 2 * k), xbuf, wt, st, b1c, y1s, sbuf), unroll=4)

    def row(k):
        yb[k] = second_row(k + todo, w2t, b2_ref, y1s, sbuf)
        pltpu.make_async_copy(yb.at[k], out_ref.at[last, k + todo], sem.at[2]).start()

    loop(0, left, row, unroll=8)
    for copy in copies:
        copy.wait()
    pltpu.make_async_copy(yb, out_ref.at[last, pl.ds(todo, left)], sem.at[2]).wait()


def solution(mesh):
    n = mesh.shape['model']

    def local_step(images, w_conv1, b_conv1, w_conv2, b_conv2, w_short):
        ni, height, width, ch = images.shape
        c_mid, c_out = w_conv1.shape[3], w_short.shape[1]
        tile, halves, nz = height // n, width // LANES, n // 2
        kb = n * 4 * ch
        x = images.transpose(0, 1, 3, 2).reshape(ni, height, ch, halves, LANES).transpose(0, 1, 3, 2, 4)
        vmem = pl.BlockSpec(memory_space=pltpu.VMEM)
        hbm = pl.BlockSpec(memory_space=pltpu.HBM)
        dma = pltpu.SemaphoreType.DMA
        y1s = pltpu.VMEM(((tile + 2) * 3 * c_mid, width), jnp.bfloat16)
        sbuf = pltpu.VMEM((tile + 2, c_out, width), jnp.float32)
        parts = pl.pallas_call(
            functools.partial(gather_kernel, n),
            out_shape=[
                pltpu.VMEM((ni, n, tile + 4, halves, ch, LANES), jnp.bfloat16),
                pltpu.VMEM((2 * c_mid, 3 * kb), jnp.bfloat16),
                pltpu.VMEM((2 * c_out, kb), jnp.bfloat16),
                pltpu.VMEM((c_out, 9 * c_mid), jnp.bfloat16),
                pltpu.VMEM((c_mid, LANES), jnp.float32),
                pltpu.VMEM((1, c_out), jnp.float32),
                y1s,
                sbuf,
                pltpu.VMEM((ni, tile, width, c_out), jnp.float32),
            ],
            in_specs=[hbm] * 6,
            out_specs=[vmem] * 9,
            scratch_shapes=[
                pltpu.VMEM((nz, 2, 3, 3, ch, c_mid), jnp.bfloat16),
                pltpu.VMEM((nz, 2, ch, c_out), jnp.bfloat16),
                pltpu.VMEM((3, n, 4 * ch, 2 * c_mid), jnp.float32),
                pltpu.VMEM((n, 4 * ch, 2 * c_out), jnp.float32),
                pltpu.VMEM(w_conv2.shape, w_conv2.dtype),
                pltpu.VMEM((1, c_mid), jnp.float32),
                dma((3,)), pltpu.SemaphoreType.REGULAR((nz // 2,)),
                dma, dma((ni + 1,)), dma((ni,)), dma((ni,)), dma((2,)), dma((2,)), dma((2,)), dma((2,)),
            ],
            compiler_params=pltpu.CompilerParams(collective_id=0, has_side_effects=True, vmem_limit_bytes=20 * 2**20),
        )(*[pltpu.with_memory_space_constraint(v, pltpu.HBM) for v in (x, w_conv1, b_conv1.reshape(1, c_mid), w_conv2, b_conv2.reshape(1, c_out), w_short)])
        return pl.pallas_call(
            functools.partial(finish_kernel, n, height),
            out_shape=jax.ShapeDtypeStruct((ni, tile, width, c_out), jnp.float32),
            in_specs=[vmem] * 9,
            out_specs=hbm,
            scratch_shapes=[y1s, sbuf, pltpu.VMEM((LATE + 2, width, c_out), jnp.float32), dma((3,))],
            compiler_params=pltpu.CompilerParams(vmem_limit_bytes=20 * 2**20),
        )(*parts)

    return jax.shard_map(local_step, mesh=mesh, in_specs=(P('data', None, None, 'model'), P(None, None, 'model', None), P(), P(), P(), P('model', None)), out_specs=P('data', 'model', None, None), check_vma=False)
```

```python
import functools

import jax
import jax.numpy as jnp
from jax import lax
from jax.experimental import pallas as pl
from jax.experimental.pallas import tpu as pltpu
from jax.sharding import PartitionSpec as P

MESH = pl.DeviceIdType.MESH
LANES = 128
LATE = 6


def shift_right(v):
    first = lax.broadcasted_iota(jnp.int32, v.shape, 1) == 0
    return jnp.where(first, jnp.zeros_like(v), pltpu.roll(v, 1, axis=1))


def shift_left(v):
    last = lax.broadcasted_iota(jnp.int32, v.shape, 1) == v.shape[1] - 1
    return jnp.where(last, jnp.zeros_like(v), pltpu.roll(v, v.shape[1] - 1, axis=1))


def first_pair(n, height, img, p, xbuf, wt, st, b1c, y1s, sbuf):
    ni, _, rows, halves, ch, _ = xbuf.shape
    tile = rows - 4
    c_mid, c_out = wt.shape[0] // 2, st.shape[0] // 2
    kb = n * 4 * ch
    me = lax.axis_index('model')
    x_left = xbuf[img, :, pl.ds(2 * p, 4), 0]
    x_right = xbuf[img, :, pl.ds(2 * p, 4), 1]
    x0 = jnp.concatenate([x_left.reshape(kb, LANES), x_right.reshape(kb, LANES)], axis=1)
    rhs = jnp.concatenate([shift_right(x0), x0, shift_left(x0)], axis=0)
    z2 = jnp.dot(wt[...], rhs, preferred_element_type=jnp.float32)
    s2 = jnp.dot(st[...], x0, preferred_element_type=jnp.float32)
    for a in range(2):
        y = jnp.maximum(z2[a * c_mid:(a + 1) * c_mid] + jnp.concatenate([b1c[...]] * halves, axis=1), 0.0)
        row = me * tile - 1 + 2 * p + a
        y = jnp.where((row >= 0) & (row < height), y, 0.0).astype(jnp.bfloat16)
        base = pl.multiple_of((2 * p + a) * 3 * c_mid, c_mid)
        y1s[pl.ds(base, c_mid), :] = shift_right(y)
        y1s[pl.ds(base + c_mid, c_mid), :] = y
        y1s[pl.ds(base + 2 * c_mid, c_mid), :] = shift_left(y)
        sbuf[2 * p + a] = s2[a * c_out:(a + 1) * c_out]


def second_row(r, w2t, b2_ref, y1s, sbuf):
    c_mid = w2t.shape[1] // 9
    base = pl.multiple_of(r * 3 * c_mid, c_mid)
    y2 = jnp.dot(w2t[...], y1s[pl.ds(base, 9 * c_mid), :], preferred_element_type=jnp.float32) + sbuf[r + 1]
    return y2.T + b2_ref[...]


def loop(lo, hi, body, unroll=1):
    def step(i, _):
        body(i)
        return 0

    lax.fori_loop(lo, hi, step, 0, unroll=unroll)


def gather_kernel(n, x_ref, w1_ref, b1_hbm, w2_hbm, b2_hbm, ws_ref,
                  xbuf, wt, st, w2t, b1c, b2_ref, y1s, sbuf, y2,
                  gw, gs, wk, sk, w2_ref, b1_ref,
                  local, phase, send_x, recv_x, send_h, recv_h, send_w, recv_w, send_v, recv_v):
    ni, height, halves, ch, _ = x_ref.shape
    tile = height // n
    nz = n // 2
    last = ni - 1
    c_mid, c_out = w1_ref.shape[3], ws_ref.shape[1]
    kb = n * 4 * ch
    me = lax.axis_index('model')
    my_z, my_c = me // 2, me % 2
    sibling = me + 1 - 2 * my_c

    def core(d, c):
        return ((my_z + d) % nz) * 2 + (my_c + c) % 2

    barrier = pltpu.get_barrier_semaphore()
    for dest in (sibling, core(1, 0), core(1, 1), core(nz - 1, 0), core(nz - 1, 1)):
        pl.semaphore_signal(barrier, inc=1, device_id={'model': dest}, device_id_type=MESH)

    block = tile + 2
    inner, outer = (block - LATE, last), (LATE, ni)

    def part_copy(img, dest, odd, part):
        rows, k = part
        if img < last:
            base, off = dest * tile, 0
        else:
            base = jnp.clip(dest * tile - 2 * (1 - odd), 0, height - block)
            off = (1 - odd) * LATE if part is inner else odd * (block - LATE)
        return (x_ref.at[img, pl.ds(base + off, rows)], xbuf.at[img, me, pl.ds(base + off - dest * tile + 2, rows)], recv_x.at[k])

    def parts_of(img):
        return [(tile, img)] if img < last else [inner, outer]

    def send(img, hops, parts):
        for part in parts:
            for d in hops:
                for c in range(2) if d else (1,):
                    dest = core(d, c)
                    src, dst, sem = part_copy(img, dest, (my_c + c) % 2, part)
                    pltpu.make_async_remote_copy(src_ref=src, dst_ref=dst, send_sem=send_x.at[img // last], recv_sem=sem,
                                                 device_id={'model': dest}, device_id_type=MESH).start()

    def send_weights(hops):
        for d in hops:
            for k, (src, dst) in enumerate(((w1_ref, gw), (ws_ref, gs))):
                pltpu.make_async_remote_copy(
                    src_ref=src, dst_ref=dst.at[my_z, my_c], send_sem=send_w.at[k], recv_sem=recv_w.at[k],
                    device_id={'model': core(d, 0)}, device_id_type=MESH).start()

    def arrived(ref, sem):
        pltpu.make_async_remote_copy(src_ref=ref, dst_ref=ref, send_sem=send_x.at[0], recv_sem=sem,
                                     device_id={'model': sibling}, device_id_type=MESH).wait_recv()

    for img in range(ni):
        for part in parts_of(img):
            src, dst, sem = part_copy(img, me, my_c, part)
            pltpu.make_async_copy(src, dst, sem).start()
    pltpu.make_async_copy(w1_ref, gw.at[my_z, my_c], recv_w.at[0]).start()
    pltpu.make_async_copy(ws_ref, gs.at[my_z, my_c], recv_w.at[1]).start()

    fetches = [pltpu.make_async_copy(src, dst, local.at[k])
               for k, (src, dst) in enumerate(((b1_hbm, b1_ref), (b2_hbm, b2_ref), (w2_hbm, w2_ref)))]
    for fetch in fetches:
        fetch.start()

    pl.semaphore_wait(barrier, 5)
    for d in range(1, nz // 2 + 1):
        if d < nz // 2:
            for side in (1, nz - 1):
                pl.semaphore_signal(phase.at[d - 1], inc=1, device_id={'model': core(side, 0)}, device_id_type=MESH)
        send(0, [d, nz - d] if d < nz // 2 else [d], parts_of(0))
        if d < nz // 2:
            pl.semaphore_wait(phase.at[d - 1], 2)
    send(0, [0], parts_of(0))
    near = [d for k in range(1, nz // 2) for d in (k, nz - k)]
    far = [nz // 2] + near[::-1]
    send_weights(far)
    for img in range(1, last):
        send(img, far + [0], parts_of(img))

    for owner, r0 in ((0, 0), (n - 1, tile + 2)):
        @pl.when(me == owner)
        def _():
            for img in range(ni):
                xbuf[img, :, r0:r0 + 2] = jnp.zeros((n, 2, halves, ch, LANES), xbuf.dtype)

    for fetch in fetches:
        fetch.wait()
    b1c[...] = jnp.broadcast_to(b1_ref[...], (LANES, c_mid)).T
    for t in range(9):
        w2t[:, t * c_mid:(t + 1) * c_mid] = w2_ref[t // 3, t % 3].astype(jnp.float32).T.astype(w2t.dtype)
    wk[...] = jnp.zeros_like(wk)
    sk[...] = jnp.zeros_like(sk)

    def pair(img, p):
        first_pair(n, height, img, p, xbuf, wt, st, b1c, y1s, sbuf)

    def second(img, r):
        y2[img, r] = second_row(r, w2t, b2_ref, y1s, sbuf)

    def build_weights():
        shares = []
        for k, ref in enumerate((gw.at[:, my_c], gs.at[:, my_c])):
            arrived(ref, recv_w.at[k])
            shares.append(pltpu.make_async_remote_copy(
                src_ref=ref, dst_ref=ref, send_sem=send_v.at[k], recv_sem=recv_v.at[k],
                device_id={'model': sibling}, device_id_type=MESH))
            shares[k].start()
        for share in shares:
            share.wait()

        def place(z):
            for c in range(2):
                src = z * 2 + c
                for dh in range(3):
                    for dw in range(3):
                        piece = gw[z, c, dh, dw].astype(jnp.float32)
                        for a in range(2):
                            wk[dw, src, (dh + a) * ch:(dh + a + 1) * ch, a * c_mid:(a + 1) * c_mid] = piece
                piece = gs[z, c].astype(jnp.float32)
                for a in range(2):
                    sk[src, (1 + a) * ch:(2 + a) * ch, a * c_out:(a + 1) * c_out] = piece

        loop(0, nz, place)
        for dw in range(3):
            wt[:, dw * kb:(dw + 1) * kb] = wk[dw].reshape(kb, 2 * c_mid).T.astype(wt.dtype)
        st[...] = sk[...].reshape(kb, 2 * c_out).T.astype(st.dtype)

    def inner_halo(img):
        return pltpu.make_async_remote_copy(
            src_ref=xbuf.at[img, :, pl.ds(2 + (1 - my_c) * (tile - 2), 2)],
            dst_ref=xbuf.at[img, :, pl.ds(my_c * (tile + 2), 2)],
            send_sem=send_h.at[img, 0], recv_sem=recv_h.at[img, 0], device_id={'model': sibling}, device_id_type=MESH)

    def outer_halo(img):
        return pltpu.make_async_remote_copy(
            src_ref=xbuf.at[img, :, pl.ds(2 + my_c * (tile - 2), 2)],
            dst_ref=xbuf.at[img, :, pl.ds((1 - my_c) * (tile + 2), 2)],
            send_sem=send_h.at[img, 1], recv_sem=recv_h.at[img, 1],
            device_id={'model': (me + n - 1 + 2 * my_c) % n}, device_id_type=MESH)

    has_outer = (me != 0) & (me != n - 1)
    sends_last = (me != 1) & (me != n - 2)

    def when(cond, act):
        @pl.when(cond)
        def _():
            act()

    flip = tile // 2

    def pair_in(img, k):
        pair(img, k + my_c * (flip - 2 * k))

    def rows_in(img, lo, hi, unroll):
        loop(lo, hi, lambda k: second(img, k + my_c * (tile - 1 - 2 * k)), unroll=unroll)

    def most(img):
        loop(1, flip - 1, lambda k: pair_in(img, k), unroll=3)
        inner_halo(img).wait_recv()
        loop(flip - 1, flip + 1, lambda k: pair_in(img, k), unroll=2)
        rows_in(img, 2, tile, 7)

    def edge(img):
        when(has_outer, lambda: outer_halo(img).wait_recv())
        pair_in(img, 0)
        rows_in(img, 0, 2, 2)

    for img in range(last):
        arrived(xbuf.at[img, :, pl.ds(0, tile)], recv_x.at[img])
        inner_halo(img).start()
        when(has_outer, lambda: outer_halo(img).start())
        if img == last - 2:
            send(last, far + [0], [inner])
        if img == last - 1:
            send(last, far + [0], [outer] if last > 1 else [inner, outer])
        if img == 0:
            build_weights()
        else:
            edge(img - 1)
        most(img)

    arrived(xbuf.at[last, :, pl.ds(0, block - LATE)], recv_x.at[last])
    when(sends_last, lambda: inner_halo(last).start())
    edge(last - 1)
    first_p = LATE // 2 + 1
    loop(first_p, flip - 1, lambda k: pair_in(last, k), unroll=3)
    when(has_outer, lambda: inner_halo(last).wait_recv())
    loop(flip - 1, flip + 1, lambda k: pair_in(last, k), unroll=2)
    rows_in(last, 2 * first_p, tile, 4)

    for k, sent in enumerate((xbuf.at[pl.ds(0, last), pl.ds(0, n - 1), pl.ds(0, tile)], xbuf.at[last, pl.ds(0, n - 1), pl.ds(0, block)])):
        pltpu.make_async_remote_copy(src_ref=sent, dst_ref=sent, send_sem=send_x.at[k], recv_sem=recv_x.at[0],
                                     device_id={'model': sibling}, device_id_type=MESH).wait_send()
    for k, ref in enumerate((gw.at[pl.ds(0, nz - 1), 0], gs.at[pl.ds(0, nz - 1), 0])):
        pltpu.make_async_remote_copy(src_ref=ref, dst_ref=ref, send_sem=send_w.at[k], recv_sem=recv_w.at[k],
                                     device_id={'model': sibling}, device_id_type=MESH).wait_send()
    for img in range(last):
        inner_halo(img).wait_send()
        when(has_outer, lambda: outer_halo(img).wait_send())
    when(sends_last, lambda: inner_halo(last).wait_send())
    arrived(xbuf.at[last, :, pl.ds(0, LATE)], recv_x.at[ni])


def finish_kernel(n, height, xbuf, wt, st, w2t, b1c, b2_ref, y1s_in, sbuf_in, y2, out_ref, y1s, sbuf, yb, sem):
    ni, tile = y2.shape[0], y2.shape[1]
    last = ni - 1
    my_c = lax.axis_index('model') % 2
    first_p = LATE // 2 + 1
    left = 2 * first_p
    done = tile - left
    ready = (1 - my_c) * left
    todo = my_c * done
    copies = [pltpu.make_async_copy(y2.at[img, pl.ds(r, 4)], out_ref.at[img, pl.ds(r, 4)], sem.at[0])
              for img in range(last) for r in range(0, tile, 4)]
    copies += [pltpu.make_async_copy(y2.at[last, pl.ds(ready, done)], out_ref.at[last, pl.ds(ready, done)], sem.at[1])]
    for copy in copies:
        copy.start()
    step = 3 * b1c.shape[0]
    edge = (1 - my_c) * left + my_c * (tile - left)
    y1s[pl.ds(pl.multiple_of(edge * step, step), 2 * step), :] = y1s_in[pl.ds(pl.multiple_of(edge * step, step), 2 * step), :]
    sbuf[pl.ds(edge, 2)] = sbuf_in[pl.ds(edge, 2)]
    flip = tile // 2
    loop(0, first_p, lambda k: first_pair(n, height, last, k + my_c * (flip - 2 * k), xbuf, wt, st, b1c, y1s, sbuf), unroll=2)

    def row(k):
        yb[k] = second_row(k + todo, w2t, b2_ref, y1s, sbuf)
        pltpu.make_async_copy(yb.at[k], out_ref.at[last, k + todo], sem.at[2]).start()

    loop(0, left, row, unroll=4)
    for copy in copies:
        copy.wait()
    pltpu.make_async_copy(yb, out_ref.at[last, pl.ds(todo, left)], sem.at[2]).wait()


def solution(mesh):
    n = mesh.shape['model']

    def local_step(images, w_conv1, b_conv1, w_conv2, b_conv2, w_short):
        ni, height, width, ch = images.shape
        c_mid, c_out = w_conv1.shape[3], w_short.shape[1]
        tile, halves, nz = height // n, width // LANES, n // 2
        kb = n * 4 * ch
        x = images.transpose(0, 1, 3, 2).reshape(ni, height, ch, halves, LANES).transpose(0, 1, 3, 2, 4)
        vmem = pl.BlockSpec(memory_space=pltpu.VMEM)
        hbm = pl.BlockSpec(memory_space=pltpu.HBM)
        dma = pltpu.SemaphoreType.DMA
        y1s = pltpu.VMEM(((tile + 2) * 3 * c_mid, width), jnp.bfloat16)
        sbuf = pltpu.VMEM((tile + 2, c_out, width), jnp.float32)
        parts = pl.pallas_call(
            functools.partial(gather_kernel, n),
            out_shape=[
                pltpu.VMEM((ni, n, tile + 4, halves, ch, LANES), jnp.bfloat16),
                pltpu.VMEM((2 * c_mid, 3 * kb), jnp.bfloat16),
                pltpu.VMEM((2 * c_out, kb), jnp.bfloat16),
                pltpu.VMEM((c_out, 9 * c_mid), jnp.bfloat16),
                pltpu.VMEM((c_mid, LANES), jnp.float32),
                pltpu.VMEM((1, c_out), jnp.float32),
                y1s,
                sbuf,
                pltpu.VMEM((ni, tile, width, c_out), jnp.float32),
            ],
            in_specs=[hbm] * 6,
            out_specs=[vmem] * 9,
            scratch_shapes=[
                pltpu.VMEM((nz, 2, 3, 3, ch, c_mid), jnp.bfloat16),
                pltpu.VMEM((nz, 2, ch, c_out), jnp.bfloat16),
                pltpu.VMEM((3, n, 4 * ch, 2 * c_mid), jnp.float32),
                pltpu.VMEM((n, 4 * ch, 2 * c_out), jnp.float32),
                pltpu.VMEM(w_conv2.shape, w_conv2.dtype),
                pltpu.VMEM((1, c_mid), jnp.float32),
                dma((3,)), pltpu.SemaphoreType.REGULAR((nz // 2,)),
                dma((2,)), dma((ni + 1,)), dma((ni, 2)), dma((ni, 2)), dma((2,)), dma((2,)), dma((2,)), dma((2,)),
            ],
            compiler_params=pltpu.CompilerParams(collective_id=0, has_side_effects=True, vmem_limit_bytes=20 * 2**20),
        )(*[pltpu.with_memory_space_constraint(v, pltpu.HBM) for v in (x, w_conv1, b_conv1.reshape(1, c_mid), w_conv2, b_conv2.reshape(1, c_out), w_short)])
        return pl.pallas_call(
            functools.partial(finish_kernel, n, height),
            out_shape=jax.ShapeDtypeStruct((ni, tile, width, c_out), jnp.float32),
            in_specs=[vmem] * 9,
            out_specs=hbm,
            scratch_shapes=[y1s, sbuf, pltpu.VMEM((LATE + 2, width, c_out), jnp.float32), dma((3,))],
            compiler_params=pltpu.CompilerParams(vmem_limit_bytes=20 * 2**20),
        )(*parts)

    return jax.shard_map(local_step, mesh=mesh, in_specs=(P('data', None, None, 'model'), P(None, None, 'model', None), P(), P(), P(), P('model', None)), out_specs=P('data', 'model', None, None), check_vma=False)
```

```python
import functools

import jax
import jax.numpy as jnp
from jax import lax
from jax.experimental import pallas as pl
from jax.experimental.pallas import tpu as pltpu
from jax.sharding import PartitionSpec as P

MESH = pl.DeviceIdType.MESH
LANES = 128
LATE = 6


def shift_right(v):
    first = lax.broadcasted_iota(jnp.int32, v.shape, 1) == 0
    return jnp.where(first, jnp.zeros_like(v), pltpu.roll(v, 1, axis=1))


def shift_left(v):
    last = lax.broadcasted_iota(jnp.int32, v.shape, 1) == v.shape[1] - 1
    return jnp.where(last, jnp.zeros_like(v), pltpu.roll(v, v.shape[1] - 1, axis=1))


def first_pair(n, height, img, p, xbuf, wt, b1c, y1s):
    ni, _, rows, halves, ch, _ = xbuf.shape
    tile = rows - 4
    c_mid = wt.shape[0] // 2
    kb = n * 4 * ch
    me = lax.axis_index('model')
    x_left = xbuf[img, :, pl.ds(2 * p, 4), 0]
    x_right = xbuf[img, :, pl.ds(2 * p, 4), 1]
    x0 = jnp.concatenate([x_left.reshape(kb, LANES), x_right.reshape(kb, LANES)], axis=1)
    rhs = jnp.concatenate([shift_right(x0), x0, shift_left(x0)], axis=0)
    z2 = jnp.dot(wt[...], rhs, preferred_element_type=jnp.float32)
    for a in range(2):
        y = jnp.maximum(z2[a * c_mid:(a + 1) * c_mid] + jnp.concatenate([b1c[...]] * halves, axis=1), 0.0)
        row = me * tile - 1 + 2 * p + a
        y = jnp.where((row >= 0) & (row < height), y, 0.0).astype(jnp.bfloat16)
        base = pl.multiple_of((2 * p + a) * 3 * c_mid, c_mid)
        y1s[pl.ds(base, c_mid), :] = shift_right(y)
        y1s[pl.ds(base + c_mid, c_mid), :] = y
        y1s[pl.ds(base + 2 * c_mid, c_mid), :] = shift_left(y)


def second_row(img, r, xbuf, w2x, b2_ref, y1s):
    _, n, _, halves, ch, _ = xbuf.shape
    c_mid = w2x.shape[0]
    base = pl.multiple_of(r * 3 * c_mid, c_mid)
    x_row = jnp.concatenate([xbuf[img, :, r + 2, h].reshape(n * ch, LANES) for h in range(halves)], axis=1)
    rhs = jnp.concatenate([y1s[pl.ds(base, 9 * c_mid), :], x_row], axis=0)
    y2 = jnp.dot(w2x[...], rhs, preferred_element_type=jnp.float32)
    return y2.T + b2_ref[...]


def loop(lo, hi, body, unroll=1):
    def step(i, _):
        body(i)
        return 0

    lax.fori_loop(lo, hi, step, 0, unroll=unroll)


def gather_kernel(n, x_ref, w1_ref, b1_hbm, w2_hbm, b2_hbm, ws_ref,
                  xbuf, wt, w2x, b1c, b2_ref, y1s, y2,
                  gw, gs, wk, w2_ref, b1_ref,
                  local, phase, send_x, recv_x, send_h, recv_h, send_w, recv_w, send_v, recv_v):
    ni, height, halves, ch, _ = x_ref.shape
    tile = height // n
    nz = n // 2
    last = ni - 1
    c_mid, c_out = w1_ref.shape[3], ws_ref.shape[1]
    kb = n * 4 * ch
    me = lax.axis_index('model')
    my_z, my_c = me // 2, me % 2
    sibling = me + 1 - 2 * my_c

    def core(d, c):
        return ((my_z + d) % nz) * 2 + (my_c + c) % 2

    barrier = pltpu.get_barrier_semaphore()
    for dest in (sibling, core(1, 0), core(1, 1), core(nz - 1, 0), core(nz - 1, 1)):
        pl.semaphore_signal(barrier, inc=1, device_id={'model': dest}, device_id_type=MESH)

    block = tile + 2
    inner, outer = (block - LATE, last), (LATE, ni)

    def part_copy(img, dest, odd, part):
        rows, k = part
        if img < last:
            base, off = dest * tile, 0
        else:
            base = jnp.clip(dest * tile - 2 * (1 - odd), 0, height - block)
            off = (1 - odd) * LATE if part is inner else odd * (block - LATE)
        return (x_ref.at[img, pl.ds(base + off, rows)], xbuf.at[img, me, pl.ds(base + off - dest * tile + 2, rows)], recv_x.at[k])

    def parts_of(img):
        return [(tile, img)] if img < last else [inner, outer]

    def send(img, hops, parts):
        for part in parts:
            for d in hops:
                for c in range(2) if d else (1,):
                    dest = core(d, c)
                    src, dst, sem = part_copy(img, dest, (my_c + c) % 2, part)
                    pltpu.make_async_remote_copy(src_ref=src, dst_ref=dst, send_sem=send_x.at[img // last], recv_sem=sem,
                                                 device_id={'model': dest}, device_id_type=MESH).start()

    hubs = [2, nz - 2] if nz >= 8 else [d for d in range(1, nz)]

    own = 0

    def send_weights(moves, k_sem):
        for off, d in moves:
            for k, (src, dst) in enumerate(((w1_ref, gw), (ws_ref, gs))):
                piece = dst.at[(my_z + off) % nz, my_c]
                pltpu.make_async_remote_copy(
                    src_ref=src if off is own else piece, dst_ref=piece, send_sem=send_w.at[k], recv_sem=recv_w.at[k, k_sem],
                    device_id={'model': core(d, 0)}, device_id_type=MESH).start()

    def wait_weights(pieces, k_sem):
        for k, ref in enumerate((gw, gs)):
            arrived(ref.at[pl.ds(0, pieces), my_c], recv_w.at[k, k_sem])

    def arrived(ref, sem):
        pltpu.make_async_remote_copy(src_ref=ref, dst_ref=ref, send_sem=send_x.at[0], recv_sem=sem,
                                     device_id={'model': sibling}, device_id_type=MESH).wait_recv()

    for img in range(ni):
        for part in parts_of(img):
            src, dst, sem = part_copy(img, me, my_c, part)
            pltpu.make_async_copy(src, dst, sem).start()
    pltpu.make_async_copy(w1_ref, gw.at[my_z, my_c], recv_w.at[0, 1]).start()
    pltpu.make_async_copy(ws_ref, gs.at[my_z, my_c], recv_w.at[1, 1]).start()

    fetches = [pltpu.make_async_copy(src, dst, local.at[k])
               for k, (src, dst) in enumerate(((b1_hbm, b1_ref), (b2_hbm, b2_ref), (w2_hbm, w2_ref)))]
    for fetch in fetches:
        fetch.start()

    pl.semaphore_wait(barrier, 5)
    for d in range(1, nz // 2 + 1):
        if d < nz // 2:
            for side in (1, nz - 1):
                pl.semaphore_signal(phase.at[d - 1], inc=1, device_id={'model': core(side, 0)}, device_id_type=MESH)
        send(0, [d, nz - d] if d < nz // 2 else [d], parts_of(0))
        if d < nz // 2:
            pl.semaphore_wait(phase.at[d - 1], 2)
        if d == 1 and nz >= 8:
            send_weights([(own, hub) for hub in hubs], 0)
    send(0, [0], parts_of(0))
    near = [d for k in range(1, nz // 2) for d in (k, nz - k)]
    far = [nz // 2] + near[::-1]
    if nz >= 8:
        wait_weights(2, 0)
        send_weights([(nz - 2, 1), (nz - 2, nz - 1), (2, 1), (2, nz - 1)], 1)
        send_weights([((2 + (nz - 4) * (1 - my_c)), (nz - 2) - (nz - 4) * (1 - my_c))], 1)
    else:
        send_weights([(own, hub) for hub in hubs], 0)
    for img in range(1, last):
        send(img, far + [0], parts_of(img))

    for owner, r0 in ((0, 0), (n - 1, tile + 2)):
        @pl.when(me == owner)
        def _():
            for img in range(ni):
                xbuf[img, :, r0:r0 + 2] = jnp.zeros((n, 2, halves, ch, LANES), xbuf.dtype)

    for fetch in fetches:
        fetch.wait()
    b1c[...] = jnp.broadcast_to(b1_ref[...], (LANES, c_mid)).T
    for t in range(9):
        w2x[:, t * c_mid:(t + 1) * c_mid] = w2_ref[t // 3, t % 3].astype(jnp.float32).T.astype(w2x.dtype)
    wk[...] = jnp.zeros_like(wk)

    def pair(img, p):
        first_pair(n, height, img, p, xbuf, wt, b1c, y1s)

    def second(img, r):
        y2[img, r] = second_row(img, r, xbuf, w2x, b2_ref, y1s)

    def build_weights():
        wait_weights(nz - 2 if nz >= 8 else 1, 1)
        if nz < 8:
            wait_weights(nz - 1, 0)
        shares = []
        for k, ref in enumerate((gw.at[:, my_c], gs.at[:, my_c])):
            shares.append(pltpu.make_async_remote_copy(
                src_ref=ref, dst_ref=ref, send_sem=send_v.at[k], recv_sem=recv_v.at[k],
                device_id={'model': sibling}, device_id_type=MESH))
            shares[k].start()
        for share in shares:
            share.wait()

        def place(z):
            for c in range(2):
                src = z * 2 + c
                for dh in range(3):
                    for dw in range(3):
                        piece = gw[z, c, dh, dw].astype(jnp.float32)
                        for a in range(2):
                            wk[dw, src, (dh + a) * ch:(dh + a + 1) * ch, a * c_mid:(a + 1) * c_mid] = piece

        loop(0, nz, place)
        for dw in range(3):
            wt[:, dw * kb:(dw + 1) * kb] = wk[dw].reshape(kb, 2 * c_mid).T.astype(wt.dtype)
        w2x[:, 9 * c_mid:] = gs[...].astype(jnp.float32).reshape(n * ch, c_out).T.astype(w2x.dtype)

    def inner_halo(img):
        return pltpu.make_async_remote_copy(
            src_ref=xbuf.at[img, :, pl.ds(2 + (1 - my_c) * (tile - 2), 2)],
            dst_ref=xbuf.at[img, :, pl.ds(my_c * (tile + 2), 2)],
            send_sem=send_h.at[img, 0], recv_sem=recv_h.at[img, 0], device_id={'model': sibling}, device_id_type=MESH)

    def outer_halo(img):
        return pltpu.make_async_remote_copy(
            src_ref=xbuf.at[img, :, pl.ds(2 + my_c * (tile - 2), 2)],
            dst_ref=xbuf.at[img, :, pl.ds((1 - my_c) * (tile + 2), 2)],
            send_sem=send_h.at[img, 1], recv_sem=recv_h.at[img, 1],
            device_id={'model': (me + n - 1 + 2 * my_c) % n}, device_id_type=MESH)

    has_outer = (me != 0) & (me != n - 1)
    sends_last = (me != 1) & (me != n - 2)

    def when(cond, act):
        @pl.when(cond)
        def _():
            act()

    flip = tile // 2

    def pair_in(img, k):
        pair(img, k + my_c * (flip - 2 * k))

    def rows_in(img, lo, hi, unroll):
        loop(lo, hi, lambda k: second(img, k + my_c * (tile - 1 - 2 * k)), unroll=unroll)

    def most(img):
        loop(1, flip - 1, lambda k: pair_in(img, k), unroll=3)
        inner_halo(img).wait_recv()
        loop(flip - 1, flip + 1, lambda k: pair_in(img, k), unroll=2)
        rows_in(img, 2, tile, 7)

    def edge(img):
        when(has_outer, lambda: outer_halo(img).wait_recv())
        pair_in(img, 0)
        rows_in(img, 0, 2, 2)

    for img in range(last):
        arrived(xbuf.at[img, :, pl.ds(0, tile)], recv_x.at[img])
        inner_halo(img).start()
        when(has_outer, lambda: outer_halo(img).start())
        if img == last - 2:
            send(last, far + [0], [inner])
        if img == last - 1:
            send(last, far + [0], [outer] if last > 1 else [inner, outer])
        if img == 0:
            build_weights()
        else:
            edge(img - 1)
        most(img)

    arrived(xbuf.at[last, :, pl.ds(0, block - LATE)], recv_x.at[last])
    when(sends_last, lambda: inner_halo(last).start())
    edge(last - 1)
    first_p = LATE // 2 + 1
    loop(first_p, flip - 1, lambda k: pair_in(last, k), unroll=3)
    when(has_outer, lambda: inner_halo(last).wait_recv())
    loop(flip - 1, flip + 1, lambda k: pair_in(last, k), unroll=2)
    rows_in(last, 2 * first_p, tile, 4)

    for k, sent in enumerate((xbuf.at[pl.ds(0, last), pl.ds(0, n - 1), pl.ds(0, tile)], xbuf.at[last, pl.ds(0, n - 1), pl.ds(0, block)])):
        pltpu.make_async_remote_copy(src_ref=sent, dst_ref=sent, send_sem=send_x.at[k], recv_sem=recv_x.at[0],
                                     device_id={'model': sibling}, device_id_type=MESH).wait_send()
    for k, ref in enumerate((gw.at[pl.ds(0, nz - 1), 0], gs.at[pl.ds(0, nz - 1), 0])):
        pltpu.make_async_remote_copy(src_ref=ref, dst_ref=ref, send_sem=send_w.at[k], recv_sem=recv_w.at[k],
                                     device_id={'model': sibling}, device_id_type=MESH).wait_send()
    for img in range(last):
        inner_halo(img).wait_send()
        when(has_outer, lambda: outer_halo(img).wait_send())
    when(sends_last, lambda: inner_halo(last).wait_send())
    arrived(xbuf.at[last, :, pl.ds(0, LATE)], recv_x.at[ni])


def finish_kernel(n, height, xbuf, wt, w2x, b1c, b2_ref, y1s_in, y2, out_ref, y1s, yb, sem):
    ni, tile = y2.shape[0], y2.shape[1]
    last = ni - 1
    my_c = lax.axis_index('model') % 2
    first_p = LATE // 2 + 1
    left = 2 * first_p
    done = tile - left
    ready = (1 - my_c) * left
    todo = my_c * done
    copies = [pltpu.make_async_copy(y2.at[img, pl.ds(r, 4)], out_ref.at[img, pl.ds(r, 4)], sem.at[0])
              for img in range(last) for r in range(0, tile, 4)]
    copies += [pltpu.make_async_copy(y2.at[last, pl.ds(ready, done)], out_ref.at[last, pl.ds(ready, done)], sem.at[1])]
    for copy in copies:
        copy.start()
    step = 3 * b1c.shape[0]
    edge = (1 - my_c) * left + my_c * (tile - left)
    y1s[pl.ds(pl.multiple_of(edge * step, step), 2 * step), :] = y1s_in[pl.ds(pl.multiple_of(edge * step, step), 2 * step), :]
    flip = tile // 2
    loop(0, first_p, lambda k: first_pair(n, height, last, k + my_c * (flip - 2 * k), xbuf, wt, b1c, y1s), unroll=2)

    def row(k):
        yb[k] = second_row(last, k + todo, xbuf, w2x, b2_ref, y1s)
        pltpu.make_async_copy(yb.at[k], out_ref.at[last, k + todo], sem.at[2]).start()

    loop(0, left, row, unroll=4)
    for copy in copies:
        copy.wait()
    pltpu.make_async_copy(yb, out_ref.at[last, pl.ds(todo, left)], sem.at[2]).wait()


def solution(mesh):
    n = mesh.shape['model']

    def local_step(images, w_conv1, b_conv1, w_conv2, b_conv2, w_short):
        ni, height, width, ch = images.shape
        c_mid, c_out = w_conv1.shape[3], w_short.shape[1]
        tile, halves, nz = height // n, width // LANES, n // 2
        kb = n * 4 * ch
        x = images.transpose(0, 1, 3, 2).reshape(ni, height, ch, halves, LANES).transpose(0, 1, 3, 2, 4)
        vmem = pl.BlockSpec(memory_space=pltpu.VMEM)
        hbm = pl.BlockSpec(memory_space=pltpu.HBM)
        dma = pltpu.SemaphoreType.DMA
        y1s = pltpu.VMEM(((tile + 2) * 3 * c_mid, width), jnp.bfloat16)
        parts = pl.pallas_call(
            functools.partial(gather_kernel, n),
            out_shape=[
                pltpu.VMEM((ni, n, tile + 4, halves, ch, LANES), jnp.bfloat16),
                pltpu.VMEM((2 * c_mid, 3 * kb), jnp.bfloat16),
                pltpu.VMEM((c_out, 9 * c_mid + n * ch), jnp.bfloat16),
                pltpu.VMEM((c_mid, LANES), jnp.float32),
                pltpu.VMEM((1, c_out), jnp.float32),
                y1s,
                pltpu.VMEM((ni, tile, width, c_out), jnp.float32),
            ],
            in_specs=[hbm] * 6,
            out_specs=[vmem] * 7,
            scratch_shapes=[
                pltpu.VMEM((nz, 2, 3, 3, ch, c_mid), jnp.bfloat16),
                pltpu.VMEM((nz, 2, ch, c_out), jnp.bfloat16),
                pltpu.VMEM((3, n, 4 * ch, 2 * c_mid), jnp.float32),
                pltpu.VMEM(w_conv2.shape, w_conv2.dtype),
                pltpu.VMEM((1, c_mid), jnp.float32),
                dma((3,)), pltpu.SemaphoreType.REGULAR((nz // 2,)),
                dma((2,)), dma((ni + 1,)), dma((ni, 2)), dma((ni, 2)), dma((2,)), dma((2, 2)), dma((2,)), dma((2,)),
            ],
            compiler_params=pltpu.CompilerParams(collective_id=0, has_side_effects=True, vmem_limit_bytes=20 * 2**20),
        )(*[pltpu.with_memory_space_constraint(v, pltpu.HBM) for v in (x, w_conv1, b_conv1.reshape(1, c_mid), w_conv2, b_conv2.reshape(1, c_out), w_short)])
        return pl.pallas_call(
            functools.partial(finish_kernel, n, height),
            out_shape=jax.ShapeDtypeStruct((ni, tile, width, c_out), jnp.float32),
            in_specs=[vmem] * 7,
            out_specs=hbm,
            scratch_shapes=[y1s, pltpu.VMEM((LATE + 2, width, c_out), jnp.float32), dma((3,))],
            compiler_params=pltpu.CompilerParams(vmem_limit_bytes=20 * 2**20),
        )(*parts)

    return jax.shard_map(local_step, mesh=mesh, in_specs=(P('data', None, None, 'model'), P(None, None, 'model', None), P(), P(), P(), P('model', None)), out_specs=P('data', 'model', None, None), check_vma=False)
```

```python
import functools

import jax
import jax.numpy as jnp
from jax import lax
from jax.experimental import pallas as pl
from jax.experimental.pallas import tpu as pltpu
from jax.sharding import PartitionSpec as P

MESH = pl.DeviceIdType.MESH
LANES = 128
LATE = 6


def shift_right(v):
    first = lax.broadcasted_iota(jnp.int32, v.shape, 1) == 0
    return jnp.where(first, jnp.zeros_like(v), pltpu.roll(v, 1, axis=1))


def shift_left(v):
    last = lax.broadcasted_iota(jnp.int32, v.shape, 1) == v.shape[1] - 1
    return jnp.where(last, jnp.zeros_like(v), pltpu.roll(v, v.shape[1] - 1, axis=1))


def first_pair(n, height, img, p, xbuf, wt, b1c, y1s):
    ni, _, rows, halves, ch, _ = xbuf.shape
    tile = rows - 4
    c_mid = wt.shape[0] // 2
    kb = n * 4 * ch
    me = lax.axis_index('model')
    x_left = xbuf[img, :, pl.ds(2 * p, 4), 0]
    x_right = xbuf[img, :, pl.ds(2 * p, 4), 1]
    x0 = jnp.concatenate([x_left.reshape(kb, LANES), x_right.reshape(kb, LANES)], axis=1)
    rhs = jnp.concatenate([shift_right(x0), x0, shift_left(x0)], axis=0)
    z2 = jnp.dot(wt[...], rhs, preferred_element_type=jnp.float32)
    for a in range(2):
        y = jnp.maximum(z2[a * c_mid:(a + 1) * c_mid] + jnp.concatenate([b1c[...]] * halves, axis=1), 0.0)
        row = me * tile - 1 + 2 * p + a
        y = jnp.where((row >= 0) & (row < height), y, 0.0).astype(jnp.bfloat16)
        base = pl.multiple_of((2 * p + a) * 3 * c_mid, c_mid)
        y1s[pl.ds(base, c_mid), :] = shift_right(y)
        y1s[pl.ds(base + c_mid, c_mid), :] = y
        y1s[pl.ds(base + 2 * c_mid, c_mid), :] = shift_left(y)


def second_row(img, r, xbuf, w2x, b2_ref, y1s):
    _, n, _, halves, ch, _ = xbuf.shape
    c_mid = w2x.shape[0]
    base = pl.multiple_of(r * 3 * c_mid, c_mid)
    x_row = jnp.concatenate([xbuf[img, :, r + 2, h].reshape(n * ch, LANES) for h in range(halves)], axis=1)
    rhs = jnp.concatenate([y1s[pl.ds(base, 9 * c_mid), :], x_row], axis=0)
    y2 = jnp.dot(w2x[...], rhs, preferred_element_type=jnp.float32)
    return y2.T + b2_ref[...]


def loop(lo, hi, body, unroll=1):
    def step(i, _):
        body(i)
        return 0

    lax.fori_loop(lo, hi, step, 0, unroll=unroll)


def gather_kernel(n, x_ref, w1_ref, b1_hbm, w2_hbm, b2_hbm, ws_ref,
                  xbuf, wt, w2x, b1c, b2_ref, y1s, y2,
                  gw, gs, wk, w2_ref, b1_ref,
                  local, phase, send_x, recv_x, send_h, recv_h, send_w, recv_w, send_v, recv_v):
    ni, height, halves, ch, _ = x_ref.shape
    tile = height // n
    nz = n // 2
    last = ni - 1
    assert last == 2
    c_mid, c_out = w1_ref.shape[3], ws_ref.shape[1]
    kb = n * 4 * ch
    me = lax.axis_index('model')
    my_z, my_c = me // 2, me % 2
    sibling = me + 1 - 2 * my_c

    def core(d, c):
        return ((my_z + d) % nz) * 2 + (my_c + c) % 2

    barrier = pltpu.get_barrier_semaphore()
    for dest in (sibling, core(1, 0), core(1, 1), core(nz - 1, 0), core(nz - 1, 1)):
        pl.semaphore_signal(barrier, inc=1, device_id={'model': dest}, device_id_type=MESH)

    block = tile + 2
    inner, outer = (block - LATE, last), (LATE, ni)

    def part_copy(img, dest, odd, part):
        rows, k = part
        if img < last:
            base, off = dest * tile, 0
        else:
            base = jnp.clip(dest * tile - 2 * (1 - odd), 0, height - block)
            off = (1 - odd) * LATE if part is inner else odd * (block - LATE)
        return (x_ref.at[img, pl.ds(base + off, rows)], xbuf.at[img, me, pl.ds(base + off - dest * tile + 2, rows)], recv_x.at[k])

    def parts_of(img):
        return [(tile, img)] if img < last else [inner, outer]

    def send(img, hops, part, batch):
        for d in hops:
            for c in range(2) if d else (1,):
                dest = core(d, c)
                src, dst, sem = part_copy(img, dest, (my_c + c) % 2, part)
                pltpu.make_async_remote_copy(src_ref=src, dst_ref=dst, send_sem=send_x.at[batch], recv_sem=sem,
                                             device_id={'model': dest}, device_id_type=MESH).start()

    def left(batch, copies, rows):
        ref = xbuf.at[0, pl.ds(0, copies), pl.ds(0, rows)]
        pltpu.make_async_remote_copy(src_ref=ref, dst_ref=ref, send_sem=send_x.at[batch], recv_sem=recv_x.at[0],
                                     device_id={'model': sibling}, device_id_type=MESH).wait_send()

    hubs = [2, nz - 2] if nz >= 8 else [d for d in range(1, nz)]

    own = 0

    def send_weights(moves, k_sem):
        for off, d in moves:
            for k, (src, dst) in enumerate(((w1_ref, gw), (ws_ref, gs))):
                piece = dst.at[(my_z + off) % nz, my_c]
                pltpu.make_async_remote_copy(
                    src_ref=src if off is own else piece, dst_ref=piece, send_sem=send_w.at[k], recv_sem=recv_w.at[k, k_sem],
                    device_id={'model': core(d, 0)}, device_id_type=MESH).start()

    def wait_weights(pieces, k_sem):
        for k, ref in enumerate((gw, gs)):
            arrived(ref.at[pl.ds(0, pieces), my_c], recv_w.at[k, k_sem])

    def arrived(ref, sem):
        pltpu.make_async_remote_copy(src_ref=ref, dst_ref=ref, send_sem=send_x.at[0], recv_sem=sem,
                                     device_id={'model': sibling}, device_id_type=MESH).wait_recv()

    for img in range(ni):
        for part in parts_of(img):
            src, dst, sem = part_copy(img, me, my_c, part)
            pltpu.make_async_copy(src, dst, sem).start()
    pltpu.make_async_copy(w1_ref, gw.at[my_z, my_c], recv_w.at[0, 1]).start()
    pltpu.make_async_copy(ws_ref, gs.at[my_z, my_c], recv_w.at[1, 1]).start()

    fetches = [pltpu.make_async_copy(src, dst, local.at[k])
               for k, (src, dst) in enumerate(((b1_hbm, b1_ref), (b2_hbm, b2_ref), (w2_hbm, w2_ref)))]
    for fetch in fetches:
        fetch.start()

    pl.semaphore_wait(barrier, 5)
    for d in range(1, nz // 2 + 1):
        if d < nz // 2:
            for side in (1, nz - 1):
                pl.semaphore_signal(phase.at[d - 1], inc=1, device_id={'model': core(side, 0)}, device_id_type=MESH)
        send(0, [d, nz - d] if d < nz // 2 else [d], parts_of(0)[0], 0 if d <= nz // 4 else 1)
        if d < nz // 2:
            pl.semaphore_wait(phase.at[d - 1], 2)
        if d == 1 and nz >= 8:
            send_weights([(own, hub) for hub in hubs], 0)
    send(0, [0], parts_of(0)[0], 1)
    near = [d for k in range(1, nz // 2) for d in (k, nz - k)]
    far = [nz // 2] + near[::-1]
    if nz >= 8:
        wait_weights(2, 0)
        send_weights([(nz - 2, 1), (nz - 2, nz - 1), (2, 1), (2, nz - 1)], 1)
        send_weights([((2 + (nz - 4) * (1 - my_c)), (nz - 2) - (nz - 4) * (1 - my_c))], 1)
    else:
        send_weights([(own, hub) for hub in hubs], 0)
    near_copies = 4 * (nz // 4)
    first, rest = far[:3], far[3:] + [0]
    left(0, near_copies, tile)
    send(1, first, parts_of(1)[0], 2)

    for owner, r0 in ((0, 0), (n - 1, tile + 2)):
        @pl.when(me == owner)
        def _():
            for img in range(ni):
                xbuf[img, :, r0:r0 + 2] = jnp.zeros((n, 2, halves, ch, LANES), xbuf.dtype)

    for fetch in fetches:
        fetch.wait()
    b1c[...] = jnp.broadcast_to(b1_ref[...], (LANES, c_mid)).T
    for t in range(9):
        w2x[:, t * c_mid:(t + 1) * c_mid] = w2_ref[t // 3, t % 3].astype(jnp.float32).T.astype(w2x.dtype)
    wk[...] = jnp.zeros_like(wk)
    left(1, n - 1 - near_copies, tile)
    send(1, rest, parts_of(1)[0], 3)

    def pair(img, p):
        first_pair(n, height, img, p, xbuf, wt, b1c, y1s)

    def second(img, r):
        y2[img, r] = second_row(img, r, xbuf, w2x, b2_ref, y1s)

    def build_weights():
        wait_weights(nz - 2 if nz >= 8 else 1, 1)
        if nz < 8:
            wait_weights(nz - 1, 0)
        shares = []
        for k, ref in enumerate((gw.at[:, my_c], gs.at[:, my_c])):
            shares.append(pltpu.make_async_remote_copy(
                src_ref=ref, dst_ref=ref, send_sem=send_v.at[k], recv_sem=recv_v.at[k],
                device_id={'model': sibling}, device_id_type=MESH))
            shares[k].start()
        for share in shares:
            share.wait()

        def place(z):
            for c in range(2):
                src = z * 2 + c
                for dh in range(3):
                    for dw in range(3):
                        piece = gw[z, c, dh, dw].astype(jnp.float32)
                        for a in range(2):
                            wk[dw, src, (dh + a) * ch:(dh + a + 1) * ch, a * c_mid:(a + 1) * c_mid] = piece

        loop(0, nz, place)
        for dw in range(3):
            wt[:, dw * kb:(dw + 1) * kb] = wk[dw].reshape(kb, 2 * c_mid).T.astype(wt.dtype)
        w2x[:, 9 * c_mid:] = gs[...].astype(jnp.float32).reshape(n * ch, c_out).T.astype(w2x.dtype)

    def inner_halo(img):
        return pltpu.make_async_remote_copy(
            src_ref=xbuf.at[img, :, pl.ds(2 + (1 - my_c) * (tile - 2), 2)],
            dst_ref=xbuf.at[img, :, pl.ds(my_c * (tile + 2), 2)],
            send_sem=send_h.at[img, 0], recv_sem=recv_h.at[img, 0], device_id={'model': sibling}, device_id_type=MESH)

    def outer_halo(img):
        return pltpu.make_async_remote_copy(
            src_ref=xbuf.at[img, :, pl.ds(2 + my_c * (tile - 2), 2)],
            dst_ref=xbuf.at[img, :, pl.ds((1 - my_c) * (tile + 2), 2)],
            send_sem=send_h.at[img, 1], recv_sem=recv_h.at[img, 1],
            device_id={'model': (me + n - 1 + 2 * my_c) % n}, device_id_type=MESH)

    has_outer = (me != 0) & (me != n - 1)
    sends_last = (me != 1) & (me != n - 2)

    def when(cond, act):
        @pl.when(cond)
        def _():
            act()

    flip = tile // 2

    def pair_in(img, k):
        pair(img, k + my_c * (flip - 2 * k))

    def rows_in(img, lo, hi, unroll):
        loop(lo, hi, lambda k: second(img, k + my_c * (tile - 1 - 2 * k)), unroll=unroll)

    def most(img, between):
        loop(1, flip - 1, lambda k: pair_in(img, k), unroll=3)
        inner_halo(img).wait_recv()
        loop(flip - 1, flip + 1, lambda k: pair_in(img, k), unroll=2)
        between()
        rows_in(img, 2, tile, 7)

    def edge(img):
        when(has_outer, lambda: outer_halo(img).wait_recv())
        pair_in(img, 0)
        rows_in(img, 0, 2, 2)

    def begin(img):
        arrived(xbuf.at[img, :, pl.ds(0, tile)], recv_x.at[img])
        inner_halo(img).start()
        when(has_outer, lambda: outer_halo(img).start())

    begin(0)
    build_weights()
    most(0, lambda: None)
    left(2, 6, tile)
    send(last, first, inner, 4)
    begin(1)
    send(last, rest, inner, 5)
    edge(0)

    def last_sends():
        left(4, 6, block - LATE)
        send(last, far + [0], outer, 6)

    most(1, last_sends)
    arrived(xbuf.at[last, :, pl.ds(0, block - LATE)], recv_x.at[last])
    when(sends_last, lambda: inner_halo(last).start())
    edge(last - 1)
    first_p = LATE // 2 + 1
    loop(first_p, flip - 1, lambda k: pair_in(last, k), unroll=3)
    when(has_outer, lambda: inner_halo(last).wait_recv())
    loop(flip - 1, flip + 1, lambda k: pair_in(last, k), unroll=2)
    rows_in(last, 2 * first_p, tile, 4)

    left(3, n - 7, tile)
    left(5, n - 7, block - LATE)
    left(6, n - 1, LATE)
    for k, ref in enumerate((gw.at[pl.ds(0, nz - 1), 0], gs.at[pl.ds(0, nz - 1), 0])):
        pltpu.make_async_remote_copy(src_ref=ref, dst_ref=ref, send_sem=send_w.at[k], recv_sem=recv_w.at[k],
                                     device_id={'model': sibling}, device_id_type=MESH).wait_send()
    for img in range(last):
        inner_halo(img).wait_send()
        when(has_outer, lambda: outer_halo(img).wait_send())
    when(sends_last, lambda: inner_halo(last).wait_send())
    arrived(xbuf.at[last, :, pl.ds(0, LATE)], recv_x.at[ni])


def finish_kernel(n, height, xbuf, wt, w2x, b1c, b2_ref, y1s_in, y2, out_ref, y1s, yb, sem):
    ni, tile = y2.shape[0], y2.shape[1]
    last = ni - 1
    my_c = lax.axis_index('model') % 2
    first_p = LATE // 2 + 1
    left = 2 * first_p
    done = tile - left
    ready = (1 - my_c) * left
    todo = my_c * done
    copies = [pltpu.make_async_copy(y2.at[img, pl.ds(r, 4)], out_ref.at[img, pl.ds(r, 4)], sem.at[0])
              for img in range(last) for r in range(0, tile, 4)]
    copies += [pltpu.make_async_copy(y2.at[last, pl.ds(ready, done)], out_ref.at[last, pl.ds(ready, done)], sem.at[1])]
    for copy in copies:
        copy.start()
    step = 3 * b1c.shape[0]
    edge = (1 - my_c) * left + my_c * (tile - left)
    y1s[pl.ds(pl.multiple_of(edge * step, step), 2 * step), :] = y1s_in[pl.ds(pl.multiple_of(edge * step, step), 2 * step), :]
    flip = tile // 2
    loop(0, first_p, lambda k: first_pair(n, height, last, k + my_c * (flip - 2 * k), xbuf, wt, b1c, y1s), unroll=2)

    def row(k):
        yb[k] = second_row(last, k + todo, xbuf, w2x, b2_ref, y1s)
        pltpu.make_async_copy(yb.at[k], out_ref.at[last, k + todo], sem.at[2]).start()

    loop(0, left, row, unroll=4)
    for copy in copies:
        copy.wait()
    pltpu.make_async_copy(yb, out_ref.at[last, pl.ds(todo, left)], sem.at[2]).wait()


def solution(mesh):
    n = mesh.shape['model']

    def local_step(images, w_conv1, b_conv1, w_conv2, b_conv2, w_short):
        ni, height, width, ch = images.shape
        c_mid, c_out = w_conv1.shape[3], w_short.shape[1]
        tile, halves, nz = height // n, width // LANES, n // 2
        kb = n * 4 * ch
        x = images.transpose(0, 1, 3, 2).reshape(ni, height, ch, halves, LANES).transpose(0, 1, 3, 2, 4)
        vmem = pl.BlockSpec(memory_space=pltpu.VMEM)
        hbm = pl.BlockSpec(memory_space=pltpu.HBM)
        dma = pltpu.SemaphoreType.DMA
        y1s = pltpu.VMEM(((tile + 2) * 3 * c_mid, width), jnp.bfloat16)
        parts = pl.pallas_call(
            functools.partial(gather_kernel, n),
            out_shape=[
                pltpu.VMEM((ni, n, tile + 4, halves, ch, LANES), jnp.bfloat16),
                pltpu.VMEM((2 * c_mid, 3 * kb), jnp.bfloat16),
                pltpu.VMEM((c_out, 9 * c_mid + n * ch), jnp.bfloat16),
                pltpu.VMEM((c_mid, LANES), jnp.float32),
                pltpu.VMEM((1, c_out), jnp.float32),
                y1s,
                pltpu.VMEM((ni, tile, width, c_out), jnp.float32),
            ],
            in_specs=[hbm] * 6,
            out_specs=[vmem] * 7,
            scratch_shapes=[
                pltpu.VMEM((nz, 2, 3, 3, ch, c_mid), jnp.bfloat16),
                pltpu.VMEM((nz, 2, ch, c_out), jnp.bfloat16),
                pltpu.VMEM((3, n, 4 * ch, 2 * c_mid), jnp.float32),
                pltpu.VMEM(w_conv2.shape, w_conv2.dtype),
                pltpu.VMEM((1, c_mid), jnp.float32),
                dma((3,)), pltpu.SemaphoreType.REGULAR((nz // 2,)),
                dma((7,)), dma((ni + 1,)), dma((ni, 2)), dma((ni, 2)), dma((2,)), dma((2, 2)), dma((2,)), dma((2,)),
            ],
            compiler_params=pltpu.CompilerParams(collective_id=0, has_side_effects=True, vmem_limit_bytes=20 * 2**20),
        )(*[pltpu.with_memory_space_constraint(v, pltpu.HBM) for v in (x, w_conv1, b_conv1.reshape(1, c_mid), w_conv2, b_conv2.reshape(1, c_out), w_short)])
        return pl.pallas_call(
            functools.partial(finish_kernel, n, height),
            out_shape=jax.ShapeDtypeStruct((ni, tile, width, c_out), jnp.float32),
            in_specs=[vmem] * 7,
            out_specs=hbm,
            scratch_shapes=[y1s, pltpu.VMEM((LATE + 2, width, c_out), jnp.float32), dma((3,))],
            compiler_params=pltpu.CompilerParams(vmem_limit_bytes=20 * 2**20),
        )(*parts)

    return jax.shard_map(local_step, mesh=mesh, in_specs=(P('data', None, None, 'model'), P(None, None, 'model', None), P(), P(), P(), P('model', None)), out_specs=P('data', 'model', None, None), check_vma=False)
```

```python
import functools

import jax
import jax.numpy as jnp
from jax import lax
from jax.experimental import pallas as pl
from jax.experimental.pallas import tpu as pltpu
from jax.sharding import PartitionSpec as P

MESH = pl.DeviceIdType.MESH
LANES = 128
LATE = 4


def shift_right(v):
    first = lax.broadcasted_iota(jnp.int32, v.shape, 1) == 0
    return jnp.where(first, jnp.zeros_like(v), pltpu.roll(v, 1, axis=1))


def shift_left(v):
    last = lax.broadcasted_iota(jnp.int32, v.shape, 1) == v.shape[1] - 1
    return jnp.where(last, jnp.zeros_like(v), pltpu.roll(v, v.shape[1] - 1, axis=1))


def first_pair(n, height, img, p, xbuf, wt, b1c, y1s):
    ni, _, rows, halves, ch, _ = xbuf.shape
    tile = rows - 4
    c_mid = wt.shape[0] // 2
    kb = n * 4 * ch
    me = lax.axis_index('model')
    x_left = xbuf[img, :, pl.ds(2 * p, 4), 0]
    x_right = xbuf[img, :, pl.ds(2 * p, 4), 1]
    x0 = jnp.concatenate([x_left.reshape(kb, LANES), x_right.reshape(kb, LANES)], axis=1)
    rhs = jnp.concatenate([shift_right(x0), x0, shift_left(x0)], axis=0)
    z2 = jnp.dot(wt[...], rhs, preferred_element_type=jnp.float32)
    for a in range(2):
        y = jnp.maximum(z2[a * c_mid:(a + 1) * c_mid] + jnp.concatenate([b1c[...]] * halves, axis=1), 0.0)
        row = me * tile - 1 + 2 * p + a
        y = jnp.where((row >= 0) & (row < height), y, 0.0).astype(jnp.bfloat16)
        base = pl.multiple_of((2 * p + a) * 3 * c_mid, c_mid)
        y1s[pl.ds(base, c_mid), :] = shift_right(y)
        y1s[pl.ds(base + c_mid, c_mid), :] = y
        y1s[pl.ds(base + 2 * c_mid, c_mid), :] = shift_left(y)


def second_row(img, r, xbuf, w2x, b2_ref, y1s):
    _, n, _, halves, ch, _ = xbuf.shape
    c_mid = w2x.shape[0]
    base = pl.multiple_of(r * 3 * c_mid, c_mid)
    x_row = jnp.concatenate([xbuf[img, :, r + 2, h].reshape(n * ch, LANES) for h in range(halves)], axis=1)
    rhs = jnp.concatenate([y1s[pl.ds(base, 9 * c_mid), :], x_row], axis=0)
    y2 = jnp.dot(w2x[...], rhs, preferred_element_type=jnp.float32)
    return y2.T + b2_ref[...]


def loop(lo, hi, body, unroll=1):
    def step(i, _):
        body(i)
        return 0

    lax.fori_loop(lo, hi, step, 0, unroll=unroll)


def gather_kernel(n, x_ref, w1_ref, b1_hbm, w2_hbm, b2_hbm, ws_ref,
                  xbuf, wt, w2x, b1c, b2_ref, y1s, y2,
                  gw, gs, wk, w2_ref, b1_ref,
                  local, phase, send_x, recv_x, send_h, recv_h, send_w, recv_w, send_v, recv_v):
    ni, height, halves, ch, _ = x_ref.shape
    tile = height // n
    nz = n // 2
    last = ni - 1
    assert last == 2
    c_mid, c_out = w1_ref.shape[3], ws_ref.shape[1]
    kb = n * 4 * ch
    me = lax.axis_index('model')
    my_z, my_c = me // 2, me % 2
    sibling = me + 1 - 2 * my_c

    def core(d, c):
        return ((my_z + d) % nz) * 2 + (my_c + c) % 2

    barrier = pltpu.get_barrier_semaphore()
    for dest in (sibling, core(1, 0), core(1, 1), core(nz - 1, 0), core(nz - 1, 1)):
        pl.semaphore_signal(barrier, inc=1, device_id={'model': dest}, device_id_type=MESH)

    block = tile + 2
    inner, outer = (block - LATE, last), (LATE, ni)

    def part_copy(img, dest, odd, part):
        rows, k = part
        if img < last:
            base, off = dest * tile, 0
        else:
            base = jnp.clip(dest * tile - 2 * (1 - odd), 0, height - block)
            off = (1 - odd) * LATE if part is inner else odd * (block - LATE)
        return (x_ref.at[img, pl.ds(base + off, rows)], xbuf.at[img, me, pl.ds(base + off - dest * tile + 2, rows)], recv_x.at[k])

    def parts_of(img):
        return [(tile, img)] if img < last else [inner, outer]

    def send(img, hops, part, batch):
        for d in hops:
            for c in range(2) if d else (1,):
                dest = core(d, c)
                src, dst, sem = part_copy(img, dest, (my_c + c) % 2, part)
                pltpu.make_async_remote_copy(src_ref=src, dst_ref=dst, send_sem=send_x.at[batch], recv_sem=sem,
                                             device_id={'model': dest}, device_id_type=MESH).start()

    def left(batch, copies, rows):
        ref = xbuf.at[0, pl.ds(0, copies), pl.ds(0, rows)]
        pltpu.make_async_remote_copy(src_ref=ref, dst_ref=ref, send_sem=send_x.at[batch], recv_sem=recv_x.at[0],
                                     device_id={'model': sibling}, device_id_type=MESH).wait_send()

    hubs = [2, nz - 2] if nz >= 8 else [d for d in range(1, nz)]

    own = 0

    def send_weights(moves, k_sem):
        for off, d in moves:
            for k, (src, dst) in enumerate(((w1_ref, gw), (ws_ref, gs))):
                piece = dst.at[(my_z + off) % nz, my_c]
                pltpu.make_async_remote_copy(
                    src_ref=src if off is own else piece, dst_ref=piece, send_sem=send_w.at[k], recv_sem=recv_w.at[k, k_sem],
                    device_id={'model': core(d, 0)}, device_id_type=MESH).start()

    def wait_weights(pieces, k_sem):
        for k, ref in enumerate((gw, gs)):
            arrived(ref.at[pl.ds(0, pieces), my_c], recv_w.at[k, k_sem])

    def arrived(ref, sem):
        pltpu.make_async_remote_copy(src_ref=ref, dst_ref=ref, send_sem=send_x.at[0], recv_sem=sem,
                                     device_id={'model': sibling}, device_id_type=MESH).wait_recv()

    for img in range(ni):
        for part in parts_of(img):
            src, dst, sem = part_copy(img, me, my_c, part)
            pltpu.make_async_copy(src, dst, sem).start()
    pltpu.make_async_copy(w1_ref, gw.at[my_z, my_c], recv_w.at[0, 1]).start()
    pltpu.make_async_copy(ws_ref, gs.at[my_z, my_c], recv_w.at[1, 1]).start()

    fetches = [pltpu.make_async_copy(src, dst, local.at[k])
               for k, (src, dst) in enumerate(((b1_hbm, b1_ref), (b2_hbm, b2_ref), (w2_hbm, w2_ref)))]
    for fetch in fetches:
        fetch.start()

    pl.semaphore_wait(barrier, 5)
    for d in range(1, nz // 2 + 1):
        if d < nz // 2:
            for side in (1, nz - 1):
                pl.semaphore_signal(phase.at[d - 1], inc=1, device_id={'model': core(side, 0)}, device_id_type=MESH)
        send(0, [d, nz - d] if d < nz // 2 else [d], parts_of(0)[0], 0 if d <= nz // 4 else 1)
        if d < nz // 2:
            pl.semaphore_wait(phase.at[d - 1], 2)
        if d == 1 and nz >= 8:
            send_weights([(own, hub) for hub in hubs], 0)
    send(0, [0], parts_of(0)[0], 1)
    near = [d for k in range(1, nz // 2) for d in (k, nz - k)]
    far = [nz // 2] + near[::-1]
    if nz >= 8:
        wait_weights(2, 0)
        send_weights([(nz - 2, 1), (nz - 2, nz - 1), (2, 1), (2, nz - 1)], 1)
        send_weights([((2 + (nz - 4) * (1 - my_c)), (nz - 2) - (nz - 4) * (1 - my_c))], 1)
    else:
        send_weights([(own, hub) for hub in hubs], 0)
    near_copies = 4 * (nz // 4)
    first, rest = far[:3], far[3:] + [0]
    left(0, near_copies, tile)
    send(1, first, parts_of(1)[0], 2)

    for owner, r0 in ((0, 0), (n - 1, tile + 2)):
        @pl.when(me == owner)
        def _():
            for img in range(ni):
                xbuf[img, :, r0:r0 + 2] = jnp.zeros((n, 2, halves, ch, LANES), xbuf.dtype)

    for fetch in fetches:
        fetch.wait()
    b1c[...] = jnp.broadcast_to(b1_ref[...], (LANES, c_mid)).T
    for t in range(9):
        w2x[:, t * c_mid:(t + 1) * c_mid] = w2_ref[t // 3, t % 3].astype(jnp.float32).T.astype(w2x.dtype)
    wk[...] = jnp.zeros_like(wk)
    left(1, n - 1 - near_copies, tile)
    send(1, rest, parts_of(1)[0], 3)

    def pair(img, p):
        first_pair(n, height, img, p, xbuf, wt, b1c, y1s)

    def second(img, r):
        y2[img, r] = second_row(img, r, xbuf, w2x, b2_ref, y1s)

    def build_weights():
        wait_weights(nz - 2 if nz >= 8 else 1, 1)
        if nz < 8:
            wait_weights(nz - 1, 0)
        shares = []
        for k, ref in enumerate((gw.at[:, my_c], gs.at[:, my_c])):
            shares.append(pltpu.make_async_remote_copy(
                src_ref=ref, dst_ref=ref, send_sem=send_v.at[k], recv_sem=recv_v.at[k],
                device_id={'model': sibling}, device_id_type=MESH))
            shares[k].start()
        for share in shares:
            share.wait()

        def place(z):
            for c in range(2):
                src = z * 2 + c
                for dh in range(3):
                    for dw in range(3):
                        piece = gw[z, c, dh, dw].astype(jnp.float32)
                        for a in range(2):
                            wk[dw, src, (dh + a) * ch:(dh + a + 1) * ch, a * c_mid:(a + 1) * c_mid] = piece

        loop(0, nz, place)
        for dw in range(3):
            wt[:, dw * kb:(dw + 1) * kb] = wk[dw].reshape(kb, 2 * c_mid).T.astype(wt.dtype)
        w2x[:, 9 * c_mid:] = gs[...].astype(jnp.float32).reshape(n * ch, c_out).T.astype(w2x.dtype)

    def inner_halo(img):
        return pltpu.make_async_remote_copy(
            src_ref=xbuf.at[img, :, pl.ds(2 + (1 - my_c) * (tile - 2), 2)],
            dst_ref=xbuf.at[img, :, pl.ds(my_c * (tile + 2), 2)],
            send_sem=send_h.at[img, 0], recv_sem=recv_h.at[img, 0], device_id={'model': sibling}, device_id_type=MESH)

    def outer_halo(img):
        return pltpu.make_async_remote_copy(
            src_ref=xbuf.at[img, :, pl.ds(2 + my_c * (tile - 2), 2)],
            dst_ref=xbuf.at[img, :, pl.ds((1 - my_c) * (tile + 2), 2)],
            send_sem=send_h.at[img, 1], recv_sem=recv_h.at[img, 1],
            device_id={'model': (me + n - 1 + 2 * my_c) % n}, device_id_type=MESH)

    has_outer = (me != 0) & (me != n - 1)
    sends_last = (me != 1) & (me != n - 2)

    def when(cond, act):
        @pl.when(cond)
        def _():
            act()

    flip = tile // 2

    def pair_in(img, k):
        pair(img, k + my_c * (flip - 2 * k))

    def rows_in(img, lo, hi, unroll):
        loop(lo, hi, lambda k: second(img, k + my_c * (tile - 1 - 2 * k)), unroll=unroll)

    def most(img, between):
        loop(1, flip - 1, lambda k: pair_in(img, k), unroll=3)
        inner_halo(img).wait_recv()
        loop(flip - 1, flip + 1, lambda k: pair_in(img, k), unroll=2)
        between()
        rows_in(img, 2, tile, 7)

    def edge(img):
        when(has_outer, lambda: outer_halo(img).wait_recv())
        pair_in(img, 0)
        rows_in(img, 0, 2, 2)

    def begin(img):
        arrived(xbuf.at[img, :, pl.ds(0, tile)], recv_x.at[img])
        inner_halo(img).start()
        when(has_outer, lambda: outer_halo(img).start())

    begin(0)
    build_weights()
    most(0, lambda: None)
    left(2, 6, tile)
    send(last, first, inner, 4)
    begin(1)
    send(last, rest, inner, 5)
    edge(0)

    def last_sends():
        left(4, 6, block - LATE)
        send(last, far + [0], outer, 6)

    most(1, last_sends)
    arrived(xbuf.at[last, :, pl.ds(0, block - LATE)], recv_x.at[last])
    when(sends_last, lambda: inner_halo(last).start())
    edge(last - 1)
    first_p = LATE // 2 + 1
    loop(first_p, flip - 1, lambda k: pair_in(last, k), unroll=2)
    when(has_outer, lambda: inner_halo(last).wait_recv())
    loop(flip - 1, flip + 1, lambda k: pair_in(last, k), unroll=2)
    rows_in(last, 2 * first_p, tile, 5)

    left(3, n - 7, tile)
    left(5, n - 7, block - LATE)
    left(6, n - 1, LATE)
    for k, ref in enumerate((gw.at[pl.ds(0, nz - 1), 0], gs.at[pl.ds(0, nz - 1), 0])):
        pltpu.make_async_remote_copy(src_ref=ref, dst_ref=ref, send_sem=send_w.at[k], recv_sem=recv_w.at[k],
                                     device_id={'model': sibling}, device_id_type=MESH).wait_send()
    for img in range(last):
        inner_halo(img).wait_send()
        when(has_outer, lambda: outer_halo(img).wait_send())
    when(sends_last, lambda: inner_halo(last).wait_send())
    arrived(xbuf.at[last, :, pl.ds(0, LATE)], recv_x.at[ni])


def finish_kernel(n, height, xbuf, wt, w2x, b1c, b2_ref, y1s_in, y2, out_ref, y1s, yb, sem):
    ni, tile = y2.shape[0], y2.shape[1]
    last = ni - 1
    my_c = lax.axis_index('model') % 2
    first_p = LATE // 2 + 1
    left = 2 * first_p
    done = tile - left
    ready = (1 - my_c) * left
    todo = my_c * done
    copies = [pltpu.make_async_copy(y2.at[img, pl.ds(r, 4)], out_ref.at[img, pl.ds(r, 4)], sem.at[0])
              for img in range(last) for r in range(0, tile, 4)]
    copies += [pltpu.make_async_copy(y2.at[last, pl.ds(ready, done)], out_ref.at[last, pl.ds(ready, done)], sem.at[1])]
    for copy in copies:
        copy.start()
    step = 3 * b1c.shape[0]
    edge = (1 - my_c) * left + my_c * (tile - left)
    y1s[pl.ds(pl.multiple_of(edge * step, step), 2 * step), :] = y1s_in[pl.ds(pl.multiple_of(edge * step, step), 2 * step), :]
    flip = tile // 2
    loop(0, first_p, lambda k: first_pair(n, height, last, k + my_c * (flip - 2 * k), xbuf, wt, b1c, y1s), unroll=3)

    def row(k):
        yb[k] = second_row(last, k + todo, xbuf, w2x, b2_ref, y1s)
        pltpu.make_async_copy(yb.at[k], out_ref.at[last, k + todo], sem.at[2]).start()

    loop(0, left, row, unroll=3)
    for copy in copies:
        copy.wait()
    pltpu.make_async_copy(yb, out_ref.at[last, pl.ds(todo, left)], sem.at[2]).wait()


def solution(mesh):
    n = mesh.shape['model']

    def local_step(images, w_conv1, b_conv1, w_conv2, b_conv2, w_short):
        ni, height, width, ch = images.shape
        c_mid, c_out = w_conv1.shape[3], w_short.shape[1]
        tile, halves, nz = height // n, width // LANES, n // 2
        kb = n * 4 * ch
        x = images.transpose(0, 1, 3, 2).reshape(ni, height, ch, halves, LANES).transpose(0, 1, 3, 2, 4)
        vmem = pl.BlockSpec(memory_space=pltpu.VMEM)
        hbm = pl.BlockSpec(memory_space=pltpu.HBM)
        dma = pltpu.SemaphoreType.DMA
        y1s = pltpu.VMEM(((tile + 2) * 3 * c_mid, width), jnp.bfloat16)
        parts = pl.pallas_call(
            functools.partial(gather_kernel, n),
            out_shape=[
                pltpu.VMEM((ni, n, tile + 4, halves, ch, LANES), jnp.bfloat16),
                pltpu.VMEM((2 * c_mid, 3 * kb), jnp.bfloat16),
                pltpu.VMEM((c_out, 9 * c_mid + n * ch), jnp.bfloat16),
                pltpu.VMEM((c_mid, LANES), jnp.float32),
                pltpu.VMEM((1, c_out), jnp.float32),
                y1s,
                pltpu.VMEM((ni, tile, width, c_out), jnp.float32),
            ],
            in_specs=[hbm] * 6,
            out_specs=[vmem] * 7,
            scratch_shapes=[
                pltpu.VMEM((nz, 2, 3, 3, ch, c_mid), jnp.bfloat16),
                pltpu.VMEM((nz, 2, ch, c_out), jnp.bfloat16),
                pltpu.VMEM((3, n, 4 * ch, 2 * c_mid), jnp.float32),
                pltpu.VMEM(w_conv2.shape, w_conv2.dtype),
                pltpu.VMEM((1, c_mid), jnp.float32),
                dma((3,)), pltpu.SemaphoreType.REGULAR((nz // 2,)),
                dma((7,)), dma((ni + 1,)), dma((ni, 2)), dma((ni, 2)), dma((2,)), dma((2, 2)), dma((2,)), dma((2,)),
            ],
            compiler_params=pltpu.CompilerParams(collective_id=0, has_side_effects=True, vmem_limit_bytes=20 * 2**20),
        )(*[pltpu.with_memory_space_constraint(v, pltpu.HBM) for v in (x, w_conv1, b_conv1.reshape(1, c_mid), w_conv2, b_conv2.reshape(1, c_out), w_short)])
        return pl.pallas_call(
            functools.partial(finish_kernel, n, height),
            out_shape=jax.ShapeDtypeStruct((ni, tile, width, c_out), jnp.float32),
            in_specs=[vmem] * 7,
            out_specs=hbm,
            scratch_shapes=[y1s, pltpu.VMEM((LATE + 2, width, c_out), jnp.float32), dma((3,))],
            compiler_params=pltpu.CompilerParams(vmem_limit_bytes=20 * 2**20),
        )(*parts)

    return jax.shard_map(local_step, mesh=mesh, in_specs=(P('data', None, None, 'model'), P(None, None, 'model', None), P(), P(), P(), P('model', None)), out_specs=P('data', 'model', None, None), check_vma=False)
```

```python
import functools

import jax
import jax.numpy as jnp
from jax import lax
from jax.experimental import pallas as pl
from jax.experimental.pallas import tpu as pltpu
from jax.sharding import PartitionSpec as P

MESH = pl.DeviceIdType.MESH
LANES = 128
LATE = 6


def shift_right(v):
    first = lax.broadcasted_iota(jnp.int32, v.shape, 1) == 0
    return jnp.where(first, jnp.zeros_like(v), pltpu.roll(v, 1, axis=1))


def shift_left(v):
    last = lax.broadcasted_iota(jnp.int32, v.shape, 1) == v.shape[1] - 1
    return jnp.where(last, jnp.zeros_like(v), pltpu.roll(v, v.shape[1] - 1, axis=1))


def first_pair(n, height, img, p, xbuf, wt, b1c, y1s):
    ni, _, rows, halves, ch, _ = xbuf.shape
    tile = rows - 4
    c_mid = wt.shape[0] // 2
    kb = n * 4 * ch
    me = lax.axis_index('model')
    x_left = xbuf[img, :, pl.ds(2 * p, 4), 0]
    x_right = xbuf[img, :, pl.ds(2 * p, 4), 1]
    x0 = jnp.concatenate([x_left.reshape(kb, LANES), x_right.reshape(kb, LANES)], axis=1)
    rhs = jnp.concatenate([shift_right(x0), x0, shift_left(x0)], axis=0)
    z2 = jnp.dot(wt[...], rhs, preferred_element_type=jnp.float32)
    for a in range(2):
        y = jnp.maximum(z2[a * c_mid:(a + 1) * c_mid] + jnp.concatenate([b1c[...]] * halves, axis=1), 0.0)
        row = me * tile - 1 + 2 * p + a
        y = jnp.where((row >= 0) & (row < height), y, 0.0).astype(jnp.bfloat16)
        base = pl.multiple_of((2 * p + a) * 3 * c_mid, c_mid)
        y1s[pl.ds(base, c_mid), :] = shift_right(y)
        y1s[pl.ds(base + c_mid, c_mid), :] = y
        y1s[pl.ds(base + 2 * c_mid, c_mid), :] = shift_left(y)


def second_row(img, r, xbuf, w2x, b2_ref, y1s):
    _, n, _, halves, ch, _ = xbuf.shape
    c_mid = w2x.shape[0]
    base = pl.multiple_of(r * 3 * c_mid, c_mid)
    x_row = jnp.concatenate([xbuf[img, :, r + 2, h].reshape(n * ch, LANES) for h in range(halves)], axis=1)
    rhs = jnp.concatenate([y1s[pl.ds(base, 9 * c_mid), :], x_row], axis=0)
    y2 = jnp.dot(w2x[...], rhs, preferred_element_type=jnp.float32)
    return y2.T + b2_ref[...]


def loop(lo, hi, body, unroll=1):
    def step(i, _):
        body(i)
        return 0

    lax.fori_loop(lo, hi, step, 0, unroll=unroll)


def gather_kernel(n, x_ref, w1_ref, b1_hbm, w2_hbm, b2_hbm, ws_ref,
                  xbuf, wt, w2x, b1c, b2_ref, y1s, y2,
                  gw, gs, wk, w2_ref, b1_ref,
                  local, phase, send_x, recv_x, send_h, recv_h, send_w, recv_w, send_v, recv_v):
    ni, height, halves, ch, _ = x_ref.shape
    tile = height // n
    nz = n // 2
    last = ni - 1
    assert last == 2
    c_mid, c_out = w1_ref.shape[3], ws_ref.shape[1]
    kb = n * 4 * ch
    me = lax.axis_index('model')
    my_z, my_c = me // 2, me % 2
    sibling = me + 1 - 2 * my_c

    def core(d, c):
        return ((my_z + d) % nz) * 2 + (my_c + c) % 2

    barrier = pltpu.get_barrier_semaphore()
    for dest in (sibling, core(1, 0), core(1, 1), core(nz - 1, 0), core(nz - 1, 1)):
        pl.semaphore_signal(barrier, inc=1, device_id={'model': dest}, device_id_type=MESH)

    block = tile + 2
    inner, outer = (block - LATE, last), (LATE, ni)

    def part_copy(img, dest, odd, part):
        rows, k = part
        if img < last:
            base, off = dest * tile, 0
        else:
            base = jnp.clip(dest * tile - 2 * (1 - odd), 0, height - block)
            off = (1 - odd) * LATE if part is inner else odd * (block - LATE)
        return (x_ref.at[img, pl.ds(base + off, rows)], xbuf.at[img, me, pl.ds(base + off - dest * tile + 2, rows)], recv_x.at[k])

    def parts_of(img):
        return [(tile, img)] if img < last else [inner, outer]

    def send(img, hops, part, batch):
        for d in hops:
            for c in range(2) if d else (1,):
                dest = core(d, c)
                src, dst, sem = part_copy(img, dest, (my_c + c) % 2, part)
                pltpu.make_async_remote_copy(src_ref=src, dst_ref=dst, send_sem=send_x.at[batch], recv_sem=sem,
                                             device_id={'model': dest}, device_id_type=MESH).start()

    def left(batch, copies, rows):
        ref = xbuf.at[0, pl.ds(0, copies), pl.ds(0, rows)]
        pltpu.make_async_remote_copy(src_ref=ref, dst_ref=ref, send_sem=send_x.at[batch], recv_sem=recv_x.at[0],
                                     device_id={'model': sibling}, device_id_type=MESH).wait_send()

    hubs = [2, nz - 2] if nz >= 8 else [d for d in range(1, nz)]

    own = 0

    def send_weights(moves, k_sem):
        for off, d in moves:
            for k, (src, dst) in enumerate(((w1_ref, gw), (ws_ref, gs))):
                piece = dst.at[(my_z + off) % nz, my_c]
                pltpu.make_async_remote_copy(
                    src_ref=src if off is own else piece, dst_ref=piece, send_sem=send_w.at[k], recv_sem=recv_w.at[k, k_sem],
                    device_id={'model': core(d, 0)}, device_id_type=MESH).start()

    def wait_weights(pieces, k_sem):
        for k, ref in enumerate((gw, gs)):
            arrived(ref.at[pl.ds(0, pieces), my_c], recv_w.at[k, k_sem])

    def arrived(ref, sem):
        pltpu.make_async_remote_copy(src_ref=ref, dst_ref=ref, send_sem=send_x.at[0], recv_sem=sem,
                                     device_id={'model': sibling}, device_id_type=MESH).wait_recv()

    for img in range(ni):
        for part in parts_of(img):
            src, dst, sem = part_copy(img, me, my_c, part)
            pltpu.make_async_copy(src, dst, sem).start()
    pltpu.make_async_copy(w1_ref, gw.at[my_z, my_c], recv_w.at[0, 1]).start()
    pltpu.make_async_copy(ws_ref, gs.at[my_z, my_c], recv_w.at[1, 1]).start()

    fetches = [pltpu.make_async_copy(src, dst, local.at[k])
               for k, (src, dst) in enumerate(((b1_hbm, b1_ref), (b2_hbm, b2_ref), (w2_hbm, w2_ref)))]
    for fetch in fetches:
        fetch.start()

    pl.semaphore_wait(barrier, 5)
    for d in range(1, nz // 2 + 1):
        if d < nz // 2:
            for side in (1, nz - 1):
                pl.semaphore_signal(phase.at[d - 1], inc=1, device_id={'model': core(side, 0)}, device_id_type=MESH)
        send(0, [d, nz - d] if d < nz // 2 else [d], parts_of(0)[0], 0 if d <= nz // 4 else 1)
        if d < nz // 2:
            pl.semaphore_wait(phase.at[d - 1], 2)
        if d == 1 and nz >= 8:
            send_weights([(own, hub) for hub in hubs], 0)
    send(0, [0], parts_of(0)[0], 1)
    near = [d for k in range(1, nz // 2) for d in (k, nz - k)]
    far = [nz // 2] + near[::-1]
    if nz >= 8:
        wait_weights(2, 0)
        send_weights([(nz - 2, 1), (nz - 2, nz - 1), (2, 1), (2, nz - 1)], 1)
        send_weights([((2 + (nz - 4) * (1 - my_c)), (nz - 2) - (nz - 4) * (1 - my_c))], 1)
    else:
        send_weights([(own, hub) for hub in hubs], 0)
    near_copies = 4 * (nz // 4)
    first, rest = far[:3], far[3:] + [0]
    left(0, near_copies, tile)
    send(1, first, parts_of(1)[0], 2)

    for owner, r0 in ((0, 0), (n - 1, tile + 2)):
        @pl.when(me == owner)
        def _():
            for img in range(ni):
                xbuf[img, :, r0:r0 + 2] = jnp.zeros((n, 2, halves, ch, LANES), xbuf.dtype)

    for fetch in fetches:
        fetch.wait()
    b1c[...] = jnp.broadcast_to(b1_ref[...], (LANES, c_mid)).T
    for t in range(9):
        w2x[:, t * c_mid:(t + 1) * c_mid] = w2_ref[t // 3, t % 3].astype(jnp.float32).T.astype(w2x.dtype)
    wk[...] = jnp.zeros_like(wk)
    left(1, n - 1 - near_copies, tile)
    send(1, rest, parts_of(1)[0], 3)

    def pair(img, p):
        first_pair(n, height, img, p, xbuf, wt, b1c, y1s)

    def second(img, r):
        y2[img, r] = second_row(img, r, xbuf, w2x, b2_ref, y1s)

    def build_weights():
        wait_weights(nz - 2 if nz >= 8 else 1, 1)
        if nz < 8:
            wait_weights(nz - 1, 0)
        shares = []
        for k, ref in enumerate((gw.at[:, my_c], gs.at[:, my_c])):
            shares.append(pltpu.make_async_remote_copy(
                src_ref=ref, dst_ref=ref, send_sem=send_v.at[k], recv_sem=recv_v.at[k],
                device_id={'model': sibling}, device_id_type=MESH))
            shares[k].start()
        for share in shares:
            share.wait()

        def place(z):
            for c in range(2):
                src = z * 2 + c
                for dh in range(3):
                    for dw in range(3):
                        piece = gw[z, c, dh, dw].astype(jnp.float32)
                        for a in range(2):
                            wk[dw, src, (dh + a) * ch:(dh + a + 1) * ch, a * c_mid:(a + 1) * c_mid] = piece

        loop(0, nz, place)
        for dw in range(3):
            wt[:, dw * kb:(dw + 1) * kb] = wk[dw].reshape(kb, 2 * c_mid).T.astype(wt.dtype)
        w2x[:, 9 * c_mid:] = gs[...].astype(jnp.float32).reshape(n * ch, c_out).T.astype(w2x.dtype)

    def inner_halo(img):
        return pltpu.make_async_remote_copy(
            src_ref=xbuf.at[img, :, pl.ds(2 + (1 - my_c) * (tile - 2), 2)],
            dst_ref=xbuf.at[img, :, pl.ds(my_c * (tile + 2), 2)],
            send_sem=send_h.at[img, 0], recv_sem=recv_h.at[img, 0], device_id={'model': sibling}, device_id_type=MESH)

    def outer_halo(img):
        return pltpu.make_async_remote_copy(
            src_ref=xbuf.at[img, :, pl.ds(2 + my_c * (tile - 2), 2)],
            dst_ref=xbuf.at[img, :, pl.ds((1 - my_c) * (tile + 2), 2)],
            send_sem=send_h.at[img, 1], recv_sem=recv_h.at[img, 1],
            device_id={'model': (me + n - 1 + 2 * my_c) % n}, device_id_type=MESH)

    has_outer = (me != 0) & (me != n - 1)
    sends_last = (me != 1) & (me != n - 2)

    def when(cond, act):
        @pl.when(cond)
        def _():
            act()

    flip = tile // 2

    def pair_in(img, k):
        pair(img, k + my_c * (flip - 2 * k))

    def rows_in(img, lo, hi, unroll):
        loop(lo, hi, lambda k: second(img, k + my_c * (tile - 1 - 2 * k)), unroll=unroll)

    def most(img, between):
        loop(1, flip - 1, lambda k: pair_in(img, k), unroll=3)
        inner_halo(img).wait_recv()
        loop(flip - 1, flip + 1, lambda k: pair_in(img, k), unroll=2)
        between()
        rows_in(img, 2, tile, 7)

    def edge(img):
        when(has_outer, lambda: outer_halo(img).wait_recv())
        pair_in(img, 0)
        rows_in(img, 0, 2, 2)

    def begin(img):
        arrived(xbuf.at[img, :, pl.ds(0, tile)], recv_x.at[img])
        inner_halo(img).start()
        when(has_outer, lambda: outer_halo(img).start())

    begin(0)
    build_weights()
    most(0, lambda: None)
    left(2, 6, tile)
    send(last, first, inner, 4)
    begin(1)
    send(last, rest, inner, 5)
    edge(0)

    def last_sends():
        left(4, 6, block - LATE)
        send(last, first, outer, 6)

    most(1, last_sends)
    left(5, n - 7, block - LATE)
    send(last, rest, outer, 7)
    edge(1)
    arrived(xbuf.at[last, :, pl.ds(0, block - LATE)], recv_x.at[last])
    when(sends_last, lambda: inner_halo(last).start())
    first_p = LATE // 2 + 1
    loop(first_p, flip - 1, lambda k: pair_in(last, k), unroll=3)
    when(has_outer, lambda: inner_halo(last).wait_recv())
    loop(flip - 1, flip + 1, lambda k: pair_in(last, k), unroll=2)
    rows_in(last, 2 * first_p, tile, 4)

    left(3, n - 7, tile)
    left(6, 6, LATE)
    left(7, n - 7, LATE)
    for k, ref in enumerate((gw.at[pl.ds(0, nz - 1), 0], gs.at[pl.ds(0, nz - 1), 0])):
        pltpu.make_async_remote_copy(src_ref=ref, dst_ref=ref, send_sem=send_w.at[k], recv_sem=recv_w.at[k],
                                     device_id={'model': sibling}, device_id_type=MESH).wait_send()
    for img in range(last):
        inner_halo(img).wait_send()
        when(has_outer, lambda: outer_halo(img).wait_send())
    when(sends_last, lambda: inner_halo(last).wait_send())
    arrived(xbuf.at[last, :, pl.ds(0, LATE)], recv_x.at[ni])


def finish_kernel(n, height, xbuf, wt, w2x, b1c, b2_ref, y1s_in, y2, out_ref, y1s, yb, sem):
    ni, tile = y2.shape[0], y2.shape[1]
    last = ni - 1
    my_c = lax.axis_index('model') % 2
    first_p = LATE // 2 + 1
    left = 2 * first_p
    done = tile - left
    ready = (1 - my_c) * left
    todo = my_c * done
    copies = [pltpu.make_async_copy(y2.at[img, pl.ds(r, 4)], out_ref.at[img, pl.ds(r, 4)], sem.at[0])
              for img in range(last) for r in range(0, tile, 4)]
    copies += [pltpu.make_async_copy(y2.at[last, pl.ds(ready, done)], out_ref.at[last, pl.ds(ready, done)], sem.at[1])]
    for copy in copies:
        copy.start()
    step = 3 * b1c.shape[0]
    edge = (1 - my_c) * left + my_c * (tile - left)
    y1s[pl.ds(pl.multiple_of(edge * step, step), 2 * step), :] = y1s_in[pl.ds(pl.multiple_of(edge * step, step), 2 * step), :]
    flip = tile // 2
    loop(0, first_p, lambda k: first_pair(n, height, last, k + my_c * (flip - 2 * k), xbuf, wt, b1c, y1s), unroll=2)

    def row(k):
        yb[k] = second_row(last, k + todo, xbuf, w2x, b2_ref, y1s)
        pltpu.make_async_copy(yb.at[k], out_ref.at[last, k + todo], sem.at[2]).start()

    loop(0, left, row, unroll=4)
    for copy in copies:
        copy.wait()
    pltpu.make_async_copy(yb, out_ref.at[last, pl.ds(todo, left)], sem.at[2]).wait()


def solution(mesh):
    n = mesh.shape['model']

    def local_step(images, w_conv1, b_conv1, w_conv2, b_conv2, w_short):
        ni, height, width, ch = images.shape
        c_mid, c_out = w_conv1.shape[3], w_short.shape[1]
        tile, halves, nz = height // n, width // LANES, n // 2
        kb = n * 4 * ch
        x = images.transpose(0, 1, 3, 2).reshape(ni, height, ch, halves, LANES).transpose(0, 1, 3, 2, 4)
        vmem = pl.BlockSpec(memory_space=pltpu.VMEM)
        hbm = pl.BlockSpec(memory_space=pltpu.HBM)
        dma = pltpu.SemaphoreType.DMA
        y1s = pltpu.VMEM(((tile + 2) * 3 * c_mid, width), jnp.bfloat16)
        parts = pl.pallas_call(
            functools.partial(gather_kernel, n),
            out_shape=[
                pltpu.VMEM((ni, n, tile + 4, halves, ch, LANES), jnp.bfloat16),
                pltpu.VMEM((2 * c_mid, 3 * kb), jnp.bfloat16),
                pltpu.VMEM((c_out, 9 * c_mid + n * ch), jnp.bfloat16),
                pltpu.VMEM((c_mid, LANES), jnp.float32),
                pltpu.VMEM((1, c_out), jnp.float32),
                y1s,
                pltpu.VMEM((ni, tile, width, c_out), jnp.float32),
            ],
            in_specs=[hbm] * 6,
            out_specs=[vmem] * 7,
            scratch_shapes=[
                pltpu.VMEM((nz, 2, 3, 3, ch, c_mid), jnp.bfloat16),
                pltpu.VMEM((nz, 2, ch, c_out), jnp.bfloat16),
                pltpu.VMEM((3, n, 4 * ch, 2 * c_mid), jnp.float32),
                pltpu.VMEM(w_conv2.shape, w_conv2.dtype),
                pltpu.VMEM((1, c_mid), jnp.float32),
                dma((3,)), pltpu.SemaphoreType.REGULAR((nz // 2,)),
                dma((8,)), dma((ni + 1,)), dma((ni, 2)), dma((ni, 2)), dma((2,)), dma((2, 2)), dma((2,)), dma((2,)),
            ],
            compiler_params=pltpu.CompilerParams(collective_id=0, has_side_effects=True, vmem_limit_bytes=20 * 2**20),
        )(*[pltpu.with_memory_space_constraint(v, pltpu.HBM) for v in (x, w_conv1, b_conv1.reshape(1, c_mid), w_conv2, b_conv2.reshape(1, c_out), w_short)])
        return pl.pallas_call(
            functools.partial(finish_kernel, n, height),
            out_shape=jax.ShapeDtypeStruct((ni, tile, width, c_out), jnp.float32),
            in_specs=[vmem] * 7,
            out_specs=hbm,
            scratch_shapes=[y1s, pltpu.VMEM((LATE + 2, width, c_out), jnp.float32), dma((3,))],
            compiler_params=pltpu.CompilerParams(vmem_limit_bytes=20 * 2**20),
        )(*parts)

    return jax.shard_map(local_step, mesh=mesh, in_specs=(P('data', None, None, 'model'), P(None, None, 'model', None), P(), P(), P(), P('model', None)), out_specs=P('data', 'model', None, None), check_vma=False)
```

```python
import functools

import jax
import jax.numpy as jnp
from jax import lax
from jax.experimental import pallas as pl
from jax.experimental.pallas import tpu as pltpu
from jax.sharding import PartitionSpec as P

MESH = pl.DeviceIdType.MESH
LANES = 128
LATE = 6


def shift_right(v):
    first = lax.broadcasted_iota(jnp.int32, v.shape, 1) == 0
    return jnp.where(first, jnp.zeros_like(v), pltpu.roll(v, 1, axis=1))


def shift_left(v):
    last = lax.broadcasted_iota(jnp.int32, v.shape, 1) == v.shape[1] - 1
    return jnp.where(last, jnp.zeros_like(v), pltpu.roll(v, v.shape[1] - 1, axis=1))


def first_pair(n, height, img, p, xbuf, wt, b1c, y1s):
    ni, _, rows, halves, ch, _ = xbuf.shape
    tile = rows - 4
    c_mid = wt.shape[0] // 2
    kb = n * 4 * ch
    me = lax.axis_index('model')
    x_left = xbuf[img, :, pl.ds(2 * p, 4), 0]
    x_right = xbuf[img, :, pl.ds(2 * p, 4), 1]
    x0 = jnp.concatenate([x_left.reshape(kb, LANES), x_right.reshape(kb, LANES)], axis=1)
    rhs = jnp.concatenate([shift_right(x0), x0, shift_left(x0)], axis=0)
    z2 = jnp.dot(wt[...], rhs, preferred_element_type=jnp.float32)
    for a in range(2):
        y = jnp.maximum(z2[a * c_mid:(a + 1) * c_mid] + jnp.concatenate([b1c[...]] * halves, axis=1), 0.0)
        row = me * tile - 1 + 2 * p + a
        y = jnp.where((row >= 0) & (row < height), y, 0.0).astype(jnp.bfloat16)
        base = pl.multiple_of((2 * p + a) * 3 * c_mid, c_mid)
        y1s[pl.ds(base, c_mid), :] = shift_right(y)
        y1s[pl.ds(base + c_mid, c_mid), :] = y
        y1s[pl.ds(base + 2 * c_mid, c_mid), :] = shift_left(y)


def second_row(img, r, xbuf, w2x, b2_ref, y1s):
    _, n, _, halves, ch, _ = xbuf.shape
    c_mid = w2x.shape[0]
    base = pl.multiple_of(r * 3 * c_mid, c_mid)
    x_row = jnp.concatenate([xbuf[img, :, r + 2, h].reshape(n * ch, LANES) for h in range(halves)], axis=1)
    rhs = jnp.concatenate([y1s[pl.ds(base, 9 * c_mid), :], x_row], axis=0)
    y2 = jnp.dot(w2x[...], rhs, preferred_element_type=jnp.float32)
    return y2.T + b2_ref[...]


def loop(lo, hi, body, unroll=1):
    def step(i, _):
        body(i)
        return 0

    lax.fori_loop(lo, hi, step, 0, unroll=unroll)


def gather_kernel(n, x_ref, w1_ref, b1_hbm, w2_hbm, b2_hbm, ws_ref,
                  xbuf, wt, w2x, b1c, b2_ref, y1s, y2,
                  gw, gs, wk, w2_ref, b1_ref,
                  local, phase, send_x, recv_x, send_h, recv_h, send_w, recv_w, send_v, recv_v):
    ni, height, halves, ch, _ = x_ref.shape
    tile = height // n
    nz = n // 2
    last = ni - 1
    assert last == 2
    c_mid, c_out = w1_ref.shape[3], ws_ref.shape[1]
    kb = n * 4 * ch
    me = lax.axis_index('model')
    my_z, my_c = me // 2, me % 2
    sibling = me + 1 - 2 * my_c

    def core(d, c):
        return ((my_z + d) % nz) * 2 + (my_c + c) % 2

    barrier = pltpu.get_barrier_semaphore()
    for dest in (sibling, core(1, 0), core(1, 1), core(nz - 1, 0), core(nz - 1, 1)):
        pl.semaphore_signal(barrier, inc=1, device_id={'model': dest}, device_id_type=MESH)

    block = tile + 2
    inner, outer = (block - LATE, last), (LATE, ni)

    def part_copy(img, dest, odd, part):
        rows, k = part
        if img < last:
            base, off = dest * tile, 0
        else:
            base = jnp.clip(dest * tile - 2 * (1 - odd), 0, height - block)
            off = (1 - odd) * LATE if part is inner else odd * (block - LATE)
        return (x_ref.at[img, pl.ds(base + off, rows)], xbuf.at[img, me, pl.ds(base + off - dest * tile + 2, rows)], recv_x.at[k])

    def parts_of(img):
        return [(tile, img)] if img < last else [inner, outer]

    def send(img, hops, part, batch):
        for d in hops:
            for c in range(2) if d else (1,):
                dest = core(d, c)
                src, dst, sem = part_copy(img, dest, (my_c + c) % 2, part)
                pltpu.make_async_remote_copy(src_ref=src, dst_ref=dst, send_sem=send_x.at[batch], recv_sem=sem,
                                             device_id={'model': dest}, device_id_type=MESH).start()

    def left(batch, copies, rows):
        ref = xbuf.at[0, pl.ds(0, copies), pl.ds(0, rows)]
        pltpu.make_async_remote_copy(src_ref=ref, dst_ref=ref, send_sem=send_x.at[batch], recv_sem=recv_x.at[0],
                                     device_id={'model': sibling}, device_id_type=MESH).wait_send()

    hubs = [2, nz - 2] if nz >= 8 else [d for d in range(1, nz)]

    own = 0

    def send_weights(moves, k_sem):
        for off, d in moves:
            for k, (src, dst) in enumerate(((w1_ref, gw), (ws_ref, gs))):
                piece = dst.at[(my_z + off) % nz, my_c]
                pltpu.make_async_remote_copy(
                    src_ref=src if off is own else piece, dst_ref=piece, send_sem=send_w.at[k], recv_sem=recv_w.at[k, k_sem],
                    device_id={'model': core(d, 0)}, device_id_type=MESH).start()

    def wait_weights(pieces, k_sem):
        for k, ref in enumerate((gw, gs)):
            arrived(ref.at[pl.ds(0, pieces), my_c], recv_w.at[k, k_sem])

    def arrived(ref, sem):
        pltpu.make_async_remote_copy(src_ref=ref, dst_ref=ref, send_sem=send_x.at[0], recv_sem=sem,
                                     device_id={'model': sibling}, device_id_type=MESH).wait_recv()

    for img in range(ni):
        for part in parts_of(img):
            src, dst, sem = part_copy(img, me, my_c, part)
            pltpu.make_async_copy(src, dst, sem).start()
    pltpu.make_async_copy(w1_ref, gw.at[my_z, my_c], recv_w.at[0, 1]).start()
    pltpu.make_async_copy(ws_ref, gs.at[my_z, my_c], recv_w.at[1, 1]).start()

    fetches = [pltpu.make_async_copy(src, dst, local.at[k])
               for k, (src, dst) in enumerate(((b1_hbm, b1_ref), (b2_hbm, b2_ref), (w2_hbm, w2_ref)))]
    for fetch in fetches:
        fetch.start()

    pl.semaphore_wait(barrier, 5)
    for d in range(1, nz // 2 + 1):
        if d < nz // 2:
            for side in (1, nz - 1):
                pl.semaphore_signal(phase.at[d - 1], inc=1, device_id={'model': core(side, 0)}, device_id_type=MESH)
        send(0, [d, nz - d] if d < nz // 2 else [d], parts_of(0)[0], 0 if d <= nz // 4 else 1)
        if d < nz // 2:
            pl.semaphore_wait(phase.at[d - 1], 2)
        if d == 1 and nz >= 8:
            send_weights([(own, hub) for hub in hubs], 0)
    send(0, [0], parts_of(0)[0], 1)
    near = [d for k in range(1, nz // 2) for d in (k, nz - k)]
    far = [nz // 2] + near[::-1]
    if nz >= 8:
        wait_weights(2, 0)
        send_weights([(nz - 2, 1), (nz - 2, nz - 1), (2, 1), (2, nz - 1)], 1)
        send_weights([((2 + (nz - 4) * (1 - my_c)), (nz - 2) - (nz - 4) * (1 - my_c))], 1)
    else:
        send_weights([(own, hub) for hub in hubs], 0)
    near_copies = 4 * (nz // 4)
    first, rest = far[:3], far[3:] + [0]
    left(0, near_copies, tile)
    send(1, first, parts_of(1)[0], 2)

    for owner, r0 in ((0, 0), (n - 1, tile + 2)):
        @pl.when(me == owner)
        def _():
            for img in range(ni):
                xbuf[img, :, r0:r0 + 2] = jnp.zeros((n, 2, halves, ch, LANES), xbuf.dtype)

    for fetch in fetches:
        fetch.wait()
    b1c[...] = jnp.broadcast_to(b1_ref[...], (LANES, c_mid)).T
    for t in range(9):
        w2x[:, t * c_mid:(t + 1) * c_mid] = w2_ref[t // 3, t % 3].astype(jnp.float32).T.astype(w2x.dtype)
    wk[...] = jnp.zeros_like(wk)
    left(1, n - 1 - near_copies, tile)
    send(1, rest, parts_of(1)[0], 3)

    def pair(img, p):
        first_pair(n, height, img, p, xbuf, wt, b1c, y1s)

    def second(img, r):
        y2[img, r] = second_row(img, r, xbuf, w2x, b2_ref, y1s)

    def build_weights():
        wait_weights(nz - 2 if nz >= 8 else 1, 1)
        if nz < 8:
            wait_weights(nz - 1, 0)
        shares = []
        for k, ref in enumerate((gw.at[:, my_c], gs.at[:, my_c])):
            shares.append(pltpu.make_async_remote_copy(
                src_ref=ref, dst_ref=ref, send_sem=send_v.at[k], recv_sem=recv_v.at[k],
                device_id={'model': sibling}, device_id_type=MESH))
            shares[k].start()
        for share in shares:
            share.wait()

        def place(z):
            for c in range(2):
                src = z * 2 + c
                for dh in range(3):
                    for dw in range(3):
                        piece = gw[z, c, dh, dw].astype(jnp.float32)
                        for a in range(2):
                            wk[dw, src, (dh + a) * ch:(dh + a + 1) * ch, a * c_mid:(a + 1) * c_mid] = piece

        loop(0, nz, place)
        for dw in range(3):
            wt[:, dw * kb:(dw + 1) * kb] = wk[dw].reshape(kb, 2 * c_mid).T.astype(wt.dtype)
        w2x[:, 9 * c_mid:] = gs[...].astype(jnp.float32).reshape(n * ch, c_out).T.astype(w2x.dtype)

    def inner_halo(img):
        return pltpu.make_async_remote_copy(
            src_ref=xbuf.at[img, :, pl.ds(2 + (1 - my_c) * (tile - 2), 2)],
            dst_ref=xbuf.at[img, :, pl.ds(my_c * (tile + 2), 2)],
            send_sem=send_h.at[img, 0], recv_sem=recv_h.at[img, 0], device_id={'model': sibling}, device_id_type=MESH)

    def outer_halo(img):
        return pltpu.make_async_remote_copy(
            src_ref=xbuf.at[img, :, pl.ds(2 + my_c * (tile - 2), 2)],
            dst_ref=xbuf.at[img, :, pl.ds((1 - my_c) * (tile + 2), 2)],
            send_sem=send_h.at[img, 1], recv_sem=recv_h.at[img, 1],
            device_id={'model': (me + n - 1 + 2 * my_c) % n}, device_id_type=MESH)

    has_outer = (me != 0) & (me != n - 1)
    sends_last = (me != 1) & (me != n - 2)

    def when(cond, act):
        @pl.when(cond)
        def _():
            act()

    flip = tile // 2

    def pair_in(img, k):
        pair(img, k + my_c * (flip - 2 * k))

    def rows_in(img, lo, hi, unroll):
        loop(lo, hi, lambda k: second(img, k + my_c * (tile - 1 - 2 * k)), unroll=unroll)

    def most(img, between):
        loop(1, flip - 1, lambda k: pair_in(img, k), unroll=3)
        inner_halo(img).wait_recv()
        loop(flip - 1, flip + 1, lambda k: pair_in(img, k), unroll=2)
        between()
        rows_in(img, 2, tile, 7)

    def edge(img):
        when(has_outer, lambda: outer_halo(img).wait_recv())
        pair_in(img, 0)
        rows_in(img, 0, 2, 2)

    def begin(img):
        arrived(xbuf.at[img, :, pl.ds(0, tile)], recv_x.at[img])
        inner_halo(img).start()
        when(has_outer, lambda: outer_halo(img).start())

    begin(0)
    build_weights()
    most(0, lambda: None)
    left(2, 6, tile)
    send(last, first, inner, 4)
    begin(1)
    send(last, rest, inner, 5)
    edge(0)

    def last_sends():
        left(4, 6, block - LATE)
        send(last, first, outer, 6)

    most(1, last_sends)
    left(5, n - 7, block - LATE)
    send(last, rest, outer, 7)
    edge(1)
    arrived(xbuf.at[last, :, pl.ds(0, block - LATE)], recv_x.at[last])
    when(sends_last, lambda: inner_halo(last).start())
    first_p = LATE // 2 + 1
    loop(first_p, flip - 1, lambda k: pair_in(last, k), unroll=3)
    when(has_outer, lambda: inner_halo(last).wait_recv())
    loop(flip - 1, flip + 1, lambda k: pair_in(last, k), unroll=2)
    rows_in(last, 2 * first_p, tile, 8)

    left(3, n - 7, tile)
    left(6, 6, LATE)
    left(7, n - 7, LATE)
    for k, ref in enumerate((gw.at[pl.ds(0, nz - 1), 0], gs.at[pl.ds(0, nz - 1), 0])):
        pltpu.make_async_remote_copy(src_ref=ref, dst_ref=ref, send_sem=send_w.at[k], recv_sem=recv_w.at[k],
                                     device_id={'model': sibling}, device_id_type=MESH).wait_send()
    for img in range(last):
        inner_halo(img).wait_send()
        when(has_outer, lambda: outer_halo(img).wait_send())
    when(sends_last, lambda: inner_halo(last).wait_send())
    arrived(xbuf.at[last, :, pl.ds(0, LATE)], recv_x.at[ni])


def finish_kernel(n, height, xbuf, wt, w2x, b1c, b2_ref, y1s_in, y2, out_ref, y1s, yb, sem):
    ni, tile = y2.shape[0], y2.shape[1]
    last = ni - 1
    my_c = lax.axis_index('model') % 2
    first_p = LATE // 2 + 1
    left = 2 * first_p
    done = tile - left
    ready = (1 - my_c) * left
    todo = my_c * done
    copies = [pltpu.make_async_copy(y2.at[img, pl.ds(r, 4)], out_ref.at[img, pl.ds(r, 4)], sem.at[0])
              for img in range(last) for r in range(0, tile, 4)]
    copies += [pltpu.make_async_copy(y2.at[last, pl.ds(ready, done)], out_ref.at[last, pl.ds(ready, done)], sem.at[1])]
    for copy in copies:
        copy.start()
    step = 3 * b1c.shape[0]
    edge = (1 - my_c) * left + my_c * (tile - left)
    y1s[pl.ds(pl.multiple_of(edge * step, step), 2 * step), :] = y1s_in[pl.ds(pl.multiple_of(edge * step, step), 2 * step), :]
    flip = tile // 2
    loop(0, first_p, lambda k: first_pair(n, height, last, k + my_c * (flip - 2 * k), xbuf, wt, b1c, y1s), unroll=2)

    def row(k):
        yb[k] = second_row(last, k + todo, xbuf, w2x, b2_ref, y1s)
        pltpu.make_async_copy(yb.at[k], out_ref.at[last, k + todo], sem.at[2]).start()

    loop(0, left, row, unroll=8)
    for copy in copies:
        copy.wait()
    pltpu.make_async_copy(yb, out_ref.at[last, pl.ds(todo, left)], sem.at[2]).wait()


def solution(mesh):
    n = mesh.shape['model']

    def local_step(images, w_conv1, b_conv1, w_conv2, b_conv2, w_short):
        ni, height, width, ch = images.shape
        c_mid, c_out = w_conv1.shape[3], w_short.shape[1]
        tile, halves, nz = height // n, width // LANES, n // 2
        kb = n * 4 * ch
        x = images.transpose(0, 1, 3, 2).reshape(ni, height, ch, halves, LANES).transpose(0, 1, 3, 2, 4)
        vmem = pl.BlockSpec(memory_space=pltpu.VMEM)
        hbm = pl.BlockSpec(memory_space=pltpu.HBM)
        dma = pltpu.SemaphoreType.DMA
        y1s = pltpu.VMEM(((tile + 2) * 3 * c_mid, width), jnp.bfloat16)
        parts = pl.pallas_call(
            functools.partial(gather_kernel, n),
            out_shape=[
                pltpu.VMEM((ni, n, tile + 4, halves, ch, LANES), jnp.bfloat16),
                pltpu.VMEM((2 * c_mid, 3 * kb), jnp.bfloat16),
                pltpu.VMEM((c_out, 9 * c_mid + n * ch), jnp.bfloat16),
                pltpu.VMEM((c_mid, LANES), jnp.float32),
                pltpu.VMEM((1, c_out), jnp.float32),
                y1s,
                pltpu.VMEM((ni, tile, width, c_out), jnp.float32),
            ],
            in_specs=[hbm] * 6,
            out_specs=[vmem] * 7,
            scratch_shapes=[
                pltpu.VMEM((nz, 2, 3, 3, ch, c_mid), jnp.bfloat16),
                pltpu.VMEM((nz, 2, ch, c_out), jnp.bfloat16),
                pltpu.VMEM((3, n, 4 * ch, 2 * c_mid), jnp.float32),
                pltpu.VMEM(w_conv2.shape, w_conv2.dtype),
                pltpu.VMEM((1, c_mid), jnp.float32),
                dma((3,)), pltpu.SemaphoreType.REGULAR((nz // 2,)),
                dma((8,)), dma((ni + 1,)), dma((ni, 2)), dma((ni, 2)), dma((2,)), dma((2, 2)), dma((2,)), dma((2,)),
            ],
            compiler_params=pltpu.CompilerParams(collective_id=0, has_side_effects=True, vmem_limit_bytes=20 * 2**20),
        )(*[pltpu.with_memory_space_constraint(v, pltpu.HBM) for v in (x, w_conv1, b_conv1.reshape(1, c_mid), w_conv2, b_conv2.reshape(1, c_out), w_short)])
        return pl.pallas_call(
            functools.partial(finish_kernel, n, height),
            out_shape=jax.ShapeDtypeStruct((ni, tile, width, c_out), jnp.float32),
            in_specs=[vmem] * 7,
            out_specs=hbm,
            scratch_shapes=[y1s, pltpu.VMEM((LATE + 2, width, c_out), jnp.float32), dma((3,))],
            compiler_params=pltpu.CompilerParams(vmem_limit_bytes=20 * 2**20),
        )(*parts)

    return jax.shard_map(local_step, mesh=mesh, in_specs=(P('data', None, None, 'model'), P(None, None, 'model', None), P(), P(), P(), P('model', None)), out_specs=P('data', 'model', None, None), check_vma=False)
```

```python
import functools

import jax
import jax.numpy as jnp
from jax import lax
from jax.experimental import pallas as pl
from jax.experimental.pallas import tpu as pltpu
from jax.sharding import PartitionSpec as P

MESH = pl.DeviceIdType.MESH
LANES = 128
LATE = 6


def shift_right(v):
    first = lax.broadcasted_iota(jnp.int32, v.shape, 1) == 0
    return jnp.where(first, jnp.zeros_like(v), pltpu.roll(v, 1, axis=1))


def shift_left(v):
    last = lax.broadcasted_iota(jnp.int32, v.shape, 1) == v.shape[1] - 1
    return jnp.where(last, jnp.zeros_like(v), pltpu.roll(v, v.shape[1] - 1, axis=1))


def first_pair(n, height, img, p, xbuf, wt, b1c, y1s):
    ni, _, rows, halves, ch, _ = xbuf.shape
    tile = rows - 4
    c_mid = wt.shape[0] // 2
    kb = n * 4 * ch
    me = lax.axis_index('model')
    x_left = xbuf[img, :, pl.ds(2 * p, 4), 0]
    x_right = xbuf[img, :, pl.ds(2 * p, 4), 1]
    x0 = jnp.concatenate([x_left.reshape(kb, LANES), x_right.reshape(kb, LANES)], axis=1)
    rhs = jnp.concatenate([shift_right(x0), x0, shift_left(x0)], axis=0)
    z2 = jnp.dot(wt[...], rhs, preferred_element_type=jnp.float32)
    for a in range(2):
        y = jnp.maximum(z2[a * c_mid:(a + 1) * c_mid] + jnp.concatenate([b1c[...]] * halves, axis=1), 0.0)
        row = me * tile - 1 + 2 * p + a
        y = jnp.where((row >= 0) & (row < height), y, 0.0).astype(jnp.bfloat16)
        base = pl.multiple_of((2 * p + a) * 3 * c_mid, c_mid)
        y1s[pl.ds(base, c_mid), :] = shift_right(y)
        y1s[pl.ds(base + c_mid, c_mid), :] = y
        y1s[pl.ds(base + 2 * c_mid, c_mid), :] = shift_left(y)


def second_row(img, r, xbuf, w2x, b2_ref, y1s):
    _, n, _, halves, ch, _ = xbuf.shape
    c_mid = w2x.shape[0]
    base = pl.multiple_of(r * 3 * c_mid, c_mid)
    x_row = jnp.concatenate([xbuf[img, :, r + 2, h].reshape(n * ch, LANES) for h in range(halves)], axis=1)
    rhs = jnp.concatenate([y1s[pl.ds(base, 9 * c_mid), :], x_row], axis=0)
    y2 = jnp.dot(w2x[...], rhs, preferred_element_type=jnp.float32)
    return y2.T + b2_ref[...]


def loop(lo, hi, body, unroll=1):
    def step(i, _):
        body(i)
        return 0

    lax.fori_loop(lo, hi, step, 0, unroll=unroll)


def gather_kernel(n, x_ref, w1_ref, b1_hbm, w2_hbm, b2_hbm, ws_ref,
                  xbuf, wt, w2x, b1c, b2_ref, y1s, y2,
                  gw, gs, wk, w2_ref, b1_ref,
                  local, phase, send_x, recv_x, send_h, recv_h, send_w, recv_w, send_v, recv_v):
    ni, height, halves, ch, _ = x_ref.shape
    tile = height // n
    nz = n // 2
    last = ni - 1
    assert last == 2
    c_mid, c_out = w1_ref.shape[3], ws_ref.shape[1]
    kb = n * 4 * ch
    me = lax.axis_index('model')
    my_z, my_c = me // 2, me % 2
    sibling = me + 1 - 2 * my_c

    def core(d, c):
        return ((my_z + d) % nz) * 2 + (my_c + c) % 2

    barrier = pltpu.get_barrier_semaphore()
    for dest in (sibling, core(1, 0), core(1, 1), core(nz - 1, 0), core(nz - 1, 1)):
        pl.semaphore_signal(barrier, inc=1, device_id={'model': dest}, device_id_type=MESH)

    block = tile + 2
    inner, outer = (block - LATE, last), (LATE, ni)

    def part_copy(img, dest, odd, part):
        rows, k = part
        if img < last:
            base, off = dest * tile, 0
        else:
            base = jnp.clip(dest * tile - 2 * (1 - odd), 0, height - block)
            off = (1 - odd) * LATE if part is inner else odd * (block - LATE)
        return (x_ref.at[img, pl.ds(base + off, rows)], xbuf.at[img, me, pl.ds(base + off - dest * tile + 2, rows)], recv_x.at[k])

    def parts_of(img):
        return [(tile, img)] if img < last else [inner, outer]

    def send(img, hops, part, batch):
        for d in hops:
            for c in range(2) if d else (1,):
                dest = core(d, c)
                src, dst, sem = part_copy(img, dest, (my_c + c) % 2, part)
                pltpu.make_async_remote_copy(src_ref=src, dst_ref=dst, send_sem=send_x.at[batch], recv_sem=sem,
                                             device_id={'model': dest}, device_id_type=MESH).start()

    def left(batch, copies, rows):
        ref = xbuf.at[0, pl.ds(0, copies), pl.ds(0, rows)]
        pltpu.make_async_remote_copy(src_ref=ref, dst_ref=ref, send_sem=send_x.at[batch], recv_sem=recv_x.at[0],
                                     device_id={'model': sibling}, device_id_type=MESH).wait_send()

    hubs = [2, nz - 2] if nz >= 8 else [d for d in range(1, nz)]

    own = 0

    def send_weights(moves, k_sem):
        for off, d in moves:
            for k, (src, dst) in enumerate(((w1_ref, gw), (ws_ref, gs))):
                piece = dst.at[(my_z + off) % nz, my_c]
                pltpu.make_async_remote_copy(
                    src_ref=src if off is own else piece, dst_ref=piece, send_sem=send_w.at[k], recv_sem=recv_w.at[k, k_sem],
                    device_id={'model': core(d, 0)}, device_id_type=MESH).start()

    def wait_weights(pieces, k_sem):
        for k, ref in enumerate((gw, gs)):
            arrived(ref.at[pl.ds(0, pieces), my_c], recv_w.at[k, k_sem])

    def arrived(ref, sem):
        pltpu.make_async_remote_copy(src_ref=ref, dst_ref=ref, send_sem=send_x.at[0], recv_sem=sem,
                                     device_id={'model': sibling}, device_id_type=MESH).wait_recv()

    for img in range(ni):
        for part in parts_of(img):
            src, dst, sem = part_copy(img, me, my_c, part)
            pltpu.make_async_copy(src, dst, sem).start()
    pltpu.make_async_copy(w1_ref, gw.at[my_z, my_c], recv_w.at[0, 1]).start()
    pltpu.make_async_copy(ws_ref, gs.at[my_z, my_c], recv_w.at[1, 1]).start()

    fetches = [pltpu.make_async_copy(src, dst, local.at[k])
               for k, (src, dst) in enumerate(((b1_hbm, b1_ref), (b2_hbm, b2_ref), (w2_hbm, w2_ref)))]
    for fetch in fetches:
        fetch.start()

    pl.semaphore_wait(barrier, 5)
    for d in range(1, nz // 2 + 1):
        if d < nz // 2:
            for side in (1, nz - 1):
                pl.semaphore_signal(phase.at[d - 1], inc=1, device_id={'model': core(side, 0)}, device_id_type=MESH)
        send(0, [d, nz - d] if d < nz // 2 else [d], parts_of(0)[0], 0 if d <= nz // 4 else 1)
        if d < nz // 2:
            pl.semaphore_wait(phase.at[d - 1], 2)
        if d == 1 and nz >= 8:
            send_weights([(own, hub) for hub in hubs], 0)
    send(0, [0], parts_of(0)[0], 1)
    near = [d for k in range(1, nz // 2) for d in (k, nz - k)]
    far = [nz // 2] + near[::-1]
    if nz >= 8:
        wait_weights(2, 0)
        send_weights([(nz - 2, 1), (nz - 2, nz - 1), (2, 1), (2, nz - 1)], 1)
        send_weights([((2 + (nz - 4) * (1 - my_c)), (nz - 2) - (nz - 4) * (1 - my_c))], 1)
    else:
        send_weights([(own, hub) for hub in hubs], 0)
    near_copies = 4 * (nz // 4)
    first, rest = far[:3], far[3:] + [0]
    left(0, near_copies, tile)
    send(1, first, parts_of(1)[0], 2)

    for owner, r0 in ((0, 0), (n - 1, tile + 2)):
        @pl.when(me == owner)
        def _():
            for img in range(ni):
                xbuf[img, :, r0:r0 + 2] = jnp.zeros((n, 2, halves, ch, LANES), xbuf.dtype)

    for fetch in fetches:
        fetch.wait()
    b1c[...] = jnp.broadcast_to(b1_ref[...], (LANES, c_mid)).T
    for t in range(9):
        w2x[:, t * c_mid:(t + 1) * c_mid] = w2_ref[t // 3, t % 3].astype(jnp.float32).T.astype(w2x.dtype)
    wk[...] = jnp.zeros_like(wk)
    left(1, n - 1 - near_copies, tile)
    send(1, rest, parts_of(1)[0], 3)

    def pair(img, p):
        first_pair(n, height, img, p, xbuf, wt, b1c, y1s)

    def second(img, r):
        y2[img, r] = second_row(img, r, xbuf, w2x, b2_ref, y1s)

    def build_weights():
        wait_weights(nz - 2 if nz >= 8 else 1, 1)
        if nz < 8:
            wait_weights(nz - 1, 0)
        shares = []
        for k, ref in enumerate((gw.at[:, my_c], gs.at[:, my_c])):
            shares.append(pltpu.make_async_remote_copy(
                src_ref=ref, dst_ref=ref, send_sem=send_v.at[k], recv_sem=recv_v.at[k],
                device_id={'model': sibling}, device_id_type=MESH))
            shares[k].start()
        for share in shares:
            share.wait()

        def place(z):
            for c in range(2):
                src = z * 2 + c
                for dh in range(3):
                    for dw in range(3):
                        piece = gw[z, c, dh, dw].astype(jnp.float32)
                        for a in range(2):
                            wk[dw, src, (dh + a) * ch:(dh + a + 1) * ch, a * c_mid:(a + 1) * c_mid] = piece

        loop(0, nz, place)
        for dw in range(3):
            wt[:, dw * kb:(dw + 1) * kb] = wk[dw].reshape(kb, 2 * c_mid).T.astype(wt.dtype)
        w2x[:, 9 * c_mid:] = gs[...].astype(jnp.float32).reshape(n * ch, c_out).T.astype(w2x.dtype)

    def inner_halo(img):
        return pltpu.make_async_remote_copy(
            src_ref=xbuf.at[img, :, pl.ds(2 + (1 - my_c) * (tile - 2), 2)],
            dst_ref=xbuf.at[img, :, pl.ds(my_c * (tile + 2), 2)],
            send_sem=send_h.at[img, 0], recv_sem=recv_h.at[img, 0], device_id={'model': sibling}, device_id_type=MESH)

    def outer_halo(img):
        return pltpu.make_async_remote_copy(
            src_ref=xbuf.at[img, :, pl.ds(2 + my_c * (tile - 2), 2)],
            dst_ref=xbuf.at[img, :, pl.ds((1 - my_c) * (tile + 2), 2)],
            send_sem=send_h.at[img, 1], recv_sem=recv_h.at[img, 1],
            device_id={'model': (me + n - 1 + 2 * my_c) % n}, device_id_type=MESH)

    has_outer = (me != 0) & (me != n - 1)
    sends_last = (me != 1) & (me != n - 2)

    def when(cond, act):
        @pl.when(cond)
        def _():
            act()

    flip = tile // 2

    def pair_in(img, k):
        pair(img, k + my_c * (flip - 2 * k))

    def rows_in(img, lo, hi, unroll):
        loop(lo, hi, lambda k: second(img, k + my_c * (tile - 1 - 2 * k)), unroll=unroll)

    def most(img, between):
        loop(1, flip - 1, lambda k: pair_in(img, k), unroll=3)
        inner_halo(img).wait_recv()
        loop(flip - 1, flip + 1, lambda k: pair_in(img, k), unroll=2)
        between()
        rows_in(img, 2, tile, 7)

    def edge(img):
        when(has_outer, lambda: outer_halo(img).wait_recv())
        pair_in(img, 0)
        rows_in(img, 0, 2, 2)

    def begin(img):
        arrived(xbuf.at[img, :, pl.ds(0, tile)], recv_x.at[img])
        inner_halo(img).start()
        when(has_outer, lambda: outer_halo(img).start())

    begin(0)
    build_weights()
    def inner_sends():
        left(2, 6, tile)
        send(last, first, inner, 4)

    most(0, inner_sends)
    begin(1)
    send(last, rest, inner, 5)
    edge(0)

    def last_sends():
        left(4, 6, block - LATE)
        send(last, first, outer, 6)

    most(1, last_sends)
    left(5, n - 7, block - LATE)
    send(last, rest, outer, 7)
    edge(1)
    arrived(xbuf.at[last, :, pl.ds(0, block - LATE)], recv_x.at[last])
    when(sends_last, lambda: inner_halo(last).start())
    first_p = LATE // 2 + 1
    loop(first_p, flip - 1, lambda k: pair_in(last, k), unroll=3)
    when(has_outer, lambda: inner_halo(last).wait_recv())
    loop(flip - 1, flip + 1, lambda k: pair_in(last, k), unroll=2)
    rows_in(last, 2 * first_p, tile, 8)

    left(3, n - 7, tile)
    left(6, 6, LATE)
    left(7, n - 7, LATE)
    for k, ref in enumerate((gw.at[pl.ds(0, nz - 1), 0], gs.at[pl.ds(0, nz - 1), 0])):
        pltpu.make_async_remote_copy(src_ref=ref, dst_ref=ref, send_sem=send_w.at[k], recv_sem=recv_w.at[k],
                                     device_id={'model': sibling}, device_id_type=MESH).wait_send()
    for img in range(last):
        inner_halo(img).wait_send()
        when(has_outer, lambda: outer_halo(img).wait_send())
    when(sends_last, lambda: inner_halo(last).wait_send())
    arrived(xbuf.at[last, :, pl.ds(0, LATE)], recv_x.at[ni])


def finish_kernel(n, height, xbuf, wt, w2x, b1c, b2_ref, y1s_in, y2, out_ref, y1s, yb, sem):
    ni, tile = y2.shape[0], y2.shape[1]
    last = ni - 1
    my_c = lax.axis_index('model') % 2
    first_p = LATE // 2 + 1
    left = 2 * first_p
    done = tile - left
    ready = (1 - my_c) * left
    todo = my_c * done
    copies = [pltpu.make_async_copy(y2.at[img, pl.ds(r, 4)], out_ref.at[img, pl.ds(r, 4)], sem.at[0])
              for img in range(last) for r in range(0, tile, 4)]
    copies += [pltpu.make_async_copy(y2.at[last, pl.ds(ready, done)], out_ref.at[last, pl.ds(ready, done)], sem.at[1])]
    for copy in copies:
        copy.start()
    step = 3 * b1c.shape[0]
    edge = (1 - my_c) * left + my_c * (tile - left)
    y1s[pl.ds(pl.multiple_of(edge * step, step), 2 * step), :] = y1s_in[pl.ds(pl.multiple_of(edge * step, step), 2 * step), :]
    flip = tile // 2
    loop(0, first_p, lambda k: first_pair(n, height, last, k + my_c * (flip - 2 * k), xbuf, wt, b1c, y1s), unroll=2)

    def row(k):
        yb[k] = second_row(last, k + todo, xbuf, w2x, b2_ref, y1s)
        pltpu.make_async_copy(yb.at[k], out_ref.at[last, k + todo], sem.at[2]).start()

    loop(0, left, row, unroll=8)
    for copy in copies:
        copy.wait()
    pltpu.make_async_copy(yb, out_ref.at[last, pl.ds(todo, left)], sem.at[2]).wait()


def solution(mesh):
    n = mesh.shape['model']

    def local_step(images, w_conv1, b_conv1, w_conv2, b_conv2, w_short):
        ni, height, width, ch = images.shape
        c_mid, c_out = w_conv1.shape[3], w_short.shape[1]
        tile, halves, nz = height // n, width // LANES, n // 2
        kb = n * 4 * ch
        x = images.transpose(0, 1, 3, 2).reshape(ni, height, ch, halves, LANES).transpose(0, 1, 3, 2, 4)
        vmem = pl.BlockSpec(memory_space=pltpu.VMEM)
        hbm = pl.BlockSpec(memory_space=pltpu.HBM)
        dma = pltpu.SemaphoreType.DMA
        y1s = pltpu.VMEM(((tile + 2) * 3 * c_mid, width), jnp.bfloat16)
        parts = pl.pallas_call(
            functools.partial(gather_kernel, n),
            out_shape=[
                pltpu.VMEM((ni, n, tile + 4, halves, ch, LANES), jnp.bfloat16),
                pltpu.VMEM((2 * c_mid, 3 * kb), jnp.bfloat16),
                pltpu.VMEM((c_out, 9 * c_mid + n * ch), jnp.bfloat16),
                pltpu.VMEM((c_mid, LANES), jnp.float32),
                pltpu.VMEM((1, c_out), jnp.float32),
                y1s,
                pltpu.VMEM((ni, tile, width, c_out), jnp.float32),
            ],
            in_specs=[hbm] * 6,
            out_specs=[vmem] * 7,
            scratch_shapes=[
                pltpu.VMEM((nz, 2, 3, 3, ch, c_mid), jnp.bfloat16),
                pltpu.VMEM((nz, 2, ch, c_out), jnp.bfloat16),
                pltpu.VMEM((3, n, 4 * ch, 2 * c_mid), jnp.float32),
                pltpu.VMEM(w_conv2.shape, w_conv2.dtype),
                pltpu.VMEM((1, c_mid), jnp.float32),
                dma((3,)), pltpu.SemaphoreType.REGULAR((nz // 2,)),
                dma((8,)), dma((ni + 1,)), dma((ni, 2)), dma((ni, 2)), dma((2,)), dma((2, 2)), dma((2,)), dma((2,)),
            ],
            compiler_params=pltpu.CompilerParams(collective_id=0, has_side_effects=True, vmem_limit_bytes=20 * 2**20),
        )(*[pltpu.with_memory_space_constraint(v, pltpu.HBM) for v in (x, w_conv1, b_conv1.reshape(1, c_mid), w_conv2, b_conv2.reshape(1, c_out), w_short)])
        return pl.pallas_call(
            functools.partial(finish_kernel, n, height),
            out_shape=jax.ShapeDtypeStruct((ni, tile, width, c_out), jnp.float32),
            in_specs=[vmem] * 7,
            out_specs=hbm,
            scratch_shapes=[y1s, pltpu.VMEM((LATE + 2, width, c_out), jnp.float32), dma((3,))],
            compiler_params=pltpu.CompilerParams(vmem_limit_bytes=20 * 2**20),
        )(*parts)

    return jax.shard_map(local_step, mesh=mesh, in_specs=(P('data', None, None, 'model'), P(None, None, 'model', None), P(), P(), P(), P('model', None)), out_specs=P('data', 'model', None, None), check_vma=False)
```

```python
import functools

import jax
import jax.numpy as jnp
from jax import lax
from jax.experimental import pallas as pl
from jax.experimental.pallas import tpu as pltpu
from jax.sharding import PartitionSpec as P

MESH = pl.DeviceIdType.MESH
LANES = 128
LATE = 6


def shift_right(v):
    first = lax.broadcasted_iota(jnp.int32, v.shape, 1) == 0
    return jnp.where(first, jnp.zeros_like(v), pltpu.roll(v, 1, axis=1))


def shift_left(v):
    last = lax.broadcasted_iota(jnp.int32, v.shape, 1) == v.shape[1] - 1
    return jnp.where(last, jnp.zeros_like(v), pltpu.roll(v, v.shape[1] - 1, axis=1))


def first_pair(n, height, img, p, xbuf, wt, b1c, y1s):
    ni, _, rows, halves, ch, _ = xbuf.shape
    tile = rows - 4
    c_mid = wt.shape[0] // 2
    kb = n * 4 * ch
    me = lax.axis_index('model')
    x_left = xbuf[img, :, pl.ds(2 * p, 4), 0]
    x_right = xbuf[img, :, pl.ds(2 * p, 4), 1]
    x0 = jnp.concatenate([x_left.reshape(kb, LANES), x_right.reshape(kb, LANES)], axis=1)
    rhs = jnp.concatenate([shift_right(x0), x0, shift_left(x0)], axis=0)
    z2 = jnp.dot(wt[...], rhs, preferred_element_type=jnp.float32)
    for a in range(2):
        y = jnp.maximum(z2[a * c_mid:(a + 1) * c_mid] + jnp.concatenate([b1c[...]] * halves, axis=1), 0.0)
        row = me * tile - 1 + 2 * p + a
        y = jnp.where((row >= 0) & (row < height), y, 0.0).astype(jnp.bfloat16)
        base = pl.multiple_of((2 * p + a) * 3 * c_mid, c_mid)
        y1s[pl.ds(base, c_mid), :] = shift_right(y)
        y1s[pl.ds(base + c_mid, c_mid), :] = y
        y1s[pl.ds(base + 2 * c_mid, c_mid), :] = shift_left(y)


def second_row(img, r, xbuf, w2x, b2_ref, y1s):
    _, n, _, halves, ch, _ = xbuf.shape
    c_mid = w2x.shape[0]
    base = pl.multiple_of(r * 3 * c_mid, c_mid)
    x_row = jnp.concatenate([xbuf[img, :, r + 2, h].reshape(n * ch, LANES) for h in range(halves)], axis=1)
    rhs = jnp.concatenate([y1s[pl.ds(base, 9 * c_mid), :], x_row], axis=0)
    y2 = jnp.dot(w2x[...], rhs, preferred_element_type=jnp.float32)
    return y2.T + b2_ref[...]


def loop(lo, hi, body, unroll=1):
    def step(i, _):
        body(i)
        return 0

    lax.fori_loop(lo, hi, step, 0, unroll=unroll)


def gather_kernel(n, x_ref, w1_ref, b1_hbm, w2_hbm, b2_hbm, ws_ref,
                  xbuf, wt, w2x, b1c, b2_ref, y1s, y2,
                  gw, gs, wk, w2_ref, b1_ref,
                  local, phase, send_x, recv_x, send_h, recv_h, send_w, recv_w, send_v, recv_v):
    ni, height, halves, ch, _ = x_ref.shape
    tile = height // n
    nz = n // 2
    last = ni - 1
    assert last == 2
    c_mid, c_out = w1_ref.shape[3], ws_ref.shape[1]
    kb = n * 4 * ch
    me = lax.axis_index('model')
    my_z, my_c = me // 2, me % 2
    sibling = me + 1 - 2 * my_c

    def core(d, c):
        return ((my_z + d) % nz) * 2 + (my_c + c) % 2

    barrier = pltpu.get_barrier_semaphore()
    for dest in (sibling, core(1, 0), core(1, 1), core(nz - 1, 0), core(nz - 1, 1)):
        pl.semaphore_signal(barrier, inc=1, device_id={'model': dest}, device_id_type=MESH)

    block = tile + 2
    inner, outer = (block - LATE, last), (LATE, ni)

    def part_copy(img, dest, odd, part):
        rows, k = part
        if img < last:
            base, off = dest * tile, 0
        else:
            base = jnp.clip(dest * tile - 2 * (1 - odd), 0, height - block)
            off = (1 - odd) * LATE if part is inner else odd * (block - LATE)
        return (x_ref.at[img, pl.ds(base + off, rows)], xbuf.at[img, me, pl.ds(base + off - dest * tile + 2, rows)], recv_x.at[k])

    def parts_of(img):
        return [(tile, img)] if img < last else [inner, outer]

    def send(img, hops, part, batch):
        for d in hops:
            for c in range(2) if d else (1,):
                dest = core(d, c)
                src, dst, sem = part_copy(img, dest, (my_c + c) % 2, part)
                pltpu.make_async_remote_copy(src_ref=src, dst_ref=dst, send_sem=send_x.at[batch], recv_sem=sem,
                                             device_id={'model': dest}, device_id_type=MESH).start()

    def left(batch, copies, rows):
        ref = xbuf.at[0, pl.ds(0, copies), pl.ds(0, rows)]
        pltpu.make_async_remote_copy(src_ref=ref, dst_ref=ref, send_sem=send_x.at[batch], recv_sem=recv_x.at[0],
                                     device_id={'model': sibling}, device_id_type=MESH).wait_send()

    hubs = [2, nz - 2] if nz >= 8 else [d for d in range(1, nz)]

    own = 0

    def send_weights(moves, k_sem):
        for off, d in moves:
            for k, (src, dst) in enumerate(((w1_ref, gw), (ws_ref, gs))):
                piece = dst.at[(my_z + off) % nz, my_c]
                pltpu.make_async_remote_copy(
                    src_ref=src if off is own else piece, dst_ref=piece, send_sem=send_w.at[k], recv_sem=recv_w.at[k, k_sem],
                    device_id={'model': core(d, 0)}, device_id_type=MESH).start()

    def wait_weights(pieces, k_sem):
        for k, ref in enumerate((gw, gs)):
            arrived(ref.at[pl.ds(0, pieces), my_c], recv_w.at[k, k_sem])

    def arrived(ref, sem):
        pltpu.make_async_remote_copy(src_ref=ref, dst_ref=ref, send_sem=send_x.at[0], recv_sem=sem,
                                     device_id={'model': sibling}, device_id_type=MESH).wait_recv()

    for img in range(ni):
        for part in parts_of(img):
            src, dst, sem = part_copy(img, me, my_c, part)
            pltpu.make_async_copy(src, dst, sem).start()
    pltpu.make_async_copy(w1_ref, gw.at[my_z, my_c], recv_w.at[0, 1]).start()
    pltpu.make_async_copy(ws_ref, gs.at[my_z, my_c], recv_w.at[1, 1]).start()

    fetches = [pltpu.make_async_copy(src, dst, local.at[k])
               for k, (src, dst) in enumerate(((b1_hbm, b1_ref), (b2_hbm, b2_ref), (w2_hbm, w2_ref)))]
    for fetch in fetches:
        fetch.start()

    pl.semaphore_wait(barrier, 5)
    for d in range(1, nz // 2 + 1):
        if d < nz // 2:
            for side in (1, nz - 1):
                pl.semaphore_signal(phase.at[d - 1], inc=1, device_id={'model': core(side, 0)}, device_id_type=MESH)
        send(0, [d, nz - d] if d < nz // 2 else [d], parts_of(0)[0], 0 if d <= nz // 4 else 1)
        if d < nz // 2:
            pl.semaphore_wait(phase.at[d - 1], 2)
        if d == 1 and nz >= 8:
            send_weights([(own, hub) for hub in hubs], 0)
    send(0, [0], parts_of(0)[0], 1)
    near = [d for k in range(1, nz // 2) for d in (k, nz - k)]
    far = [nz // 2] + near[::-1]
    if nz >= 8:
        wait_weights(2, 0)
        send_weights([(nz - 2, 1), (nz - 2, nz - 1), (2, 1), (2, nz - 1)], 1)
        send_weights([((2 + (nz - 4) * (1 - my_c)), (nz - 2) - (nz - 4) * (1 - my_c))], 1)
    else:
        send_weights([(own, hub) for hub in hubs], 0)
    near_copies = 4 * (nz // 4)
    first, rest = far[:3], far[3:] + [0]
    left(0, near_copies, tile)
    send(1, first[:1], parts_of(1)[0], 2)

    for owner, r0 in ((0, 0), (n - 1, tile + 2)):
        @pl.when(me == owner)
        def _():
            for img in range(ni):
                xbuf[img, :, r0:r0 + 2] = jnp.zeros((n, 2, halves, ch, LANES), xbuf.dtype)

    for fetch in fetches:
        fetch.wait()
    b1c[...] = jnp.broadcast_to(b1_ref[...], (LANES, c_mid)).T
    for t in range(9):
        w2x[:, t * c_mid:(t + 1) * c_mid] = w2_ref[t // 3, t % 3].astype(jnp.float32).T.astype(w2x.dtype)
    wk[...] = jnp.zeros_like(wk)
    left(1, n - 1 - near_copies, tile)
    send(1, first[1:], parts_of(1)[0], 2)
    send(1, rest, parts_of(1)[0], 3)

    def pair(img, p):
        first_pair(n, height, img, p, xbuf, wt, b1c, y1s)

    def second(img, r):
        y2[img, r] = second_row(img, r, xbuf, w2x, b2_ref, y1s)

    def build_weights():
        wait_weights(nz - 2 if nz >= 8 else 1, 1)
        if nz < 8:
            wait_weights(nz - 1, 0)
        shares = []
        for k, ref in enumerate((gw.at[:, my_c], gs.at[:, my_c])):
            shares.append(pltpu.make_async_remote_copy(
                src_ref=ref, dst_ref=ref, send_sem=send_v.at[k], recv_sem=recv_v.at[k],
                device_id={'model': sibling}, device_id_type=MESH))
            shares[k].start()
        for share in shares:
            share.wait()

        def place(z):
            for c in range(2):
                src = z * 2 + c
                for dh in range(3):
                    for dw in range(3):
                        piece = gw[z, c, dh, dw].astype(jnp.float32)
                        for a in range(2):
                            wk[dw, src, (dh + a) * ch:(dh + a + 1) * ch, a * c_mid:(a + 1) * c_mid] = piece

        loop(0, nz, place)
        for dw in range(3):
            wt[:, dw * kb:(dw + 1) * kb] = wk[dw].reshape(kb, 2 * c_mid).T.astype(wt.dtype)
        w2x[:, 9 * c_mid:] = gs[...].astype(jnp.float32).reshape(n * ch, c_out).T.astype(w2x.dtype)

    def inner_halo(img):
        return pltpu.make_async_remote_copy(
            src_ref=xbuf.at[img, :, pl.ds(2 + (1 - my_c) * (tile - 2), 2)],
            dst_ref=xbuf.at[img, :, pl.ds(my_c * (tile + 2), 2)],
            send_sem=send_h.at[img, 0], recv_sem=recv_h.at[img, 0], device_id={'model': sibling}, device_id_type=MESH)

    def outer_halo(img):
        return pltpu.make_async_remote_copy(
            src_ref=xbuf.at[img, :, pl.ds(2 + my_c * (tile - 2), 2)],
            dst_ref=xbuf.at[img, :, pl.ds((1 - my_c) * (tile + 2), 2)],
            send_sem=send_h.at[img, 1], recv_sem=recv_h.at[img, 1],
            device_id={'model': (me + n - 1 + 2 * my_c) % n}, device_id_type=MESH)

    has_outer = (me != 0) & (me != n - 1)
    sends_last = (me != 1) & (me != n - 2)

    def when(cond, act):
        @pl.when(cond)
        def _():
            act()

    flip = tile // 2

    def pair_in(img, k):
        pair(img, k + my_c * (flip - 2 * k))

    def rows_in(img, lo, hi, unroll):
        loop(lo, hi, lambda k: second(img, k + my_c * (tile - 1 - 2 * k)), unroll=unroll)

    def most(img, between):
        loop(1, flip - 1, lambda k: pair_in(img, k), unroll=3)
        inner_halo(img).wait_recv()
        loop(flip - 1, flip + 1, lambda k: pair_in(img, k), unroll=2)
        between()
        rows_in(img, 2, tile, 7)

    def edge(img):
        when(has_outer, lambda: outer_halo(img).wait_recv())
        pair_in(img, 0)
        rows_in(img, 0, 2, 2)

    def begin(img):
        arrived(xbuf.at[img, :, pl.ds(0, tile)], recv_x.at[img])
        inner_halo(img).start()
        when(has_outer, lambda: outer_halo(img).start())

    begin(0)
    build_weights()
    most(0, lambda: None)
    left(2, 6, tile)
    send(last, first, inner, 4)
    begin(1)
    send(last, rest, inner, 5)
    edge(0)

    def last_sends():
        left(4, 6, block - LATE)
        send(last, first, outer, 6)

    most(1, last_sends)
    left(5, n - 7, block - LATE)
    send(last, rest, outer, 7)
    edge(1)
    arrived(xbuf.at[last, :, pl.ds(0, block - LATE)], recv_x.at[last])
    when(sends_last, lambda: inner_halo(last).start())
    first_p = LATE // 2 + 1
    loop(first_p, flip - 1, lambda k: pair_in(last, k), unroll=3)
    when(has_outer, lambda: inner_halo(last).wait_recv())
    loop(flip - 1, flip + 1, lambda k: pair_in(last, k), unroll=2)
    rows_in(last, 2 * first_p, tile, 8)

    left(3, n - 7, tile)
    left(6, 6, LATE)
    left(7, n - 7, LATE)
    for k, ref in enumerate((gw.at[pl.ds(0, nz - 1), 0], gs.at[pl.ds(0, nz - 1), 0])):
        pltpu.make_async_remote_copy(src_ref=ref, dst_ref=ref, send_sem=send_w.at[k], recv_sem=recv_w.at[k],
                                     device_id={'model': sibling}, device_id_type=MESH).wait_send()
    for img in range(last):
        inner_halo(img).wait_send()
        when(has_outer, lambda: outer_halo(img).wait_send())
    when(sends_last, lambda: inner_halo(last).wait_send())
    arrived(xbuf.at[last, :, pl.ds(0, LATE)], recv_x.at[ni])


def finish_kernel(n, height, xbuf, wt, w2x, b1c, b2_ref, y1s_in, y2, out_ref, y1s, yb, sem):
    ni, tile = y2.shape[0], y2.shape[1]
    last = ni - 1
    my_c = lax.axis_index('model') % 2
    first_p = LATE // 2 + 1
    left = 2 * first_p
    done = tile - left
    ready = (1 - my_c) * left
    todo = my_c * done
    copies = [pltpu.make_async_copy(y2.at[img, pl.ds(r, 4)], out_ref.at[img, pl.ds(r, 4)], sem.at[0])
              for img in range(last) for r in range(0, tile, 4)]
    copies += [pltpu.make_async_copy(y2.at[last, pl.ds(ready, done)], out_ref.at[last, pl.ds(ready, done)], sem.at[1])]
    for copy in copies:
        copy.start()
    step = 3 * b1c.shape[0]
    edge = (1 - my_c) * left + my_c * (tile - left)
    y1s[pl.ds(pl.multiple_of(edge * step, step), 2 * step), :] = y1s_in[pl.ds(pl.multiple_of(edge * step, step), 2 * step), :]
    flip = tile // 2
    loop(0, first_p, lambda k: first_pair(n, height, last, k + my_c * (flip - 2 * k), xbuf, wt, b1c, y1s), unroll=2)

    def row(k):
        yb[k] = second_row(last, k + todo, xbuf, w2x, b2_ref, y1s)
        pltpu.make_async_copy(yb.at[k], out_ref.at[last, k + todo], sem.at[2]).start()

    loop(0, left, row, unroll=8)
    for copy in copies:
        copy.wait()
    pltpu.make_async_copy(yb, out_ref.at[last, pl.ds(todo, left)], sem.at[2]).wait()


def solution(mesh):
    n = mesh.shape['model']

    def local_step(images, w_conv1, b_conv1, w_conv2, b_conv2, w_short):
        ni, height, width, ch = images.shape
        c_mid, c_out = w_conv1.shape[3], w_short.shape[1]
        tile, halves, nz = height // n, width // LANES, n // 2
        kb = n * 4 * ch
        x = images.transpose(0, 1, 3, 2).reshape(ni, height, ch, halves, LANES).transpose(0, 1, 3, 2, 4)
        vmem = pl.BlockSpec(memory_space=pltpu.VMEM)
        hbm = pl.BlockSpec(memory_space=pltpu.HBM)
        dma = pltpu.SemaphoreType.DMA
        y1s = pltpu.VMEM(((tile + 2) * 3 * c_mid, width), jnp.bfloat16)
        parts = pl.pallas_call(
            functools.partial(gather_kernel, n),
            out_shape=[
                pltpu.VMEM((ni, n, tile + 4, halves, ch, LANES), jnp.bfloat16),
                pltpu.VMEM((2 * c_mid, 3 * kb), jnp.bfloat16),
                pltpu.VMEM((c_out, 9 * c_mid + n * ch), jnp.bfloat16),
                pltpu.VMEM((c_mid, LANES), jnp.float32),
                pltpu.VMEM((1, c_out), jnp.float32),
                y1s,
                pltpu.VMEM((ni, tile, width, c_out), jnp.float32),
            ],
            in_specs=[hbm] * 6,
            out_specs=[vmem] * 7,
            scratch_shapes=[
                pltpu.VMEM((nz, 2, 3, 3, ch, c_mid), jnp.bfloat16),
                pltpu.VMEM((nz, 2, ch, c_out), jnp.bfloat16),
                pltpu.VMEM((3, n, 4 * ch, 2 * c_mid), jnp.float32),
                pltpu.VMEM(w_conv2.shape, w_conv2.dtype),
                pltpu.VMEM((1, c_mid), jnp.float32),
                dma((3,)), pltpu.SemaphoreType.REGULAR((nz // 2,)),
                dma((8,)), dma((ni + 1,)), dma((ni, 2)), dma((ni, 2)), dma((2,)), dma((2, 2)), dma((2,)), dma((2,)),
            ],
            compiler_params=pltpu.CompilerParams(collective_id=0, has_side_effects=True, vmem_limit_bytes=20 * 2**20),
        )(*[pltpu.with_memory_space_constraint(v, pltpu.HBM) for v in (x, w_conv1, b_conv1.reshape(1, c_mid), w_conv2, b_conv2.reshape(1, c_out), w_short)])
        return pl.pallas_call(
            functools.partial(finish_kernel, n, height),
            out_shape=jax.ShapeDtypeStruct((ni, tile, width, c_out), jnp.float32),
            in_specs=[vmem] * 7,
            out_specs=hbm,
            scratch_shapes=[y1s, pltpu.VMEM((LATE + 2, width, c_out), jnp.float32), dma((3,))],
            compiler_params=pltpu.CompilerParams(vmem_limit_bytes=20 * 2**20),
        )(*parts)

    return jax.shard_map(local_step, mesh=mesh, in_specs=(P('data', None, None, 'model'), P(None, None, 'model', None), P(), P(), P(), P('model', None)), out_specs=P('data', 'model', None, None), check_vma=False)
```

```python
import functools

import jax
import jax.numpy as jnp
from jax import lax
from jax.experimental import pallas as pl
from jax.experimental.pallas import tpu as pltpu
from jax.sharding import PartitionSpec as P

MESH = pl.DeviceIdType.MESH
LANES = 128
LATE = 6


def shift_right(v):
    first = lax.broadcasted_iota(jnp.int32, v.shape, 1) == 0
    return jnp.where(first, jnp.zeros_like(v), pltpu.roll(v, 1, axis=1))


def shift_left(v):
    last = lax.broadcasted_iota(jnp.int32, v.shape, 1) == v.shape[1] - 1
    return jnp.where(last, jnp.zeros_like(v), pltpu.roll(v, v.shape[1] - 1, axis=1))


def first_pair(n, height, img, p, xbuf, wt, b1c, y1s):
    ni, _, rows, halves, ch, _ = xbuf.shape
    tile = rows - 4
    c_mid = wt.shape[0] // 2
    kb = n * 4 * ch
    me = lax.axis_index('model')
    x_left = xbuf[img, :, pl.ds(2 * p, 4), 0]
    x_right = xbuf[img, :, pl.ds(2 * p, 4), 1]
    x0 = jnp.concatenate([x_left.reshape(kb, LANES), x_right.reshape(kb, LANES)], axis=1)
    rhs = jnp.concatenate([shift_right(x0), x0, shift_left(x0)], axis=0)
    z2 = jnp.dot(wt[...], rhs, preferred_element_type=jnp.float32)
    for a in range(2):
        y = jnp.maximum(z2[a * c_mid:(a + 1) * c_mid] + jnp.concatenate([b1c[...]] * halves, axis=1), 0.0)
        row = me * tile - 1 + 2 * p + a
        y = jnp.where((row >= 0) & (row < height), y, 0.0).astype(jnp.bfloat16)
        base = pl.multiple_of((2 * p + a) * 3 * c_mid, c_mid)
        y1s[pl.ds(base, c_mid), :] = shift_right(y)
        y1s[pl.ds(base + c_mid, c_mid), :] = y
        y1s[pl.ds(base + 2 * c_mid, c_mid), :] = shift_left(y)


def second_row(img, r, xbuf, w2x, b2_ref, y1s):
    _, n, _, halves, ch, _ = xbuf.shape
    c_mid = w2x.shape[0]
    base = pl.multiple_of(r * 3 * c_mid, c_mid)
    x_row = jnp.concatenate([xbuf[img, :, r + 2, h].reshape(n * ch, LANES) for h in range(halves)], axis=1)
    rhs = jnp.concatenate([y1s[pl.ds(base, 9 * c_mid), :], x_row], axis=0)
    y2 = jnp.dot(w2x[...], rhs, preferred_element_type=jnp.float32)
    return y2.T + b2_ref[...]


def loop(lo, hi, body, unroll=1):
    def step(i, _):
        body(i)
        return 0

    lax.fori_loop(lo, hi, step, 0, unroll=unroll)


def gather_kernel(n, x_ref, w1_ref, b1_hbm, w2_hbm, b2_hbm, ws_ref,
                  xbuf, wt, w2x, b1c, b2_ref, y1s, y2,
                  gw, gs, wk, w2_ref, b1_ref,
                  local, phase, send_x, recv_x, send_h, recv_h, send_w, recv_w, send_v, recv_v):
    ni, height, halves, ch, _ = x_ref.shape
    tile = height // n
    nz = n // 2
    last = ni - 1
    assert last == 2
    c_mid, c_out = w1_ref.shape[3], ws_ref.shape[1]
    kb = n * 4 * ch
    me = lax.axis_index('model')
    my_z, my_c = me // 2, me % 2
    sibling = me + 1 - 2 * my_c

    def core(d, c):
        return ((my_z + d) % nz) * 2 + (my_c + c) % 2

    barrier = pltpu.get_barrier_semaphore()
    for dest in (sibling, core(1, 0), core(1, 1), core(nz - 1, 0), core(nz - 1, 1)):
        pl.semaphore_signal(barrier, inc=1, device_id={'model': dest}, device_id_type=MESH)

    block = tile + 2
    inner, outer = (block - LATE, last), (LATE, ni)

    def part_copy(img, dest, odd, part):
        rows, k = part
        if img < last:
            base, off = dest * tile, 0
        else:
            base = jnp.clip(dest * tile - 2 * (1 - odd), 0, height - block)
            off = (1 - odd) * LATE if part is inner else odd * (block - LATE)
        return (x_ref.at[img, pl.ds(base + off, rows)], xbuf.at[img, me, pl.ds(base + off - dest * tile + 2, rows)], recv_x.at[k])

    def parts_of(img):
        return [(tile, img)] if img < last else [inner, outer]

    def send(img, hops, part, batch):
        for d in hops:
            for c in range(2) if d else (1,):
                dest = core(d, c)
                src, dst, sem = part_copy(img, dest, (my_c + c) % 2, part)
                pltpu.make_async_remote_copy(src_ref=src, dst_ref=dst, send_sem=send_x.at[batch], recv_sem=sem,
                                             device_id={'model': dest}, device_id_type=MESH).start()

    def left(batch, copies, rows):
        ref = xbuf.at[0, pl.ds(0, copies), pl.ds(0, rows)]
        pltpu.make_async_remote_copy(src_ref=ref, dst_ref=ref, send_sem=send_x.at[batch], recv_sem=recv_x.at[0],
                                     device_id={'model': sibling}, device_id_type=MESH).wait_send()

    hubs = [2, nz - 2] if nz >= 8 else [d for d in range(1, nz)]

    own = 0

    def send_weights(moves, k_sem):
        for off, d in moves:
            for k, (src, dst) in enumerate(((w1_ref, gw), (ws_ref, gs))):
                piece = dst.at[(my_z + off) % nz, my_c]
                pltpu.make_async_remote_copy(
                    src_ref=src if off is own else piece, dst_ref=piece, send_sem=send_w.at[k], recv_sem=recv_w.at[k, k_sem],
                    device_id={'model': core(d, 0)}, device_id_type=MESH).start()

    def wait_weights(pieces, k_sem):
        for k, ref in enumerate((gw, gs)):
            arrived(ref.at[pl.ds(0, pieces), my_c], recv_w.at[k, k_sem])

    def arrived(ref, sem):
        pltpu.make_async_remote_copy(src_ref=ref, dst_ref=ref, send_sem=send_x.at[0], recv_sem=sem,
                                     device_id={'model': sibling}, device_id_type=MESH).wait_recv()

    for img in range(ni):
        for part in parts_of(img):
            src, dst, sem = part_copy(img, me, my_c, part)
            pltpu.make_async_copy(src, dst, sem).start()
    pltpu.make_async_copy(w1_ref, gw.at[my_z, my_c], recv_w.at[0, 1]).start()
    pltpu.make_async_copy(ws_ref, gs.at[my_z, my_c], recv_w.at[1, 1]).start()

    fetches = [pltpu.make_async_copy(src, dst, local.at[k])
               for k, (src, dst) in enumerate(((b1_hbm, b1_ref), (b2_hbm, b2_ref), (w2_hbm, w2_ref)))]
    for fetch in fetches:
        fetch.start()

    pl.semaphore_wait(barrier, 5)
    for d in range(1, nz // 2 + 1):
        if d < nz // 2:
            for side in (1, nz - 1):
                pl.semaphore_signal(phase.at[d - 1], inc=1, device_id={'model': core(side, 0)}, device_id_type=MESH)
        send(0, [d, nz - d] if d < nz // 2 else [d], parts_of(0)[0], 0 if d <= nz // 4 else 1)
        if d < nz // 2:
            pl.semaphore_wait(phase.at[d - 1], 2)
        if d == 1 and nz >= 8:
            send_weights([(own, hub) for hub in hubs], 0)
    send(0, [0], parts_of(0)[0], 1)
    near = [d for k in range(1, nz // 2) for d in (k, nz - k)]
    far = [nz // 2] + near[::-1]
    if nz >= 8:
        wait_weights(2, 0)
        send_weights([(nz - 2, 1), (nz - 2, nz - 1), (2, 1), (2, nz - 1)], 1)
        send_weights([((2 + (nz - 4) * (1 - my_c)), (nz - 2) - (nz - 4) * (1 - my_c))], 1)
    else:
        send_weights([(own, hub) for hub in hubs], 0)
    near_copies = 4 * (nz // 4)
    first, rest = far[:3], far[3:] + [0]
    left(0, near_copies, tile)
    send(1, first, parts_of(1)[0], 2)

    for owner, r0 in ((0, 0), (n - 1, tile + 2)):
        @pl.when(me == owner)
        def _():
            for img in range(ni):
                xbuf[img, :, r0:r0 + 2] = jnp.zeros((n, 2, halves, ch, LANES), xbuf.dtype)

    for fetch in fetches:
        fetch.wait()
    b1c[...] = jnp.broadcast_to(b1_ref[...], (LANES, c_mid)).T
    for t in range(9):
        w2x[:, t * c_mid:(t + 1) * c_mid] = w2_ref[t // 3, t % 3].astype(jnp.float32).T.astype(w2x.dtype)
    wk[...] = jnp.zeros_like(wk)
    left(1, n - 1 - near_copies, tile)
    send(1, rest, parts_of(1)[0], 3)

    def pair(img, p):
        first_pair(n, height, img, p, xbuf, wt, b1c, y1s)

    def second(img, r):
        y2[img, r] = second_row(img, r, xbuf, w2x, b2_ref, y1s)

    def build_weights():
        wait_weights(nz - 2 if nz >= 8 else 1, 1)
        if nz < 8:
            wait_weights(nz - 1, 0)
        shares = []
        for k, ref in enumerate((gw.at[:, my_c], gs.at[:, my_c])):
            shares.append(pltpu.make_async_remote_copy(
                src_ref=ref, dst_ref=ref, send_sem=send_v.at[k], recv_sem=recv_v.at[k],
                device_id={'model': sibling}, device_id_type=MESH))
            shares[k].start()
        for share in shares:
            share.wait()

        def place(z):
            for c in range(2):
                src = z * 2 + c
                for dh in range(3):
                    for dw in range(3):
                        piece = gw[z, c, dh, dw].astype(jnp.float32)
                        for a in range(2):
                            wk[dw, src, (dh + a) * ch:(dh + a + 1) * ch, a * c_mid:(a + 1) * c_mid] = piece

        loop(0, nz, place)
        for dw in range(3):
            wt[:, dw * kb:(dw + 1) * kb] = wk[dw].reshape(kb, 2 * c_mid).T.astype(wt.dtype)
        w2x[:, 9 * c_mid:] = gs[...].astype(jnp.float32).reshape(n * ch, c_out).T.astype(w2x.dtype)

    def inner_halo(img):
        return pltpu.make_async_remote_copy(
            src_ref=xbuf.at[img, :, pl.ds(2 + (1 - my_c) * (tile - 2), 2)],
            dst_ref=xbuf.at[img, :, pl.ds(my_c * (tile + 2), 2)],
            send_sem=send_h.at[img, 0], recv_sem=recv_h.at[img, 0], device_id={'model': sibling}, device_id_type=MESH)

    def outer_halo(img):
        return pltpu.make_async_remote_copy(
            src_ref=xbuf.at[img, :, pl.ds(2 + my_c * (tile - 2), 2)],
            dst_ref=xbuf.at[img, :, pl.ds((1 - my_c) * (tile + 2), 2)],
            send_sem=send_h.at[img, 1], recv_sem=recv_h.at[img, 1],
            device_id={'model': (me + n - 1 + 2 * my_c) % n}, device_id_type=MESH)

    has_outer = (me != 0) & (me != n - 1)
    sends_last = (me != 1) & (me != n - 2)

    def when(cond, act):
        @pl.when(cond)
        def _():
            act()

    flip = tile // 2

    def pair_in(img, k):
        pair(img, k + my_c * (flip - 2 * k))

    def rows_in(img, lo, hi, unroll):
        loop(lo, hi, lambda k: second(img, k + my_c * (tile - 1 - 2 * k)), unroll=unroll)

    def most(img, between):
        loop(1, flip - 1, lambda k: pair_in(img, k), unroll=3)
        inner_halo(img).wait_recv()
        loop(flip - 1, flip + 1, lambda k: pair_in(img, k), unroll=2)
        between()
        rows_in(img, 2, tile, 7)

    def edge(img):
        when(has_outer, lambda: outer_halo(img).wait_recv())
        pair_in(img, 0)
        rows_in(img, 0, 2, 2)

    def begin(img):
        arrived(xbuf.at[img, :, pl.ds(0, tile)], recv_x.at[img])
        inner_halo(img).start()
        when(has_outer, lambda: outer_halo(img).start())

    begin(0)
    build_weights()
    most(0, lambda: None)
    left(2, 6, tile)
    send(last, first, inner, 4)
    begin(1)
    send(last, rest, inner, 5)
    edge(0)

    def last_sends():
        left(4, 6, block - LATE)
        send(last, first, outer, 6)
        send(last, rest, outer, 7)

    most(1, last_sends)
    edge(1)
    arrived(xbuf.at[last, :, pl.ds(0, block - LATE)], recv_x.at[last])
    when(sends_last, lambda: inner_halo(last).start())
    first_p = LATE // 2 + 1
    loop(first_p, flip - 1, lambda k: pair_in(last, k), unroll=3)
    when(has_outer, lambda: inner_halo(last).wait_recv())
    loop(flip - 1, flip + 1, lambda k: pair_in(last, k), unroll=2)
    rows_in(last, 2 * first_p, tile, 8)

    left(3, n - 7, tile)
    left(5, n - 7, block - LATE)
    left(6, 6, LATE)
    left(7, n - 7, LATE)
    for k, ref in enumerate((gw.at[pl.ds(0, nz - 1), 0], gs.at[pl.ds(0, nz - 1), 0])):
        pltpu.make_async_remote_copy(src_ref=ref, dst_ref=ref, send_sem=send_w.at[k], recv_sem=recv_w.at[k],
                                     device_id={'model': sibling}, device_id_type=MESH).wait_send()
    for img in range(last):
        inner_halo(img).wait_send()
        when(has_outer, lambda: outer_halo(img).wait_send())
    when(sends_last, lambda: inner_halo(last).wait_send())
    arrived(xbuf.at[last, :, pl.ds(0, LATE)], recv_x.at[ni])


def finish_kernel(n, height, xbuf, wt, w2x, b1c, b2_ref, y1s_in, y2, out_ref, y1s, yb, sem):
    ni, tile = y2.shape[0], y2.shape[1]
    last = ni - 1
    my_c = lax.axis_index('model') % 2
    first_p = LATE // 2 + 1
    left = 2 * first_p
    done = tile - left
    ready = (1 - my_c) * left
    todo = my_c * done
    copies = [pltpu.make_async_copy(y2.at[img, pl.ds(r, 4)], out_ref.at[img, pl.ds(r, 4)], sem.at[0])
              for img in range(last) for r in range(0, tile, 4)]
    copies += [pltpu.make_async_copy(y2.at[last, pl.ds(ready, done)], out_ref.at[last, pl.ds(ready, done)], sem.at[1])]
    for copy in copies:
        copy.start()
    step = 3 * b1c.shape[0]
    edge = (1 - my_c) * left + my_c * (tile - left)
    y1s[pl.ds(pl.multiple_of(edge * step, step), 2 * step), :] = y1s_in[pl.ds(pl.multiple_of(edge * step, step), 2 * step), :]
    flip = tile // 2
    loop(0, first_p, lambda k: first_pair(n, height, last, k + my_c * (flip - 2 * k), xbuf, wt, b1c, y1s), unroll=2)

    def row(k):
        yb[k] = second_row(last, k + todo, xbuf, w2x, b2_ref, y1s)
        pltpu.make_async_copy(yb.at[k], out_ref.at[last, k + todo], sem.at[2]).start()

    loop(0, left, row, unroll=8)
    for copy in copies:
        copy.wait()
    pltpu.make_async_copy(yb, out_ref.at[last, pl.ds(todo, left)], sem.at[2]).wait()


def solution(mesh):
    n = mesh.shape['model']

    def local_step(images, w_conv1, b_conv1, w_conv2, b_conv2, w_short):
        ni, height, width, ch = images.shape
        c_mid, c_out = w_conv1.shape[3], w_short.shape[1]
        tile, halves, nz = height // n, width // LANES, n // 2
        kb = n * 4 * ch
        x = images.transpose(0, 1, 3, 2).reshape(ni, height, ch, halves, LANES).transpose(0, 1, 3, 2, 4)
        vmem = pl.BlockSpec(memory_space=pltpu.VMEM)
        hbm = pl.BlockSpec(memory_space=pltpu.HBM)
        dma = pltpu.SemaphoreType.DMA
        y1s = pltpu.VMEM(((tile + 2) * 3 * c_mid, width), jnp.bfloat16)
        parts = pl.pallas_call(
            functools.partial(gather_kernel, n),
            out_shape=[
                pltpu.VMEM((ni, n, tile + 4, halves, ch, LANES), jnp.bfloat16),
                pltpu.VMEM((2 * c_mid, 3 * kb), jnp.bfloat16),
                pltpu.VMEM((c_out, 9 * c_mid + n * ch), jnp.bfloat16),
                pltpu.VMEM((c_mid, LANES), jnp.float32),
                pltpu.VMEM((1, c_out), jnp.float32),
                y1s,
                pltpu.VMEM((ni, tile, width, c_out), jnp.float32),
            ],
            in_specs=[hbm] * 6,
            out_specs=[vmem] * 7,
            scratch_shapes=[
                pltpu.VMEM((nz, 2, 3, 3, ch, c_mid), jnp.bfloat16),
                pltpu.VMEM((nz, 2, ch, c_out), jnp.bfloat16),
                pltpu.VMEM((3, n, 4 * ch, 2 * c_mid), jnp.float32),
                pltpu.VMEM(w_conv2.shape, w_conv2.dtype),
                pltpu.VMEM((1, c_mid), jnp.float32),
                dma((3,)), pltpu.SemaphoreType.REGULAR((nz // 2,)),
                dma((8,)), dma((ni + 1,)), dma((ni, 2)), dma((ni, 2)), dma((2,)), dma((2, 2)), dma((2,)), dma((2,)),
            ],
            compiler_params=pltpu.CompilerParams(collective_id=0, has_side_effects=True, vmem_limit_bytes=20 * 2**20),
        )(*[pltpu.with_memory_space_constraint(v, pltpu.HBM) for v in (x, w_conv1, b_conv1.reshape(1, c_mid), w_conv2, b_conv2.reshape(1, c_out), w_short)])
        return pl.pallas_call(
            functools.partial(finish_kernel, n, height),
            out_shape=jax.ShapeDtypeStruct((ni, tile, width, c_out), jnp.float32),
            in_specs=[vmem] * 7,
            out_specs=hbm,
            scratch_shapes=[y1s, pltpu.VMEM((LATE + 2, width, c_out), jnp.float32), dma((3,))],
            compiler_params=pltpu.CompilerParams(vmem_limit_bytes=20 * 2**20),
        )(*parts)

    return jax.shard_map(local_step, mesh=mesh, in_specs=(P('data', None, None, 'model'), P(None, None, 'model', None), P(), P(), P(), P('model', None)), out_specs=P('data', 'model', None, None), check_vma=False)
```
